32 devices in a mesh: chan: 4 (over z), pulse: 4 (over x, core), range: 2 (over y).
Axes of the slice: x: 2, y: 2, z: 4, core: 2. Of those that a mesh axis runs over, the one named last changes fastest.
Arguments:
- signal: bfloat16 [2, 64, 32, 8192], P(None, 'chan', 'pulse', 'range'), may hold values from -6 to 6
- steering: bfloat16 [2, 32, 64], replicated, may hold values from -0.5 to 0.5
- spectrum: float32 [2, 8192], replicated, may hold values from -6 to 6
Outputs:
- detection: float32 [32, 32, 8192], P('chan', 'pulse', 'range')
The draws below stay inside these ranges and needn't reach their ends.
All inputs are finite; a program needn't handle non-finite values.
Results may differ from the reference program's by a relative error of at most 0.0087.
Values may be sent and summed in bfloat16 or wider, within the bound.
A program may use at most 64 MiB of HBM per device.

```python
import math
import jax
import jax.numpy as jnp
from jax import lax

CH = 64
BEAMS = 32
GUARD = 4
TRAIN = 16
PULSES = 32
RANGE = 8192


def block_levels(own_key, shape, pieces, low, top_value):
    loudness, own = 1.0, jax.random.fold_in(own_key, 6)
    for position, blocks in pieces:
        draws = jnp.exp(jax.random.uniform(jax.random.fold_in(own, position), (blocks,), jnp.float32, low / len(pieces), top_value / len(pieces)))
        loudness = loudness * jnp.repeat(draws, shape[position] // blocks).reshape([-1 if axis == position else 1 for axis in range(len(shape))])
    return loudness


def scatter_about(stream_key, extent, width, reach, split=(), held_as=jnp.bfloat16):
    entries = jax.random.normal(stream_key, extent, jnp.float32) * width
    if len(split) > 0:
        entries = block_levels(stream_key, extent, split, -0.22, 0.18) * entries
    return jnp.clip(entries, min=-reach, max=reach).astype(held_as)


def setup_inputs(seed: int = 0) -> dict:
    splits = jax.random.split(jax.random.key(seed), 4)
    return {
        "signal": scatter_about(splits[0], (2, CH, PULSES, RANGE), 1.0, 6.0, ((1, 4), (2, 4), (3, 2))),
        "steering": scatter_about(splits[1], (2, BEAMS, CH), (2 * CH) ** -0.5, 0.5),
        "spectrum": scatter_about(splits[2], (2, RANGE), 1.0, 6.0, (), jnp.float32),
    }


NOISE_FLOOR = 0.25

def doppler_tables(pulse_count):
    row_ids = lax.broadcasted_iota(jnp.int32, (pulse_count, pulse_count), 0)
    col_ids = lax.broadcasted_iota(jnp.int32, (pulse_count, pulse_count), 1)
    phase_angle = (row_ids * col_ids % pulse_count).astype(jnp.float32) * (2.0 * math.pi / pulse_count)
    norm_scale = 1.0 / math.sqrt(pulse_count)
    table_real = (jnp.cos(phase_angle) * norm_scale).astype(jnp.bfloat16)
    table_imag = (-jnp.sin(phase_angle) * norm_scale).astype(jnp.bfloat16)
    return (table_real, table_imag)

def reference(signal, steering, spectrum):
    w_real = steering[0]
    w_imag = steering[1]
    stacked = jnp.concatenate([jnp.concatenate([w_real, -w_imag], 1), jnp.concatenate([w_imag, w_real], 1)], 0)
    flat_signal = signal.reshape(2 * CH, PULSES * RANGE)
    beam_data = jnp.dot(stacked, flat_signal, preferred_element_type=jnp.float32).astype(jnp.bfloat16)
    beam_data = beam_data.reshape(2, BEAMS, PULSES, RANGE)
    response = lax.complex(spectrum[0], spectrum[1])
    dop_real, dop_imag = doppler_tables(PULSES)
    halo_width = GUARD + TRAIN

    def one_beam(beam_slab):
        line_field = lax.complex(beam_slab[0].astype(jnp.float32), beam_slab[1].astype(jnp.float32))
        compressed = jnp.fft.ifft(jnp.fft.fft(line_field, axis=-1) * response, axis=-1)
        comp_real = jnp.real(compressed).astype(jnp.bfloat16)
        comp_imag = jnp.imag(compressed).astype(jnp.bfloat16)
        mixed_real = jnp.dot(dop_real, comp_real, preferred_element_type=jnp.float32) - jnp.dot(dop_imag, comp_imag, preferred_element_type=jnp.float32)
        mixed_imag = jnp.dot(dop_real, comp_imag, preferred_element_type=jnp.float32) + jnp.dot(dop_imag, comp_real, preferred_element_type=jnp.float32)
        power_map = mixed_real * mixed_real + mixed_imag * mixed_imag
        padded = jnp.pad(power_map, ((0, 0), (halo_width, halo_width)))
        window_sum = jnp.zeros_like(power_map)
        for offset in range(1, TRAIN + 1):
            left_start = halo_width - GUARD - offset
            right_start = halo_width + GUARD + offset
            window_sum = window_sum + padded[:, left_start:left_start + RANGE] + padded[:, right_start:right_start + RANGE]
        noise_level = window_sum / (2.0 * TRAIN)
        return power_map / (noise_level + NOISE_FLOOR)
    return lax.map(one_beam, jnp.transpose(beam_data, (1, 0, 2, 3)))
```

```python
import functools
import math

import jax
import jax.numpy as jnp
import numpy as np
from jax import lax
from jax.experimental import pallas as pl
from jax.experimental.pallas import tpu as pltpu
from jax.sharding import PartitionSpec as P

GUARD = 4
TRAIN = 16
NOISE_FLOOR = 0.25
LANES = 128
ROWS = 8
CHUNKS = 16
BF = jnp.bfloat16
F32 = jnp.float32
VM = 60 * 1024 * 1024


def dot(a, b):
    return jnp.dot(a, b, preferred_element_type=F32)


def doppler_table(count):
    ids = np.arange(count)
    angle = (np.outer(ids, ids) % count) * (2.0 * np.pi / count)
    scale = 1.0 / math.sqrt(count)
    return jnp.asarray(np.cos(angle) * scale, BF), jnp.asarray(-np.sin(angle) * scale, BF)


def expand(left_ids, left_tag, table, right_ids, right_tag):
    n, m = table.shape
    left = (jnp.asarray(left_ids, jnp.int32)[:, None] == jnp.arange(n)[None, :]).astype(BF)
    right = (jnp.arange(m)[:, None] == jnp.asarray(right_ids, jnp.int32)[None, :]).astype(BF)
    wide = dot(dot(left, table).astype(BF), right)
    same = jnp.asarray(left_tag, jnp.int32)[:, None] == jnp.asarray(right_tag, jnp.int32)[None, :]
    return jnp.where(same, wide, 0.0).astype(BF)


def grid_ids(*sizes):
    return [g.reshape(-1) for g in np.meshgrid(*[np.arange(s) for s in sizes], indexing="ij")]


def call(body, out_shape, name):
    return pl.pallas_call(
        body,
        out_shape=out_shape,
        compiler_params=pltpu.CompilerParams(vmem_limit_bytes=VM),
        name=name,
    )


def form_kernel(w_ref, x_ref, o_ref):
    o_ref[...] = dot(w_ref[...], x_ref[...]).astype(BF)


def range_kernel(blocks, x_ref, f_ref, fi_ref, t_ref, l_ref, li_ref, h_ref, o_ref):
    sources, rows, width = x_ref.shape
    per = width // LANES
    groups = rows // 16
    m_count = sources * per
    tile = []
    for g in range(groups):
        parts = [
            x_ref[s, 16 * g : 16 * g + 16, LANES * j : LANES * j + LANES]
            for s in range(sources)
            for j in range(per)
        ]
        tile.append(jnp.concatenate(parts, axis=0))
    outer = dot(f_ref[...], jnp.concatenate(tile, axis=1))
    tr, ti = t_ref[0], t_ref[1]
    hr, hi = h_ref[0], h_ref[1]
    back = []
    for g in range(groups):
        a = outer[:, LANES * g : LANES * g + LANES].reshape(m_count, 2, ROWS, LANES)
        ar, ai = a[:, 0], a[:, 1]
        b = jnp.concatenate([ar * tr - ai * ti, ar * ti + ai * tr], axis=-1)
        c = dot(b.reshape(m_count * ROWS, 2 * LANES).astype(BF), l_ref[...])
        c = c.reshape(m_count, ROWS, 2 * LANES)
        cr, ci = c[..., :LANES], c[..., LANES:]
        d = jnp.concatenate([cr * hr - ci * hi, cr * hi + ci * hr], axis=-1)
        e = dot(d.reshape(m_count * ROWS, 2 * LANES).astype(BF), li_ref[...])
        e = e.reshape(m_count, ROWS, 2 * LANES)
        er, ei = e[..., :LANES], e[..., LANES:]
        f = jnp.stack([er * tr + ei * ti, ei * tr - er * ti], axis=1)
        back.append(f.reshape(m_count * 16, LANES).astype(BF))
    y = dot(fi_ref[...], jnp.concatenate(back, axis=1)).astype(BF)
    span = m_count // blocks
    for d in range(blocks):
        for j in range(-1, span + 1):
            m = d * span + j
            for g in range(groups):
                if 0 <= m < m_count:
                    v = y[16 * m : 16 * m + 16, LANES * g : LANES * g + LANES]
                else:
                    v = jnp.zeros((16, LANES), BF)
                o_ref[d, 16 * g : 16 * g + 16, LANES * (j + 1) : LANES * (j + 2)] = v


def cfar_kernel(d_ref, x_ref, n_ref, o_ref):
    half = d_ref.shape[0] // 2
    mix = dot(d_ref[...], x_ref[...].reshape(d_ref.shape[1], x_ref.shape[-1]))
    re, im = mix[:half], mix[half:]
    power = re * re + im * im
    narrow = power.astype(BF)
    shape = o_ref.shape[:-1] + (LANES,)
    for j in range(o_ref.shape[-1] // LANES):
        noise = dot(narrow[:, LANES * j : LANES * (j + 3)], n_ref[...])
        own = power[:, LANES * (j + 1) : LANES * (j + 2)]
        found = (own / (noise + NOISE_FLOOR)).astype(BF)
        o_ref[..., LANES * j : LANES * j + LANES] = found.reshape(shape)


def cfar_only_kernel(p_ref, n_ref, o_ref):
    narrow = p_ref[...].astype(BF)
    for j in range(o_ref.shape[1] // LANES):
        noise = dot(narrow[:, LANES * j : LANES * (j + 3)], n_ref[...])
        own = p_ref[:, LANES * (j + 1) : LANES * (j + 2)]
        o_ref[:, LANES * j : LANES * j + LANES] = (own / (noise + NOISE_FLOOR)).astype(BF)


def place_kernel(x_ref, o_ref):
    count, _, width = x_ref.shape
    for s in range(count):
        o_ref[:, width * s : width * s + width] = x_ref[s].astype(F32)


def complex_rows(re, im):
    top = np.stack([re, -im], -1)
    low = np.stack([im, re], -1)
    return np.stack([top, low], 1).reshape(2 * re.shape[0], 2 * re.shape[1])


def shards_split(signal, steering, spectrum):
    beams, chans = steering.shape[1], steering.shape[2]
    _, chan_own, pulse_own, gates = signal.shape
    zs, xs, ys = (lax.axis_size(a) for a in ("chan", "pulse", "range"))
    beam_own = beams // zs
    part = pulse_own // ys
    full = gates * ys
    block = gates // zs
    m_count = full // LANES
    groups = beam_own * part // ROWS
    pulses = pulse_own * xs

    w_real, w_imag = steering[0], steering[1]
    weights = jnp.concatenate(
        [jnp.concatenate([w_real, -w_imag], 1), jnp.concatenate([w_imag, w_real], 1)], 0
    )
    dy, dz, gr, cp, it = grid_ids(ys, zs, groups, 2, ROWS)
    bp = gr * ROWS + it
    left = cp * beams + dz * beam_own + bp // part
    left_pulse = dy * part + bp % part
    sz, ci, ch, pi = grid_ids(zs, 2, chan_own, pulse_own)
    right = ci * chans + sz * chan_own + ch
    form = expand(left, left_pulse, weights, right, pi)

    ms = np.arange(m_count)
    angle = 2.0 * np.pi * (np.outer(ms, ms) % m_count) / m_count
    outer_f = jnp.asarray(complex_rows(np.cos(angle), -np.sin(angle)), BF)
    outer_i = jnp.asarray(complex_rows(np.cos(angle), np.sin(angle)), BF)
    mk, mc, mi = grid_ids(m_count, 2, ROWS)
    outer_f = expand(mk * 2 + mc, mi, outer_f, mk * 2 + mc, mi)
    outer_i = expand(mk * 2 + mc, mi, outer_i, mk * 2 + mc, mi)
    ls = np.arange(LANES)
    angle = 2.0 * np.pi * (np.outer(ls, ls) % LANES) / LANES
    co, si = np.cos(angle), np.sin(angle)
    inner_f = jnp.asarray(np.block([[co, -si], [si, co]]), BF)
    inner_i = jnp.asarray(np.block([[co, si], [-si, co]]), BF)
    angle = 2.0 * np.pi * np.outer(ms, ls) / full
    twiddle = jnp.asarray(np.stack([np.cos(angle), -np.sin(angle)]), F32)
    spread = (2, m_count, ROWS, LANES)
    twiddle = jnp.broadcast_to(twiddle[:, :, None, :], spread)
    response = jnp.swapaxes(spectrum.reshape(2, LANES, m_count), 1, 2) * (1.0 / full)
    response = jnp.broadcast_to(response[:, :, None, :], spread)

    samples = lax.all_to_all(signal, "chan", split_axis=3, concat_axis=0, tiled=True)
    samples = samples.reshape(zs * 2 * chan_own * pulse_own, block)
    rows = 2 * beam_own * part
    formed = call(
        form_kernel, jax.ShapeDtypeStruct((ys * zs * rows, block), BF), "form"
    )(form, samples).reshape(ys * zs, rows, block)
    formed = lax.all_to_all(formed, ("range", "chan"), split_axis=0, concat_axis=0, tiled=True)

    blocks = ys * xs
    own = full // blocks
    padded = own + 2 * LANES
    packed = call(
        functools.partial(range_kernel, blocks),
        jax.ShapeDtypeStruct((blocks, rows, padded), BF),
        "compress",
    )(formed, outer_f, outer_i, twiddle, inner_f, inner_i, response)
    columns = lax.all_to_all(packed, ("range", "pulse"), split_axis=0, concat_axis=0, tiled=True)

    src, dst = np.arange(3 * LANES)[:, None] - LANES, np.arange(LANES)[None, :]
    gap = np.abs(src - dst)
    window = jnp.asarray(((gap > GUARD) & (gap <= GUARD + TRAIN)) / (2.0 * TRAIN), BF)

    dr, di = doppler_table(pulses)
    out_shape = jax.ShapeDtypeStruct((pulses * beam_own, own), BF)
    if 2 * pulses * beam_own <= 1024:
        table = jnp.concatenate([jnp.concatenate([dr, -di], 1), jnp.concatenate([di, dr], 1)], 0)
        oc, oq, ob, of = grid_ids(2, xs, beam_own, pulse_own)
        sy, sx, gr, cp, it = grid_ids(ys, xs, groups, 2, ROWS)
        bp = gr * ROWS + it
        pulse = sx * pulse_own + sy * part + bp % part
        mix = expand(oc * pulses + oq * pulse_own + of, ob, table, cp * pulses + pulse, bp // part)
        found = call(cfar_kernel, out_shape, "cfar")(
            mix, columns.reshape(blocks * rows, padded), window
        )
    else:
        v = columns.reshape(ys, xs, groups, 2, ROWS // part, part, padded)
        v = jnp.transpose(v, (3, 2, 4, 1, 0, 5, 6)).reshape(2, beam_own, pulses, padded)

        def product(t, x):
            return jnp.einsum("fp,bpr->fbr", t, x, preferred_element_type=F32)

        re = product(dr, v[0]) - product(di, v[1])
        im = product(dr, v[1]) + product(di, v[0])
        power = (re * re + im * im).reshape(xs, pulse_own, beam_own, padded)
        power = jnp.swapaxes(power, 1, 2).reshape(pulses * beam_own, padded)
        found = call(cfar_only_kernel, out_shape, "cfar")(power, window)
    found = found.reshape(xs, beam_own * pulse_own, own)
    found = lax.all_to_all(found, "pulse", split_axis=0, concat_axis=0, tiled=True)
    out = call(
        place_kernel, jax.ShapeDtypeStruct((beam_own * pulse_own, gates), F32), "place"
    )(found)
    return out.reshape(beam_own, pulse_own, gates)


MESH = pl.DeviceIdType.MESH


def iota(shape, dim):
    return lax.broadcasted_iota(jnp.int32, shape, dim)


def pick(ids, other):
    return (ids == other).astype(F32).astype(BF)


def widen(row_ids, row_tags, table, col_ids, col_tags):
    n, m = table.shape
    r, c = row_ids.shape[0], col_ids.shape[1]
    wide = dot(pick(row_ids, iota((r, n), 1)), table).astype(BF)
    wide = dot(wide, pick(iota((m, c), 0), col_ids))
    return jnp.where(row_tags == col_tags, wide, 0.0).astype(BF)


def chain_kernel(
    sizes, sig, steer_h, spec_h, f_h, fi_h, inf_h, ini_h, tw_h, dop_h, win_h, out,
    steer, spec, f_t, fi_t, inf, ini, tw, dop_t, win,
    own1, recv1, sendp, recvp, acc, send2, recv2, dop, send4, recv4,
    wide_w, wide_f, wide_i, mix, spread, gates_t,
    const_sem, own_sem, s1, r1, sp, rp, s2, r2, s4, r4,
):
    zs, ys, xs, chunks = sizes
    depth, gates = own1.shape
    width = gates // chunks
    beams, chans = steer.shape[1], steer.shape[2]
    count = ys * xs
    beam_rows = send2.shape[1]
    part_rows = send4.shape[2]
    m_count = tw.shape[1]
    z, y, x = (lax.axis_index(a) for a in ("chan", "range", "pulse"))
    me = y * xs + x
    half = lax.div(z, 2)
    hub, edge = 1 + half, 3 * half
    is_hub = z == hub
    is_edge = z == edge

    consts = [
        pltpu.make_async_copy(a, b, const_sem.at[i])
        for i, (a, b) in enumerate(
            zip(
                (steer_h, spec_h, f_h, fi_h, inf_h, ini_h, tw_h, dop_h, win_h),
                (steer, spec, f_t, fi_t, inf, ini, tw, dop_t, win),
            )
        )
    ]

    def lanes(c):
        return pl.ds(pl.multiple_of(c * width, LANES), width)

    def mine(c):
        return pltpu.make_async_copy(
            sig.at[:, lanes(c)], own1.at[:, lanes(c)], own_sem.at[c]
        )

    def loop(body, start=0, stop=chunks):
        def step(c, carry):
            body(c)
            return carry

        lax.fori_loop(start, stop, step, 0)

    for copy in consts:
        copy.start()

    @pl.when(is_hub)
    def _():
        loop(lambda c: mine(c).start())

    def plane(i):
        d = lax.rem(i, count)
        return {
            "chan": jnp.where(i < count, hub, edge),
            "range": lax.div(d, xs),
            "pulse": lax.rem(d, xs),
        }

    both = 2 * count
    me_both = me + jnp.where(is_hub, 0, count)
    barrier = pltpu.get_barrier_semaphore()
    for k in range(1, both):
        pl.semaphore_signal(
            barrier, inc=1, device_id=plane(lax.rem(me_both + k, both)), device_id_type=MESH
        )
    pl.semaphore_signal(barrier, inc=1, device_id={"chan": 3 - z}, device_id_type=MESH)
    pl.semaphore_wait(barrier, both)

    def plan(src, dst, send, recv, target):
        return pltpu.make_async_remote_copy(
            src_ref=src, dst_ref=dst, send_sem=send, recv_sem=recv,
            device_id=target, device_id_type=MESH,
        )

    def raw(c):
        return plan(
            sig.at[:, lanes(c)], recv1.at[:, lanes(c)], s1.at[c], r1.at[c], {"chan": hub}
        )

    @pl.when(is_edge)
    def _():
        loop(lambda c: raw(c).start())

    for copy in consts:
        copy.wait()

    def tables():
        r, c = iota((m_count * 2 * ROWS, 1), 0), iota((1, m_count * 2 * ROWS), 1)
        ids = (lax.div(r, ROWS), lax.rem(r, ROWS)), (lax.div(c, ROWS), lax.rem(c, ROWS))
        wide_f[...] = widen(*ids[0], f_t[...], *ids[1])
        wide_i[...] = widen(*ids[0], fi_t[...], *ids[1])
        for i in range(2):
            spread[i] = jnp.broadcast_to(tw[i][:, None, :], (m_count, ROWS, LANES))
            for t in range(m_count):
                gates_t[i, t : t + 1] = spec[i : i + 1, LANES * t : LANES * t + LANES]
            turned = gates_t[i].T * (1.0 / (m_count * LANES))
            turned = jnp.concatenate([turned[:m_count], turned[m_count:]], axis=1)
            spread[2 + i] = jnp.broadcast_to(turned[:, None, :], (m_count, ROWS, LANES))
        chip, core = lax.div(x, 2), lax.rem(x, 2)
        for i, g in enumerate(order):
            mix[beam_rows * i : beam_rows * i + beam_rows] = dop_t[
                pl.ds(pl.multiple_of(beam_rows * g, beam_rows), beam_rows)
            ]

    chip, core = lax.div(x, 2), lax.rem(x, 2)
    order = [2 * (1 - chip), 2 * (1 - chip) + 1, 2 * chip + 1 - core, x]

    def doppler(c):
        for i in range(ys):
            dop[i, :, lanes(c)] = dot(mix[...], recv2[i, :, lanes(c)]).astype(BF)

    @pl.when(is_hub)
    def _():
        re, im = steer[0], steer[1]
        weights = jnp.concatenate(
            [jnp.concatenate([re, -im], 1), jnp.concatenate([im, re], 1)], 0
        )
        pulse_own = beam_rows // 2
        chan_own = chans // zs
        r = iota((both * beam_rows, 1), 0)
        c = iota((1, depth), 1)
        row_tag, col_tag = lax.rem(r, pulse_own), lax.rem(c, pulse_own)
        r, c = lax.div(r, pulse_own), lax.div(c, pulse_own)
        dest = lax.div(r, 2)
        for i, h in enumerate((half, 1 - half)):
            at = jnp.where(dest < count, 1 + h, 3 * h)
            row = lax.rem(r, 2) * beams + at * count + lax.rem(dest, count)
            for j, source in enumerate((hub, edge)):
                col = lax.div(c, chan_own) * chans + source * chan_own + lax.rem(c, chan_own)
                wide_w[i, j] = widen(row, row_tag, weights, col, col_tag)

        def swap(c):
            return plan(
                sendp.at[:, lanes(c)], recvp.at[:, lanes(c)], sp.at[c], rp.at[c],
                {"chan": 3 - hub},
            )

        def form(c):
            mine(c).wait()
            raw(c).wait_recv()
            a, b = own1[:, lanes(c)], recv1[:, lanes(c)]
            sendp[:, lanes(c)] = (dot(wide_w[1, 0], a) + dot(wide_w[1, 1], b)).astype(BF)
            swap(c).start()
            acc[:, lanes(c)] = dot(wide_w[0, 0], a) + dot(wide_w[0, 1], b)

        def finish(c):
            swap(c).wait_recv()
            total = (acc[:, lanes(c)] + recvp[:, lanes(c)].astype(F32)).astype(BF)
            send2[:, :, lanes(c)] = total.reshape(both, beam_rows, width)
            mine_rows = pl.ds(pl.multiple_of(beam_rows * x, beam_rows), beam_rows)
            for k in range(1, both):
                to = lax.rem(me + k, both)
                plan(
                    send2.at[to, :, lanes(c)], recv2.at[y, mine_rows, lanes(c)],
                    s2.at[c], r2.at[c], plane(to),
                ).start()
            recv2[y, mine_rows, lanes(c)] = send2[me, :, lanes(c)]

        def arrived(c):
            plan(
                send2.at[pl.ds(0, count - 1), :, lanes(c)],
                send2.at[pl.ds(0, count - 1), :, lanes(c)],
                s2.at[c], r2.at[c], {"chan": edge},
            ).wait_recv()

        def body(c):
            form(c)

            @pl.when(c == 0)
            def _():
                tables()

            @pl.when(c >= 1)
            def _():
                finish(c - 1)

            @pl.when(c >= 3)
            def _():
                arrived(c - 3)
                doppler(c - 3)

        loop(body)
        finish(chunks - 1)

        def rest(c):
            arrived(c)
            doppler(c)

        loop(rest, chunks - 3)

    @pl.when(is_edge)
    def _():
        tables()

        def body(c):
            plan(
                send2.at[pl.ds(0, count), :, lanes(c)],
                send2.at[pl.ds(0, count), :, lanes(c)],
                s2.at[c], r2.at[c], {"chan": hub},
            ).wait_recv()
            doppler(c)

        loop(body)

    tr, ti = spread[0], spread[1]
    hr, hi = spread[2], spread[3]
    fourth = []
    for q in range(xs // 2):
        tile = []
        for j in range(2):
            rows = slice(beam_rows * (2 * q + j), beam_rows * (2 * q + j + 1))
            parts = [
                dop[i, rows, LANES * t : LANES * t + LANES]
                for i in range(ys)
                for t in range(gates // LANES)
            ]
            tile.append(jnp.concatenate(parts, axis=0))
        outer = dot(wide_f[...], jnp.concatenate(tile, axis=1))
        back = []
        for j in range(2):
            a = outer[:, LANES * j : LANES * j + LANES].reshape(m_count, 2, ROWS, LANES)
            ar, ai = a[:, 0], a[:, 1]
            b = jnp.concatenate([ar * tr - ai * ti, ar * ti + ai * tr], axis=-1)
            c = dot(b.reshape(m_count * ROWS, 2 * LANES).astype(BF), inf[...])
            c = c.reshape(m_count, ROWS, 2 * LANES)
            cr, ci = c[..., :LANES], c[..., LANES:]
            d = jnp.concatenate([cr * hr - ci * hi, cr * hi + ci * hr], axis=-1)
            e = dot(d.reshape(m_count * ROWS, 2 * LANES).astype(BF), ini[...])
            e = e.reshape(m_count, ROWS, 2 * LANES)
            er, ei = e[..., :LANES], e[..., LANES:]
            f = jnp.stack([er * tr + ei * ti, ei * tr - er * ti], axis=1)
            back.append(f.reshape(m_count * 2 * ROWS, LANES).astype(BF))
        final = dot(wide_i[...], jnp.concatenate(back, axis=1))
        for j in range(2):
            v = final[:, LANES * j : LANES * j + LANES].reshape(m_count, 2, ROWS, LANES)
            re, im = v[:, 0], v[:, 1]
            power = (re * re + im * im).reshape(m_count * ROWS, LANES)
            none = jnp.zeros((ROWS, LANES), F32)
            before = jnp.concatenate([none, power[:-ROWS]], axis=0)
            after = jnp.concatenate([power[ROWS:], none], axis=0)
            near = jnp.concatenate([before, power, after], axis=1).astype(BF)
            found = power / (dot(near, win[...]) + NOISE_FLOOR)
            p = 2 * q + j
            send4[p] = found.astype(BF).reshape(send4.shape[1:])
            for k in range(ys):
                if p == xs - 1 and k == 0:
                    recv4[me] = send4[p, y]
                    continue
                to_y = lax.rem(y + k, ys)
                copy = plan(
                    send4.at[p, to_y], recv4.at[me], s4.at[p, k], r4.at[me],
                    {"range": to_y, "pulse": order[p]},
                )
                copy.start()
                fourth.append(copy)

    def place(i):
        for t in range(part_rows // ROWS):
            out[i, :, LANES * t : LANES * t + LANES] = recv4[
                i, ROWS * t : ROWS * t + ROWS
            ].astype(F32)

    def final_step(k, carry):
        i = lax.rem(me + k, count)

        @pl.when(k > 0)
        def _():
            plan(
                send4.at[0, 0], recv4.at[i], s4.at[0, 0], r4.at[i], {"chan": 3 - z}
            ).wait_recv()

        place(i)
        return carry

    lax.fori_loop(0, count, final_step, 0)
    for copy in fourth:
        copy.wait_send()

    @pl.when(is_edge)
    def _():
        loop(lambda c: raw(c).wait_send())

    @pl.when(is_hub)
    def _():
        def body(c):
            plan(
                sendp.at[:, lanes(c)], recvp.at[:, lanes(c)], sp.at[c], rp.at[c],
                {"chan": 3 - hub},
            ).wait_send()
            plan(
                send2.at[pl.ds(0, both - 1), :, lanes(c)],
                send2.at[pl.ds(0, both - 1), :, lanes(c)],
                s2.at[c], r2.at[c], {"chan": edge},
            ).wait_send()

        loop(body)


def shards_chain(signal, steering, spectrum):
    beams, chans = steering.shape[1], steering.shape[2]
    _, chan_own, pulse_own, gates = signal.shape
    zs, xs, ys = (lax.axis_size(a) for a in ("chan", "pulse", "range"))
    count = xs * ys
    full = gates * ys
    m_count = full // LANES
    pulses = pulse_own * xs
    depth = 2 * chan_own * pulse_own
    chunks = CHUNKS

    ms = np.arange(m_count)
    angle = 2.0 * np.pi * (np.outer(ms, ms) % m_count) / m_count
    outer_f = jnp.asarray(complex_rows(np.cos(angle), -np.sin(angle)), BF)
    outer_i = jnp.asarray(complex_rows(np.cos(angle), np.sin(angle)), BF)
    ls = np.arange(LANES)
    times = LANES // m_count
    bins = (ls % m_count) * times + ls // m_count
    angle = 2.0 * np.pi * (np.outer(ls, bins) % LANES) / LANES
    co, si = np.cos(angle), np.sin(angle)
    inner_f = jnp.asarray(np.block([[co, -si], [si, co]]), BF)
    inner_i = jnp.asarray(np.block([[co.T, si.T], [-si.T, co.T]]), BF)
    angle = 2.0 * np.pi * np.outer(ms, ls) / full
    twiddle = jnp.asarray(np.stack([np.cos(angle), -np.sin(angle)]), F32)

    src, dst = np.arange(3 * LANES)[:, None] - LANES, np.arange(LANES)[None, :]
    gap = np.abs(src - dst)
    window = jnp.asarray(((gap > GUARD) & (gap <= GUARD + TRAIN)) / (2.0 * TRAIN), BF)

    ids = np.arange(pulses)
    angle = (np.outer(ids, ids) % pulses) * (2.0 * np.pi / pulses)
    scale = 1.0 / math.sqrt(pulses)
    dr, di = np.cos(angle) * scale, -np.sin(angle) * scale
    table = np.stack([np.stack([dr, -di], -1), np.stack([di, dr], -1)])
    table = table.reshape(2, xs, pulse_own, xs, pulse_own, 2)
    table = table.transpose(1, 0, 2, 3, 5, 4).reshape(2 * pulses, 2 * pulses)
    table = jnp.asarray(table, BF)

    beam_rows = 2 * pulse_own
    vmem, dma = pltpu.VMEM, pltpu.SemaphoreType.DMA
    any_space = pl.BlockSpec(memory_space=pl.ANY)
    consts = (steering, spectrum, outer_f, outer_i, inner_f, inner_i, twiddle, table, window)
    return pl.pallas_call(
        functools.partial(chain_kernel, (zs, ys, xs, chunks)),
        out_shape=jax.ShapeDtypeStruct((count, pulse_own, gates), F32),
        in_specs=[any_space] * (1 + len(consts)),
        out_specs=pl.BlockSpec(memory_space=vmem),
        scratch_shapes=[vmem(a.shape, a.dtype) for a in consts]
        + [
            vmem((depth, gates), BF),
            vmem((depth, gates), BF),
            vmem((2 * count * beam_rows, gates), BF),
            vmem((2 * count * beam_rows, gates), BF),
            vmem((2 * count * beam_rows, gates), F32),
            vmem((2 * count, beam_rows, gates), BF),
            vmem((ys, xs * beam_rows, gates), BF),
            vmem((ys, xs * beam_rows, gates), BF),
            vmem((xs, ys, gates // LANES * pulse_own, LANES), BF),
            vmem((count, gates // LANES * pulse_own, LANES), BF),
            vmem((2, 2, 2 * count * beam_rows, depth), BF),
            vmem((m_count * 2 * ROWS, m_count * 2 * ROWS), BF),
            vmem((m_count * 2 * ROWS, m_count * 2 * ROWS), BF),
            vmem((2 * pulses, 2 * pulses), BF),
            vmem((4, m_count, ROWS, LANES), F32),
            vmem((2, m_count, LANES), F32),
            dma((len(consts),)),
            dma((chunks,)),
            dma((chunks,)), dma((chunks,)),
            dma((chunks,)), dma((chunks,)),
            dma((chunks,)), dma((chunks,)),
            dma((xs, ys)), dma((count,)),
        ],
        compiler_params=pltpu.CompilerParams(
            collective_id=0, has_side_effects=True, vmem_limit_bytes=VM
        ),
        name="chain",
    )(signal.reshape(depth, gates), *consts)


def shards(signal, steering, spectrum):
    zs, xs, ys = (lax.axis_size(a) for a in ("chan", "pulse", "range"))
    _, _, pulse_own, gates = signal.shape
    fits = (
        zs == 4
        and xs == 4
        and pulse_own == ROWS
        and steering.shape[1] == zs * xs * ys
        and gates * ys * 2 == LANES * LANES
        and gates % (CHUNKS * LANES) == 0
    )
    return (shards_chain if fits else shards_split)(signal, steering, spectrum)


def solution(mesh):
    in_specs = (P(None, "chan", "pulse", "range"), P(), P())
    out_specs = P("chan", "pulse", "range")
    return jax.shard_map(shards, mesh=mesh, in_specs=in_specs, out_specs=out_specs, check_vma=False)
```

```python
import functools
import math

import jax
import jax.numpy as jnp
import numpy as np
from jax import lax
from jax.experimental import pallas as pl
from jax.experimental.pallas import tpu as pltpu
from jax.sharding import PartitionSpec as P

GUARD = 4
TRAIN = 16
NOISE_FLOOR = 0.25
LANES = 128
ROWS = 8
CHUNKS = 16
GROUP = 1
LAG = 2
BF = jnp.bfloat16
F32 = jnp.float32
VM = 44 * 1024 * 1024


def dot(a, b):
    return jnp.dot(a, b, preferred_element_type=F32)


def doppler_table(count):
    ids = np.arange(count)
    angle = (np.outer(ids, ids) % count) * (2.0 * np.pi / count)
    scale = 1.0 / math.sqrt(count)
    return jnp.asarray(np.cos(angle) * scale, BF), jnp.asarray(-np.sin(angle) * scale, BF)


def expand(left_ids, left_tag, table, right_ids, right_tag):
    n, m = table.shape
    left = (jnp.asarray(left_ids, jnp.int32)[:, None] == jnp.arange(n)[None, :]).astype(BF)
    right = (jnp.arange(m)[:, None] == jnp.asarray(right_ids, jnp.int32)[None, :]).astype(BF)
    wide = dot(dot(left, table).astype(BF), right)
    same = jnp.asarray(left_tag, jnp.int32)[:, None] == jnp.asarray(right_tag, jnp.int32)[None, :]
    return jnp.where(same, wide, 0.0).astype(BF)


def grid_ids(*sizes):
    return [g.reshape(-1) for g in np.meshgrid(*[np.arange(s) for s in sizes], indexing="ij")]


def call(body, out_shape, name):
    return pl.pallas_call(
        body,
        out_shape=out_shape,
        compiler_params=pltpu.CompilerParams(vmem_limit_bytes=VM),
        name=name,
    )


def form_kernel(w_ref, x_ref, o_ref):
    o_ref[...] = dot(w_ref[...], x_ref[...]).astype(BF)


def range_kernel(blocks, x_ref, f_ref, fi_ref, t_ref, l_ref, li_ref, h_ref, o_ref):
    sources, rows, width = x_ref.shape
    per = width // LANES
    groups = rows // 16
    m_count = sources * per
    tile = []
    for g in range(groups):
        parts = [
            x_ref[s, 16 * g : 16 * g + 16, LANES * j : LANES * j + LANES]
            for s in range(sources)
            for j in range(per)
        ]
        tile.append(jnp.concatenate(parts, axis=0))
    outer = dot(f_ref[...], jnp.concatenate(tile, axis=1))
    tr, ti = t_ref[0], t_ref[1]
    hr, hi = h_ref[0], h_ref[1]
    back = []
    for g in range(groups):
        a = outer[:, LANES * g : LANES * g + LANES].reshape(m_count, 2, ROWS, LANES)
        ar, ai = a[:, 0], a[:, 1]
        b = jnp.concatenate([ar * tr - ai * ti, ar * ti + ai * tr], axis=-1)
        c = dot(b.reshape(m_count * ROWS, 2 * LANES).astype(BF), l_ref[...])
        c = c.reshape(m_count, ROWS, 2 * LANES)
        cr, ci = c[..., :LANES], c[..., LANES:]
        d = jnp.concatenate([cr * hr - ci * hi, cr * hi + ci * hr], axis=-1)
        e = dot(d.reshape(m_count * ROWS, 2 * LANES).astype(BF), li_ref[...])
        e = e.reshape(m_count, ROWS, 2 * LANES)
        er, ei = e[..., :LANES], e[..., LANES:]
        f = jnp.stack([er * tr + ei * ti, ei * tr - er * ti], axis=1)
        back.append(f.reshape(m_count * 16, LANES).astype(BF))
    y = dot(fi_ref[...], jnp.concatenate(back, axis=1)).astype(BF)
    span = m_count // blocks
    for d in range(blocks):
        for j in range(-1, span + 1):
            m = d * span + j
            for g in range(groups):
                if 0 <= m < m_count:
                    v = y[16 * m : 16 * m + 16, LANES * g : LANES * g + LANES]
                else:
                    v = jnp.zeros((16, LANES), BF)
                o_ref[d, 16 * g : 16 * g + 16, LANES * (j + 1) : LANES * (j + 2)] = v


def cfar_kernel(d_ref, x_ref, n_ref, o_ref):
    half = d_ref.shape[0] // 2
    mix = dot(d_ref[...], x_ref[...].reshape(d_ref.shape[1], x_ref.shape[-1]))
    re, im = mix[:half], mix[half:]
    power = re * re + im * im
    narrow = power.astype(BF)
    shape = o_ref.shape[:-1] + (LANES,)
    for j in range(o_ref.shape[-1] // LANES):
        noise = dot(narrow[:, LANES * j : LANES * (j + 3)], n_ref[...])
        own = power[:, LANES * (j + 1) : LANES * (j + 2)]
        found = (own / (noise + NOISE_FLOOR)).astype(BF)
        o_ref[..., LANES * j : LANES * j + LANES] = found.reshape(shape)


def cfar_only_kernel(p_ref, n_ref, o_ref):
    narrow = p_ref[...].astype(BF)
    for j in range(o_ref.shape[1] // LANES):
        noise = dot(narrow[:, LANES * j : LANES * (j + 3)], n_ref[...])
        own = p_ref[:, LANES * (j + 1) : LANES * (j + 2)]
        o_ref[:, LANES * j : LANES * j + LANES] = (own / (noise + NOISE_FLOOR)).astype(BF)


def place_kernel(x_ref, o_ref):
    count, _, width = x_ref.shape
    for s in range(count):
        o_ref[:, width * s : width * s + width] = x_ref[s].astype(F32)


def complex_rows(re, im):
    top = np.stack([re, -im], -1)
    low = np.stack([im, re], -1)
    return np.stack([top, low], 1).reshape(2 * re.shape[0], 2 * re.shape[1])


def shards_split(signal, steering, spectrum):
    beams, chans = steering.shape[1], steering.shape[2]
    _, chan_own, pulse_own, gates = signal.shape
    zs, xs, ys = (lax.axis_size(a) for a in ("chan", "pulse", "range"))
    beam_own = beams // zs
    part = pulse_own // ys
    full = gates * ys
    block = gates // zs
    m_count = full // LANES
    groups = beam_own * part // ROWS
    pulses = pulse_own * xs

    w_real, w_imag = steering[0], steering[1]
    weights = jnp.concatenate(
        [jnp.concatenate([w_real, -w_imag], 1), jnp.concatenate([w_imag, w_real], 1)], 0
    )
    dy, dz, gr, cp, it = grid_ids(ys, zs, groups, 2, ROWS)
    bp = gr * ROWS + it
    left = cp * beams + dz * beam_own + bp // part
    left_pulse = dy * part + bp % part
    sz, ci, ch, pi = grid_ids(zs, 2, chan_own, pulse_own)
    right = ci * chans + sz * chan_own + ch
    form = expand(left, left_pulse, weights, right, pi)

    ms = np.arange(m_count)
    angle = 2.0 * np.pi * (np.outer(ms, ms) % m_count) / m_count
    outer_f = jnp.asarray(complex_rows(np.cos(angle), -np.sin(angle)), BF)
    outer_i = jnp.asarray(complex_rows(np.cos(angle), np.sin(angle)), BF)
    mk, mc, mi = grid_ids(m_count, 2, ROWS)
    outer_f = expand(mk * 2 + mc, mi, outer_f, mk * 2 + mc, mi)
    outer_i = expand(mk * 2 + mc, mi, outer_i, mk * 2 + mc, mi)
    ls = np.arange(LANES)
    angle = 2.0 * np.pi * (np.outer(ls, ls) % LANES) / LANES
    co, si = np.cos(angle), np.sin(angle)
    inner_f = jnp.asarray(np.block([[co, -si], [si, co]]), BF)
    inner_i = jnp.asarray(np.block([[co, si], [-si, co]]), BF)
    angle = 2.0 * np.pi * np.outer(ms, ls) / full
    twiddle = jnp.asarray(np.stack([np.cos(angle), -np.sin(angle)]), F32)
    spread = (2, m_count, ROWS, LANES)
    twiddle = jnp.broadcast_to(twiddle[:, :, None, :], spread)
    response = jnp.swapaxes(spectrum.reshape(2, LANES, m_count), 1, 2) * (1.0 / full)
    response = jnp.broadcast_to(response[:, :, None, :], spread)

    samples = lax.all_to_all(signal, "chan", split_axis=3, concat_axis=0, tiled=True)
    samples = samples.reshape(zs * 2 * chan_own * pulse_own, block)
    rows = 2 * beam_own * part
    formed = call(
        form_kernel, jax.ShapeDtypeStruct((ys * zs * rows, block), BF), "form"
    )(form, samples).reshape(ys * zs, rows, block)
    formed = lax.all_to_all(formed, ("range", "chan"), split_axis=0, concat_axis=0, tiled=True)

    blocks = ys * xs
    own = full // blocks
    padded = own + 2 * LANES
    packed = call(
        functools.partial(range_kernel, blocks),
        jax.ShapeDtypeStruct((blocks, rows, padded), BF),
        "compress",
    )(formed, outer_f, outer_i, twiddle, inner_f, inner_i, response)
    columns = lax.all_to_all(packed, ("range", "pulse"), split_axis=0, concat_axis=0, tiled=True)

    src, dst = np.arange(3 * LANES)[:, None] - LANES, np.arange(LANES)[None, :]
    gap = np.abs(src - dst)
    window = jnp.asarray(((gap > GUARD) & (gap <= GUARD + TRAIN)) / (2.0 * TRAIN), BF)

    dr, di = doppler_table(pulses)
    out_shape = jax.ShapeDtypeStruct((pulses * beam_own, own), BF)
    if 2 * pulses * beam_own <= 1024:
        table = jnp.concatenate([jnp.concatenate([dr, -di], 1), jnp.concatenate([di, dr], 1)], 0)
        oc, oq, ob, of = grid_ids(2, xs, beam_own, pulse_own)
        sy, sx, gr, cp, it = grid_ids(ys, xs, groups, 2, ROWS)
        bp = gr * ROWS + it
        pulse = sx * pulse_own + sy * part + bp % part
        mix = expand(oc * pulses + oq * pulse_own + of, ob, table, cp * pulses + pulse, bp // part)
        found = call(cfar_kernel, out_shape, "cfar")(
            mix, columns.reshape(blocks * rows, padded), window
        )
    else:
        v = columns.reshape(ys, xs, groups, 2, ROWS // part, part, padded)
        v = jnp.transpose(v, (3, 2, 4, 1, 0, 5, 6)).reshape(2, beam_own, pulses, padded)

        def product(t, x):
            return jnp.einsum("fp,bpr->fbr", t, x, preferred_element_type=F32)

        re = product(dr, v[0]) - product(di, v[1])
        im = product(dr, v[1]) + product(di, v[0])
        power = (re * re + im * im).reshape(xs, pulse_own, beam_own, padded)
        power = jnp.swapaxes(power, 1, 2).reshape(pulses * beam_own, padded)
        found = call(cfar_only_kernel, out_shape, "cfar")(power, window)
    found = found.reshape(xs, beam_own * pulse_own, own)
    found = lax.all_to_all(found, "pulse", split_axis=0, concat_axis=0, tiled=True)
    out = call(
        place_kernel, jax.ShapeDtypeStruct((beam_own * pulse_own, gates), F32), "place"
    )(found)
    return out.reshape(beam_own, pulse_own, gates)


MESH = pl.DeviceIdType.MESH


def iota(shape, dim):
    return lax.broadcasted_iota(jnp.int32, shape, dim)


def pick(ids, other):
    return (ids == other).astype(F32).astype(BF)


def widen(row_ids, row_tags, table, col_ids, col_tags):
    n, m = table.shape
    r, c = row_ids.shape[0], col_ids.shape[1]
    wide = dot(pick(row_ids, iota((r, n), 1)), table).astype(BF)
    wide = dot(wide, pick(iota((m, c), 0), col_ids))
    return jnp.where(row_tags == col_tags, wide, 0.0).astype(BF)


def chain_kernel(
    sizes, sig, steer_h, spec_h, f_h, fi_h, inf_h, ini_h, tw_h, dop_h, win_h, out,
    steer, spec, f_t, fi_t, inf, ini, tw, dop_t, win,
    own1, recv1, sendp, recvp, acc, send2, recv2, dop, send4, recv4,
    wide_w, wide_f, wide_i, mix, spread, gates_t,
    const_sem, own_sem, s1, r1, sp, rp, s2, r2, s4, r4,
):
    zs, ys, xs, chunks = sizes
    depth, gates = own1.shape
    width = gates // chunks
    beams, chans = steer.shape[1], steer.shape[2]
    count = ys * xs
    beam_rows = send2.shape[1]
    part_rows = send4.shape[2]
    m_count = tw.shape[1]
    z, y, x = (lax.axis_index(a) for a in ("chan", "range", "pulse"))
    me = y * xs + x
    half = lax.div(z, 2)
    hub, edge = 1 + half, 3 * half
    is_hub = z == hub
    is_edge = z == edge

    consts = [
        pltpu.make_async_copy(a, b, const_sem.at[i])
        for i, (a, b) in enumerate(
            zip(
                (steer_h, spec_h, f_h, fi_h, inf_h, ini_h, tw_h, dop_h, win_h),
                (steer, spec, f_t, fi_t, inf, ini, tw, dop_t, win),
            )
        )
    ]

    def lanes(c):
        return pl.ds(pl.multiple_of(c * width, LANES), width)

    def wide_lanes(c):
        return pl.ds(pl.multiple_of(c * width * GROUP, LANES), width * GROUP)

    def mine(c):
        return pltpu.make_async_copy(
            sig.at[:, lanes(c)], own1.at[:, lanes(c)], own_sem.at[c]
        )

    def loop(body, start=0, stop=chunks):
        def step(c, carry):
            body(c)
            return carry

        lax.fori_loop(start, stop, step, 0)

    for copy in consts:
        copy.start()

    @pl.when(is_hub)
    def _():
        loop(lambda c: mine(c).start())

    def plane(i):
        d = lax.rem(i, count)
        return {
            "chan": jnp.where(i < count, hub, edge),
            "range": lax.div(d, xs),
            "pulse": lax.rem(d, xs),
        }

    both = 2 * count
    me_both = me + jnp.where(is_hub, 0, count)
    barrier = pltpu.get_barrier_semaphore()
    for k in range(1, both):
        pl.semaphore_signal(
            barrier, inc=1, device_id=plane(lax.rem(me_both + k, both)), device_id_type=MESH
        )
    pl.semaphore_signal(barrier, inc=1, device_id={"chan": 3 - z}, device_id_type=MESH)
    pl.semaphore_wait(barrier, both)

    def plan(src, dst, send, recv, target):
        return pltpu.make_async_remote_copy(
            src_ref=src, dst_ref=dst, send_sem=send, recv_sem=recv,
            device_id=target, device_id_type=MESH,
        )

    def raw(c):
        return plan(
            sig.at[:, lanes(c)], recv1.at[:, lanes(c)], s1.at[c], r1.at[c], {"chan": hub}
        )

    @pl.when(is_edge)
    def _():
        loop(lambda c: raw(c).start())

    for copy in consts:
        copy.wait()

    def tables():
        r, c = iota((m_count * 2 * ROWS, 1), 0), iota((1, m_count * 2 * ROWS), 1)
        ids = (lax.div(r, ROWS), lax.rem(r, ROWS)), (lax.div(c, ROWS), lax.rem(c, ROWS))
        wide_f[...] = widen(*ids[0], f_t[...], *ids[1])
        wide_i[...] = widen(*ids[0], fi_t[...], *ids[1])
        for i in range(2):
            spread[i] = jnp.broadcast_to(tw[i][:, None, :], (m_count, ROWS, LANES))
            for t in range(m_count):
                gates_t[i, t : t + 1] = spec[i : i + 1, LANES * t : LANES * t + LANES]
            turned = gates_t[i].T * (1.0 / (m_count * LANES))
            turned = jnp.concatenate([turned[:m_count], turned[m_count:]], axis=1)
            spread[2 + i] = jnp.broadcast_to(turned[:, None, :], (m_count, ROWS, LANES))
        chip, core = lax.div(x, 2), lax.rem(x, 2)
        for i, g in enumerate(order):
            mix[beam_rows * i : beam_rows * i + beam_rows] = dop_t[
                pl.ds(pl.multiple_of(beam_rows * g, beam_rows), beam_rows)
            ]

    chip, core = lax.div(x, 2), lax.rem(x, 2)
    order = [2 * (1 - chip), 2 * (1 - chip) + 1, 2 * chip + 1 - core, x]

    def doppler(c):
        for i in range(ys):
            dop[i, :, wide_lanes(c)] = dot(mix[...], recv2[i, :, wide_lanes(c)]).astype(BF)

    @pl.when(is_hub)
    def _():
        re, im = steer[0], steer[1]
        weights = jnp.concatenate(
            [jnp.concatenate([re, -im], 1), jnp.concatenate([im, re], 1)], 0
        )
        pulse_own = beam_rows // 2
        chan_own = chans // zs
        r = iota((both * beam_rows, 1), 0)
        c = iota((1, depth), 1)
        row_tag, col_tag = lax.rem(r, pulse_own), lax.rem(c, pulse_own)
        r, c = lax.div(r, pulse_own), lax.div(c, pulse_own)
        dest = lax.div(r, 2)
        for i, h in enumerate((half, 1 - half)):
            at = jnp.where(dest < count, 1 + h, 3 * h)
            row = lax.rem(r, 2) * beams + at * count + lax.rem(dest, count)
            for j, source in enumerate((hub, edge)):
                col = lax.div(c, chan_own) * chans + source * chan_own + lax.rem(c, chan_own)
                wide_w[i, j] = widen(row, row_tag, weights, col, col_tag)

        def swap(c):
            return plan(
                sendp.at[:, lanes(c)], recvp.at[:, lanes(c)], sp.at[c], rp.at[c],
                {"chan": 3 - hub},
            )

        def form(c):
            mine(c).wait()
            raw(c).wait_recv()
            a, b = own1[:, lanes(c)], recv1[:, lanes(c)]
            sendp[:, lanes(c)] = (dot(wide_w[1, 0], a) + dot(wide_w[1, 1], b)).astype(BF)
            swap(c).start()
            acc[:, lanes(c)] = dot(wide_w[0, 0], a) + dot(wide_w[0, 1], b)

        def finish(c):
            swap(c).wait_recv()
            total = (acc[:, lanes(c)] + recvp[:, lanes(c)].astype(F32)).astype(BF)
            send2[:, :, lanes(c)] = total.reshape(both, beam_rows, width)

        def spray(c):
            mine_rows = pl.ds(pl.multiple_of(beam_rows * x, beam_rows), beam_rows)
            for k in range(1, both):
                to = lax.rem(me + k, both)
                plan(
                    send2.at[to, :, wide_lanes(c)], recv2.at[y, mine_rows, wide_lanes(c)],
                    s2.at[c], r2.at[c], plane(to),
                ).start()
            recv2[y, mine_rows, wide_lanes(c)] = send2[me, :, wide_lanes(c)]

        def arrived(c):
            plan(
                send2.at[pl.ds(0, count - 1), :, wide_lanes(c)],
                send2.at[pl.ds(0, count - 1), :, wide_lanes(c)],
                s2.at[c], r2.at[c], {"chan": edge},
            ).wait_recv()

        def body(c):
            form(c)

            @pl.when(c == 0)
            def _():
                tables()

            @pl.when(c >= LAG)
            def _():
                step(c - LAG)

        def step(c):
            finish(c)

            @pl.when(lax.rem(c, GROUP) == GROUP - 1)
            def _():
                g = lax.div(c, GROUP)
                spray(g)

                @pl.when(g >= 3)
                def _():
                    arrived(g - 3)
                    doppler(g - 3)

        loop(body)
        loop(step, chunks - LAG)

        def rest(c):
            arrived(c)
            doppler(c)

        loop(rest, chunks // GROUP - 3, chunks // GROUP)

    @pl.when(is_edge)
    def _():
        tables()

        def body(c):
            plan(
                send2.at[pl.ds(0, count), :, wide_lanes(c)],
                send2.at[pl.ds(0, count), :, wide_lanes(c)],
                s2.at[c], r2.at[c], {"chan": hub},
            ).wait_recv()
            doppler(c)

        loop(body, 0, chunks // GROUP)

    tr, ti = spread[0], spread[1]
    hr, hi = spread[2], spread[3]
    fourth = []
    for q in range(xs // 2):
        tile = []
        for j in range(2):
            rows = slice(beam_rows * (2 * q + j), beam_rows * (2 * q + j + 1))
            parts = [
                dop[i, rows, LANES * t : LANES * t + LANES]
                for i in range(ys)
                for t in range(gates // LANES)
            ]
            tile.append(jnp.concatenate(parts, axis=0))
        outer = dot(wide_f[...], jnp.concatenate(tile, axis=1))
        back = []
        for j in range(2):
            a = outer[:, LANES * j : LANES * j + LANES].reshape(m_count, 2, ROWS, LANES)
            ar, ai = a[:, 0], a[:, 1]
            b = jnp.concatenate([ar * tr - ai * ti, ar * ti + ai * tr], axis=-1)
            c = dot(b.reshape(m_count * ROWS, 2 * LANES).astype(BF), inf[...])
            c = c.reshape(m_count, ROWS, 2 * LANES)
            cr, ci = c[..., :LANES], c[..., LANES:]
            d = jnp.concatenate([cr * hr - ci * hi, cr * hi + ci * hr], axis=-1)
            e = dot(d.reshape(m_count * ROWS, 2 * LANES).astype(BF), ini[...])
            e = e.reshape(m_count, ROWS, 2 * LANES)
            er, ei = e[..., :LANES], e[..., LANES:]
            f = jnp.stack([er * tr + ei * ti, ei * tr - er * ti], axis=1)
            back.append(f.reshape(m_count * 2 * ROWS, LANES).astype(BF))
        final = dot(wide_i[...], jnp.concatenate(back, axis=1))
        for j in range(2):
            v = final[:, LANES * j : LANES * j + LANES].reshape(m_count, 2, ROWS, LANES)
            re, im = v[:, 0], v[:, 1]
            power = (re * re + im * im).reshape(m_count * ROWS, LANES)
            none = jnp.zeros((ROWS, LANES), F32)
            before = jnp.concatenate([none, power[:-ROWS]], axis=0)
            after = jnp.concatenate([power[ROWS:], none], axis=0)
            near = jnp.concatenate([before, power, after], axis=1).astype(BF)
            found = power / (dot(near, win[...]) + NOISE_FLOOR)
            p = 2 * q + j
            send4[p] = found.astype(BF).reshape(send4.shape[1:])
            for k in range(ys):
                if p == xs - 1 and k == 0:
                    recv4[me] = send4[p, y]
                    continue
                to_y = lax.rem(y + k, ys)
                copy = plan(
                    send4.at[p, to_y], recv4.at[me], s4.at[p, k], r4.at[me],
                    {"range": to_y, "pulse": order[p]},
                )
                copy.start()
                fourth.append(copy)

    def place(i):
        for t in range(part_rows // ROWS):
            out[i, :, LANES * t : LANES * t + LANES] = recv4[
                i, ROWS * t : ROWS * t + ROWS
            ].astype(F32)

    def final_step(k, carry):
        i = lax.rem(me + k, count)

        @pl.when(k > 0)
        def _():
            plan(
                send4.at[0, 0], recv4.at[i], s4.at[0, 0], r4.at[i], {"chan": 3 - z}
            ).wait_recv()

        place(i)
        return carry

    lax.fori_loop(0, count, final_step, 0)
    for copy in fourth:
        copy.wait_send()

    @pl.when(is_edge)
    def _():
        loop(lambda c: raw(c).wait_send())

    @pl.when(is_hub)
    def _():
        def body(c):
            plan(
                sendp.at[:, lanes(c)], recvp.at[:, lanes(c)], sp.at[c], rp.at[c],
                {"chan": 3 - hub},
            ).wait_send()

        loop(body)

        def sprayed(c):
            plan(
                send2.at[pl.ds(0, both - 1), :, wide_lanes(c)],
                send2.at[pl.ds(0, both - 1), :, wide_lanes(c)],
                s2.at[c], r2.at[c], {"chan": edge},
            ).wait_send()

        loop(sprayed, 0, chunks // GROUP)


def shards_chain(signal, steering, spectrum):
    beams, chans = steering.shape[1], steering.shape[2]
    _, chan_own, pulse_own, gates = signal.shape
    zs, xs, ys = (lax.axis_size(a) for a in ("chan", "pulse", "range"))
    count = xs * ys
    full = gates * ys
    m_count = full // LANES
    pulses = pulse_own * xs
    depth = 2 * chan_own * pulse_own
    chunks = CHUNKS

    ms = np.arange(m_count)
    angle = 2.0 * np.pi * (np.outer(ms, ms) % m_count) / m_count
    outer_f = jnp.asarray(complex_rows(np.cos(angle), -np.sin(angle)), BF)
    outer_i = jnp.asarray(complex_rows(np.cos(angle), np.sin(angle)), BF)
    ls = np.arange(LANES)
    times = LANES // m_count
    bins = (ls % m_count) * times + ls // m_count
    angle = 2.0 * np.pi * (np.outer(ls, bins) % LANES) / LANES
    co, si = np.cos(angle), np.sin(angle)
    inner_f = jnp.asarray(np.block([[co, -si], [si, co]]), BF)
    inner_i = jnp.asarray(np.block([[co.T, si.T], [-si.T, co.T]]), BF)
    angle = 2.0 * np.pi * np.outer(ms, ls) / full
    twiddle = jnp.asarray(np.stack([np.cos(angle), -np.sin(angle)]), F32)

    src, dst = np.arange(3 * LANES)[:, None] - LANES, np.arange(LANES)[None, :]
    gap = np.abs(src - dst)
    window = jnp.asarray(((gap > GUARD) & (gap <= GUARD + TRAIN)) / (2.0 * TRAIN), BF)

    ids = np.arange(pulses)
    angle = (np.outer(ids, ids) % pulses) * (2.0 * np.pi / pulses)
    scale = 1.0 / math.sqrt(pulses)
    dr, di = np.cos(angle) * scale, -np.sin(angle) * scale
    table = np.stack([np.stack([dr, -di], -1), np.stack([di, dr], -1)])
    table = table.reshape(2, xs, pulse_own, xs, pulse_own, 2)
    table = table.transpose(1, 0, 2, 3, 5, 4).reshape(2 * pulses, 2 * pulses)
    table = jnp.asarray(table, BF)

    beam_rows = 2 * pulse_own
    vmem, dma = pltpu.VMEM, pltpu.SemaphoreType.DMA
    any_space = pl.BlockSpec(memory_space=pl.ANY)
    consts = (steering, spectrum, outer_f, outer_i, inner_f, inner_i, twiddle, table, window)
    return pl.pallas_call(
        functools.partial(chain_kernel, (zs, ys, xs, chunks)),
        out_shape=jax.ShapeDtypeStruct((count, pulse_own, gates), F32),
        in_specs=[any_space] * (1 + len(consts)),
        out_specs=pl.BlockSpec(memory_space=vmem),
        scratch_shapes=[vmem(a.shape, a.dtype) for a in consts]
        + [
            vmem((depth, gates), BF),
            vmem((depth, gates), BF),
            vmem((2 * count * beam_rows, gates), BF),
            vmem((2 * count * beam_rows, gates), BF),
            vmem((2 * count * beam_rows, gates), F32),
            vmem((2 * count, beam_rows, gates), BF),
            vmem((ys, xs * beam_rows, gates), BF),
            vmem((ys, xs * beam_rows, gates), BF),
            vmem((xs, ys, gates // LANES * pulse_own, LANES), BF),
            vmem((count, gates // LANES * pulse_own, LANES), BF),
            vmem((2, 2, 2 * count * beam_rows, depth), BF),
            vmem((m_count * 2 * ROWS, m_count * 2 * ROWS), BF),
            vmem((m_count * 2 * ROWS, m_count * 2 * ROWS), BF),
            vmem((2 * pulses, 2 * pulses), BF),
            vmem((4, m_count, ROWS, LANES), F32),
            vmem((2, m_count, LANES), F32),
            dma((len(consts),)),
            dma((chunks,)),
            dma((chunks,)), dma((chunks,)),
            dma((chunks,)), dma((chunks,)),
            dma((chunks,)), dma((chunks,)),
            dma((xs, ys)), dma((count,)),
        ],
        compiler_params=pltpu.CompilerParams(
            collective_id=0, has_side_effects=True, vmem_limit_bytes=VM
        ),
        name="chain",
    )(*[
        pltpu.with_memory_space_constraint(v, pltpu.HBM)
        for v in (signal.reshape(depth, gates), *map(jnp.asarray, consts))
    ])


def shards(signal, steering, spectrum):
    zs, xs, ys = (lax.axis_size(a) for a in ("chan", "pulse", "range"))
    _, _, pulse_own, gates = signal.shape
    fits = (
        zs == 4
        and xs == 4
        and pulse_own == ROWS
        and steering.shape[1] == zs * xs * ys
        and gates * ys * 2 == LANES * LANES
        and gates % (CHUNKS * LANES) == 0
    )
    return (shards_chain if fits else shards_split)(signal, steering, spectrum)


def solution(mesh):
    in_specs = (P(None, "chan", "pulse", "range"), P(), P())
    out_specs = P("chan", "pulse", "range")
    return jax.shard_map(shards, mesh=mesh, in_specs=in_specs, out_specs=out_specs, check_vma=False)
```

```python
import functools
import math

import jax
import jax.numpy as jnp
import numpy as np
from jax import lax
from jax.experimental import pallas as pl
from jax.experimental.pallas import tpu as pltpu
from jax.sharding import PartitionSpec as P

GUARD = 4
TRAIN = 16
NOISE_FLOOR = 0.25
LANES = 128
ROWS = 8
CHUNKS = 16
GROUP = 1
LAG = 2
BF = jnp.bfloat16
F32 = jnp.float32
VM = 44 * 1024 * 1024


def dot(a, b):
    return jnp.dot(a, b, preferred_element_type=F32)


def doppler_table(count):
    ids = np.arange(count)
    angle = (np.outer(ids, ids) % count) * (2.0 * np.pi / count)
    scale = 1.0 / math.sqrt(count)
    return jnp.asarray(np.cos(angle) * scale, BF), jnp.asarray(-np.sin(angle) * scale, BF)


def expand(left_ids, left_tag, table, right_ids, right_tag):
    n, m = table.shape
    left = (jnp.asarray(left_ids, jnp.int32)[:, None] == jnp.arange(n)[None, :]).astype(BF)
    right = (jnp.arange(m)[:, None] == jnp.asarray(right_ids, jnp.int32)[None, :]).astype(BF)
    wide = dot(dot(left, table).astype(BF), right)
    same = jnp.asarray(left_tag, jnp.int32)[:, None] == jnp.asarray(right_tag, jnp.int32)[None, :]
    return jnp.where(same, wide, 0.0).astype(BF)


def grid_ids(*sizes):
    return [g.reshape(-1) for g in np.meshgrid(*[np.arange(s) for s in sizes], indexing="ij")]


def call(body, out_shape, name):
    return pl.pallas_call(
        body,
        out_shape=out_shape,
        compiler_params=pltpu.CompilerParams(vmem_limit_bytes=VM),
        name=name,
    )


def form_kernel(w_ref, x_ref, o_ref):
    o_ref[...] = dot(w_ref[...], x_ref[...]).astype(BF)


def range_kernel(blocks, x_ref, f_ref, fi_ref, t_ref, l_ref, li_ref, h_ref, o_ref):
    sources, rows, width = x_ref.shape
    per = width // LANES
    groups = rows // 16
    m_count = sources * per
    tile = []
    for g in range(groups):
        parts = [
            x_ref[s, 16 * g : 16 * g + 16, LANES * j : LANES * j + LANES]
            for s in range(sources)
            for j in range(per)
        ]
        tile.append(jnp.concatenate(parts, axis=0))
    outer = dot(f_ref[...], jnp.concatenate(tile, axis=1))
    tr, ti = t_ref[0], t_ref[1]
    hr, hi = h_ref[0], h_ref[1]
    back = []
    for g in range(groups):
        a = outer[:, LANES * g : LANES * g + LANES].reshape(m_count, 2, ROWS, LANES)
        ar, ai = a[:, 0], a[:, 1]
        b = jnp.concatenate([ar * tr - ai * ti, ar * ti + ai * tr], axis=-1)
        c = dot(b.reshape(m_count * ROWS, 2 * LANES).astype(BF), l_ref[...])
        c = c.reshape(m_count, ROWS, 2 * LANES)
        cr, ci = c[..., :LANES], c[..., LANES:]
        d = jnp.concatenate([cr * hr - ci * hi, cr * hi + ci * hr], axis=-1)
        e = dot(d.reshape(m_count * ROWS, 2 * LANES).astype(BF), li_ref[...])
        e = e.reshape(m_count, ROWS, 2 * LANES)
        er, ei = e[..., :LANES], e[..., LANES:]
        f = jnp.stack([er * tr + ei * ti, ei * tr - er * ti], axis=1)
        back.append(f.reshape(m_count * 16, LANES).astype(BF))
    y = dot(fi_ref[...], jnp.concatenate(back, axis=1)).astype(BF)
    span = m_count // blocks
    for d in range(blocks):
        for j in range(-1, span + 1):
            m = d * span + j
            for g in range(groups):
                if 0 <= m < m_count:
                    v = y[16 * m : 16 * m + 16, LANES * g : LANES * g + LANES]
                else:
                    v = jnp.zeros((16, LANES), BF)
                o_ref[d, 16 * g : 16 * g + 16, LANES * (j + 1) : LANES * (j + 2)] = v


def cfar_kernel(d_ref, x_ref, n_ref, o_ref):
    half = d_ref.shape[0] // 2
    mix = dot(d_ref[...], x_ref[...].reshape(d_ref.shape[1], x_ref.shape[-1]))
    re, im = mix[:half], mix[half:]
    power = re * re + im * im
    narrow = power.astype(BF)
    shape = o_ref.shape[:-1] + (LANES,)
    for j in range(o_ref.shape[-1] // LANES):
        noise = dot(narrow[:, LANES * j : LANES * (j + 3)], n_ref[...])
        own = power[:, LANES * (j + 1) : LANES * (j + 2)]
        found = (own / (noise + NOISE_FLOOR)).astype(BF)
        o_ref[..., LANES * j : LANES * j + LANES] = found.reshape(shape)


def cfar_only_kernel(p_ref, n_ref, o_ref):
    narrow = p_ref[...].astype(BF)
    for j in range(o_ref.shape[1] // LANES):
        noise = dot(narrow[:, LANES * j : LANES * (j + 3)], n_ref[...])
        own = p_ref[:, LANES * (j + 1) : LANES * (j + 2)]
        o_ref[:, LANES * j : LANES * j + LANES] = (own / (noise + NOISE_FLOOR)).astype(BF)


def place_kernel(x_ref, o_ref):
    count, _, width = x_ref.shape
    for s in range(count):
        o_ref[:, width * s : width * s + width] = x_ref[s].astype(F32)


def complex_rows(re, im):
    top = np.stack([re, -im], -1)
    low = np.stack([im, re], -1)
    return np.stack([top, low], 1).reshape(2 * re.shape[0], 2 * re.shape[1])


def shards_split(signal, steering, spectrum):
    beams, chans = steering.shape[1], steering.shape[2]
    _, chan_own, pulse_own, gates = signal.shape
    zs, xs, ys = (lax.axis_size(a) for a in ("chan", "pulse", "range"))
    beam_own = beams // zs
    part = pulse_own // ys
    full = gates * ys
    block = gates // zs
    m_count = full // LANES
    groups = beam_own * part // ROWS
    pulses = pulse_own * xs

    w_real, w_imag = steering[0], steering[1]
    weights = jnp.concatenate(
        [jnp.concatenate([w_real, -w_imag], 1), jnp.concatenate([w_imag, w_real], 1)], 0
    )
    dy, dz, gr, cp, it = grid_ids(ys, zs, groups, 2, ROWS)
    bp = gr * ROWS + it
    left = cp * beams + dz * beam_own + bp // part
    left_pulse = dy * part + bp % part
    sz, ci, ch, pi = grid_ids(zs, 2, chan_own, pulse_own)
    right = ci * chans + sz * chan_own + ch
    form = expand(left, left_pulse, weights, right, pi)

    ms = np.arange(m_count)
    angle = 2.0 * np.pi * (np.outer(ms, ms) % m_count) / m_count
    outer_f = jnp.asarray(complex_rows(np.cos(angle), -np.sin(angle)), BF)
    outer_i = jnp.asarray(complex_rows(np.cos(angle), np.sin(angle)), BF)
    mk, mc, mi = grid_ids(m_count, 2, ROWS)
    outer_f = expand(mk * 2 + mc, mi, outer_f, mk * 2 + mc, mi)
    outer_i = expand(mk * 2 + mc, mi, outer_i, mk * 2 + mc, mi)
    ls = np.arange(LANES)
    angle = 2.0 * np.pi * (np.outer(ls, ls) % LANES) / LANES
    co, si = np.cos(angle), np.sin(angle)
    inner_f = jnp.asarray(np.block([[co, -si], [si, co]]), BF)
    inner_i = jnp.asarray(np.block([[co, si], [-si, co]]), BF)
    angle = 2.0 * np.pi * np.outer(ms, ls) / full
    twiddle = jnp.asarray(np.stack([np.cos(angle), -np.sin(angle)]), F32)
    spread = (2, m_count, ROWS, LANES)
    twiddle = jnp.broadcast_to(twiddle[:, :, None, :], spread)
    response = jnp.swapaxes(spectrum.reshape(2, LANES, m_count), 1, 2) * (1.0 / full)
    response = jnp.broadcast_to(response[:, :, None, :], spread)

    samples = lax.all_to_all(signal, "chan", split_axis=3, concat_axis=0, tiled=True)
    samples = samples.reshape(zs * 2 * chan_own * pulse_own, block)
    rows = 2 * beam_own * part
    formed = call(
        form_kernel, jax.ShapeDtypeStruct((ys * zs * rows, block), BF), "form"
    )(form, samples).reshape(ys * zs, rows, block)
    formed = lax.all_to_all(formed, ("range", "chan"), split_axis=0, concat_axis=0, tiled=True)

    blocks = ys * xs
    own = full // blocks
    padded = own + 2 * LANES
    packed = call(
        functools.partial(range_kernel, blocks),
        jax.ShapeDtypeStruct((blocks, rows, padded), BF),
        "compress",
    )(formed, outer_f, outer_i, twiddle, inner_f, inner_i, response)
    columns = lax.all_to_all(packed, ("range", "pulse"), split_axis=0, concat_axis=0, tiled=True)

    src, dst = np.arange(3 * LANES)[:, None] - LANES, np.arange(LANES)[None, :]
    gap = np.abs(src - dst)
    window = jnp.asarray(((gap > GUARD) & (gap <= GUARD + TRAIN)) / (2.0 * TRAIN), BF)

    dr, di = doppler_table(pulses)
    out_shape = jax.ShapeDtypeStruct((pulses * beam_own, own), BF)
    if 2 * pulses * beam_own <= 1024:
        table = jnp.concatenate([jnp.concatenate([dr, -di], 1), jnp.concatenate([di, dr], 1)], 0)
        oc, oq, ob, of = grid_ids(2, xs, beam_own, pulse_own)
        sy, sx, gr, cp, it = grid_ids(ys, xs, groups, 2, ROWS)
        bp = gr * ROWS + it
        pulse = sx * pulse_own + sy * part + bp % part
        mix = expand(oc * pulses + oq * pulse_own + of, ob, table, cp * pulses + pulse, bp // part)
        found = call(cfar_kernel, out_shape, "cfar")(
            mix, columns.reshape(blocks * rows, padded), window
        )
    else:
        v = columns.reshape(ys, xs, groups, 2, ROWS // part, part, padded)
        v = jnp.transpose(v, (3, 2, 4, 1, 0, 5, 6)).reshape(2, beam_own, pulses, padded)

        def product(t, x):
            return jnp.einsum("fp,bpr->fbr", t, x, preferred_element_type=F32)

        re = product(dr, v[0]) - product(di, v[1])
        im = product(dr, v[1]) + product(di, v[0])
        power = (re * re + im * im).reshape(xs, pulse_own, beam_own, padded)
        power = jnp.swapaxes(power, 1, 2).reshape(pulses * beam_own, padded)
        found = call(cfar_only_kernel, out_shape, "cfar")(power, window)
    found = found.reshape(xs, beam_own * pulse_own, own)
    found = lax.all_to_all(found, "pulse", split_axis=0, concat_axis=0, tiled=True)
    out = call(
        place_kernel, jax.ShapeDtypeStruct((beam_own * pulse_own, gates), F32), "place"
    )(found)
    return out.reshape(beam_own, pulse_own, gates)


MESH = pl.DeviceIdType.MESH


def iota(shape, dim):
    return lax.broadcasted_iota(jnp.int32, shape, dim)


def pick(ids, other):
    return (ids == other).astype(F32).astype(BF)


def widen(row_ids, row_tags, table, col_ids, col_tags):
    n, m = table.shape
    r, c = row_ids.shape[0], col_ids.shape[1]
    wide = dot(pick(row_ids, iota((r, n), 1)), table).astype(BF)
    wide = dot(wide, pick(iota((m, c), 0), col_ids))
    return jnp.where(row_tags == col_tags, wide, 0.0).astype(BF)


def chain_kernel(
    sizes, sig, steer_h, spec_h, f_h, fi_h, inf_h, ini_h, tw_h, dop_h, win_h, out,
    steer, spec, f_t, fi_t, inf, ini, tw, dop_t, win,
    own1, recv1, sendp, recvp, acc, send2, recv2, dop, send4, recv4,
    wide_w, mix, resp, gates_t, edges, turn,
    const_sem, own_sem, s1, r1, sp, rp, s2, r2, s4, r4,
):
    zs, ys, xs, chunks = sizes
    depth, gates = own1.shape
    width = gates // chunks
    beams, chans = steer.shape[1], steer.shape[2]
    count = ys * xs
    beam_rows = send2.shape[1]
    m_count = tw.shape[1]
    span = m_count // ys
    stride = m_count + ROWS
    turn_row = span + ROWS
    z, y, x = (lax.axis_index(a) for a in ("chan", "range", "pulse"))
    me = y * xs + x
    half = lax.div(z, 2)
    hub, edge = 1 + half, 3 * half
    is_hub = z == hub
    is_edge = z == edge

    consts = [
        pltpu.make_async_copy(a, b, const_sem.at[i])
        for i, (a, b) in enumerate(
            zip(
                (steer_h, spec_h, f_h, fi_h, inf_h, ini_h, tw_h, dop_h, win_h),
                (steer, spec, f_t, fi_t, inf, ini, tw, dop_t, win),
            )
        )
    ]

    def lanes(c):
        return pl.ds(pl.multiple_of(c * width, LANES), width)

    def wide_lanes(c):
        return pl.ds(pl.multiple_of(c * width * GROUP, LANES), width * GROUP)

    def mine(c):
        return pltpu.make_async_copy(
            sig.at[:, lanes(c)], own1.at[:, lanes(c)], own_sem.at[c]
        )

    def loop(body, start=0, stop=chunks):
        def step(c, carry):
            body(c)
            return carry

        lax.fori_loop(start, stop, step, 0)

    for copy in consts:
        copy.start()

    @pl.when(is_hub)
    def _():
        loop(lambda c: mine(c).start())

    def plane(i):
        d = lax.rem(i, count)
        return {
            "chan": jnp.where(i < count, hub, edge),
            "range": lax.div(d, xs),
            "pulse": lax.rem(d, xs),
        }

    both = 2 * count
    me_both = me + jnp.where(is_hub, 0, count)
    barrier = pltpu.get_barrier_semaphore()
    for k in range(1, both):
        pl.semaphore_signal(
            barrier, inc=1, device_id=plane(lax.rem(me_both + k, both)), device_id_type=MESH
        )
    pl.semaphore_signal(barrier, inc=1, device_id={"chan": 3 - z}, device_id_type=MESH)
    pl.semaphore_wait(barrier, both)

    def plan(src, dst, send, recv, target):
        return pltpu.make_async_remote_copy(
            src_ref=src, dst_ref=dst, send_sem=send, recv_sem=recv,
            device_id=target, device_id_type=MESH,
        )

    def raw(c):
        return plan(
            sig.at[:, lanes(c)], recv1.at[:, lanes(c)], s1.at[c], r1.at[c], {"chan": hub}
        )

    @pl.when(is_edge)
    def _():
        loop(lambda c: raw(c).start())

    for copy in consts:
        copy.wait()

    def tables():
        for i in range(2):
            for t in range(m_count):
                gates_t[i, t : t + 1] = spec[i : i + 1, LANES * t : LANES * t + LANES]
            turned = gates_t[i].T * (1.0 / (m_count * LANES))
            resp[i] = jnp.concatenate([turned[:m_count], turned[m_count:]], axis=1)
        edges[...] = jnp.zeros_like(edges)
        for i, g in enumerate(order):
            mix[beam_rows * i : beam_rows * i + beam_rows] = dop_t[
                pl.ds(pl.multiple_of(beam_rows * g, beam_rows), beam_rows)
            ]

    chip, core = lax.div(x, 2), lax.rem(x, 2)
    order = [2 * (1 - chip), 2 * (1 - chip) + 1, 2 * chip + 1 - core, x]

    def doppler(c):
        tiles = width * GROUP // LANES
        for i in range(ys):
            found = dot(mix[...], recv2[i, :, wide_lanes(c)])
            for t in range(tiles):
                m = i * (gates // LANES) + c * tiles + t
                dop[pl.ds(m, xs * beam_rows, stride=stride)] = found[
                    :, LANES * t : LANES * t + LANES
                ]

    @pl.when(is_hub)
    def _():
        re, im = steer[0], steer[1]
        weights = jnp.concatenate(
            [jnp.concatenate([re, -im], 1), jnp.concatenate([im, re], 1)], 0
        )
        pulse_own = beam_rows // 2
        chan_own = chans // zs
        r = iota((both * beam_rows, 1), 0)
        c = iota((1, depth), 1)
        row_tag, col_tag = lax.rem(r, pulse_own), lax.rem(c, pulse_own)
        r, c = lax.div(r, pulse_own), lax.div(c, pulse_own)
        dest = lax.div(r, 2)
        for i, h in enumerate((half, 1 - half)):
            at = jnp.where(dest < count, 1 + h, 3 * h)
            row = lax.rem(r, 2) * beams + at * count + lax.rem(dest, count)
            for j, source in enumerate((hub, edge)):
                col = lax.div(c, chan_own) * chans + source * chan_own + lax.rem(c, chan_own)
                wide_w[i, j] = widen(row, row_tag, weights, col, col_tag)

        def swap(c):
            return plan(
                sendp.at[:, lanes(c)], recvp.at[:, lanes(c)], sp.at[c], rp.at[c],
                {"chan": 3 - hub},
            )

        def form(c):
            mine(c).wait()
            raw(c).wait_recv()
            a, b = own1[:, lanes(c)], recv1[:, lanes(c)]
            sendp[:, lanes(c)] = (dot(wide_w[1, 0], a) + dot(wide_w[1, 1], b)).astype(BF)
            swap(c).start()
            acc[:, lanes(c)] = dot(wide_w[0, 0], a) + dot(wide_w[0, 1], b)

        def finish(c):
            swap(c).wait_recv()
            total = (acc[:, lanes(c)] + recvp[:, lanes(c)].astype(F32)).astype(BF)
            send2[:, :, lanes(c)] = total.reshape(both, beam_rows, width)

        def spray(c):
            mine_rows = pl.ds(pl.multiple_of(beam_rows * x, beam_rows), beam_rows)
            for k in range(1, both):
                to = lax.rem(me + k, both)
                plan(
                    send2.at[to, :, wide_lanes(c)], recv2.at[y, mine_rows, wide_lanes(c)],
                    s2.at[c], r2.at[c], plane(to),
                ).start()
            recv2[y, mine_rows, wide_lanes(c)] = send2[me, :, wide_lanes(c)]

        def arrived(c):
            plan(
                send2.at[pl.ds(0, count - 1), :, wide_lanes(c)],
                send2.at[pl.ds(0, count - 1), :, wide_lanes(c)],
                s2.at[c], r2.at[c], {"chan": edge},
            ).wait_recv()

        def body(c):
            form(c)

            @pl.when(c == 0)
            def _():
                tables()

            @pl.when(c >= LAG)
            def _():
                step(c - LAG)

        def step(c):
            finish(c)

            @pl.when(lax.rem(c, GROUP) == GROUP - 1)
            def _():
                g = lax.div(c, GROUP)
                spray(g)

                @pl.when(g >= 3)
                def _():
                    arrived(g - 3)
                    doppler(g - 3)

        loop(body)
        loop(step, chunks - LAG)

        def rest(c):
            arrived(c)
            doppler(c)

        loop(rest, chunks // GROUP - 3, chunks // GROUP)

    @pl.when(is_edge)
    def _():
        tables()

        def body(c):
            plan(
                send2.at[pl.ds(0, count), :, wide_lanes(c)],
                send2.at[pl.ds(0, count), :, wide_lanes(c)],
                s2.at[c], r2.at[c], {"chan": hub},
            ).wait_recv()
            doppler(c)

        loop(body, 0, chunks // GROUP)

    tr, ti = tw[0], tw[1]
    hr, hi = resp[0], resp[1]
    fourth = []

    def split(v, i):
        w = v[:, LANES * i : LANES * i + LANES]
        return w[:m_count], w[m_count:]

    def cut(v, i):
        w = v[m_count * i : m_count * i + m_count]
        return w[:, :LANES], w[:, LANES:]

    for p in range(xs):
        cols = []
        for i in range(ROWS):
            at = stride * (beam_rows * p + 2 * i)
            pair = [dop[at : at + m_count], dop[at + stride : at + stride + m_count]]
            cols.append(jnp.concatenate(pair, axis=0).astype(BF))
        outer = dot(f_t[...], jnp.concatenate(cols, axis=1))
        rows = []
        for i in range(ROWS):
            ar, ai = split(outer, i)
            rows.append(
                jnp.concatenate([ar * tr - ai * ti, ar * ti + ai * tr], axis=1).astype(BF)
            )
        inner = dot(jnp.concatenate(rows, axis=0), inf[...])
        rows = []
        for i in range(ROWS):
            cr, ci = cut(inner, i)
            rows.append(
                jnp.concatenate([cr * hr - ci * hi, cr * hi + ci * hr], axis=1).astype(BF)
            )
        inner = dot(jnp.concatenate(rows, axis=0), ini[...])
        cols = []
        for i in range(ROWS):
            er, ei = cut(inner, i)
            cols.append(
                jnp.concatenate([er * tr + ei * ti, ei * tr - er * ti], axis=0).astype(BF)
            )
        outer = dot(fi_t[...], jnp.concatenate(cols, axis=1))
        rows, powers = [], []
        for i in range(ROWS):
            re, im = split(outer, i)
            power = re * re + im * im
            slot = (p * ROWS + i) % edges.shape[0]
            edges[slot, ROWS : ROWS + m_count] = power
            before = edges[slot, ROWS - 1 : ROWS - 1 + m_count]
            after = edges[slot, ROWS + 1 : ROWS + 1 + m_count]
            side = jnp.where(iota((m_count, LANES), 1) < LANES // 2, after, before)
            rows.append(jnp.concatenate([power, side], axis=1).astype(BF))
            powers.append(power)
        noise = dot(jnp.concatenate(rows, axis=0), win[...])
        for i in range(ROWS):
            level = noise[m_count * i : m_count * i + m_count] + NOISE_FLOOR
            found = (powers[i] / level).astype(BF)
            for k in range(ys):
                send4[p, k, span * i : span * i + span] = found[span * k : span * k + span]
        for k in range(ys):
            if p == xs - 1 and k == 0:
                recv4[me] = send4[p, y]
                continue
            to_y = lax.rem(y + k, ys)
            copy = plan(
                send4.at[p, to_y], recv4.at[me], s4.at[p, k], r4.at[me],
                {"range": to_y, "pulse": order[p]},
            )
            copy.start()
            fourth.append(copy)

    def place(i):
        for b in range(ROWS):
            turn[turn_row * b : turn_row * b + span] = recv4[
                i, span * b : span * b + span
            ].astype(F32)
        for t in range(span):
            out[i, :, LANES * t : LANES * t + LANES] = turn[pl.ds(t, ROWS, stride=turn_row)]

    def final_step(k, carry):
        i = lax.rem(me + k, count)

        @pl.when(k > 0)
        def _():
            plan(
                send4.at[0, 0], recv4.at[i], s4.at[0, 0], r4.at[i], {"chan": 3 - z}
            ).wait_recv()

        place(i)
        return carry

    lax.fori_loop(0, count, final_step, 0)
    for copy in fourth:
        copy.wait_send()

    @pl.when(is_edge)
    def _():
        loop(lambda c: raw(c).wait_send())

    @pl.when(is_hub)
    def _():
        def body(c):
            plan(
                sendp.at[:, lanes(c)], recvp.at[:, lanes(c)], sp.at[c], rp.at[c],
                {"chan": 3 - hub},
            ).wait_send()

        loop(body)

        def sprayed(c):
            plan(
                send2.at[pl.ds(0, both - 1), :, wide_lanes(c)],
                send2.at[pl.ds(0, both - 1), :, wide_lanes(c)],
                s2.at[c], r2.at[c], {"chan": edge},
            ).wait_send()

        loop(sprayed, 0, chunks // GROUP)


def shards_chain(signal, steering, spectrum):
    beams, chans = steering.shape[1], steering.shape[2]
    _, chan_own, pulse_own, gates = signal.shape
    zs, xs, ys = (lax.axis_size(a) for a in ("chan", "pulse", "range"))
    count = xs * ys
    full = gates * ys
    m_count = full // LANES
    pulses = pulse_own * xs
    depth = 2 * chan_own * pulse_own
    chunks = CHUNKS

    ms = np.arange(m_count)
    angle = 2.0 * np.pi * (np.outer(ms, ms) % m_count) / m_count
    co, si = np.cos(angle), np.sin(angle)
    outer_f = jnp.asarray(np.block([[co, si], [-si, co]]), BF)
    outer_i = jnp.asarray(np.block([[co, -si], [si, co]]), BF)
    ls = np.arange(LANES)
    times = LANES // m_count
    bins = (ls % m_count) * times + ls // m_count
    angle = 2.0 * np.pi * (np.outer(ls, bins) % LANES) / LANES
    co, si = np.cos(angle), np.sin(angle)
    inner_f = jnp.asarray(np.block([[co, -si], [si, co]]), BF)
    inner_i = jnp.asarray(np.block([[co.T, si.T], [-si.T, co.T]]), BF)
    angle = 2.0 * np.pi * np.outer(ms, ls) / full
    twiddle = jnp.asarray(np.stack([np.cos(angle), -np.sin(angle)]), F32)

    dst = np.arange(LANES)
    side = np.where(dst < LANES // 2, dst + LANES, dst - LANES)
    gap = np.abs(np.concatenate([dst, side])[:, None] - dst[None, :])
    window = jnp.asarray(((gap > GUARD) & (gap <= GUARD + TRAIN)) / (2.0 * TRAIN), BF)

    ids = np.arange(pulses)
    angle = (np.outer(ids, ids) % pulses) * (2.0 * np.pi / pulses)
    scale = 1.0 / math.sqrt(pulses)
    dr, di = np.cos(angle) * scale, -np.sin(angle) * scale
    table = np.stack([np.stack([dr, -di], -1), np.stack([di, dr], -1)])
    table = table.reshape(2, xs, pulse_own, xs, pulse_own, 2)
    table = table.transpose(1, 2, 0, 3, 5, 4).reshape(2 * pulses, 2 * pulses)
    table = jnp.asarray(table, BF)

    beam_rows = 2 * pulse_own
    vmem, dma = pltpu.VMEM, pltpu.SemaphoreType.DMA
    any_space = pl.BlockSpec(memory_space=pl.ANY)
    consts = (steering, spectrum, outer_f, outer_i, inner_f, inner_i, twiddle, table, window)
    return pl.pallas_call(
        functools.partial(chain_kernel, (zs, ys, xs, chunks)),
        out_shape=jax.ShapeDtypeStruct((count, pulse_own, gates), F32),
        in_specs=[any_space] * (1 + len(consts)),
        out_specs=pl.BlockSpec(memory_space=vmem),
        scratch_shapes=[vmem(a.shape, a.dtype) for a in consts]
        + [
            vmem((depth, gates), BF),
            vmem((depth, gates), BF),
            vmem((2 * count * beam_rows, gates), BF),
            vmem((2 * count * beam_rows, gates), BF),
            vmem((2 * count * beam_rows, gates), F32),
            vmem((2 * count, beam_rows, gates), BF),
            vmem((ys, xs * beam_rows, gates), BF),
            vmem((xs * beam_rows * (m_count + ROWS), LANES), F32),
            vmem((xs, ys, gates // LANES * pulse_own, LANES), BF),
            vmem((count, gates // LANES * pulse_own, LANES), BF),
            vmem((2, 2, 2 * count * beam_rows, depth), BF),
            vmem((2 * pulses, 2 * pulses), BF),
            vmem((2, m_count, LANES), F32),
            vmem((2, m_count, LANES), F32),
            vmem((2 * ROWS, m_count + 2 * ROWS, LANES), F32),
            vmem((pulse_own * (m_count // ys + ROWS), LANES), F32),
            dma((len(consts),)),
            dma((chunks,)),
            dma((chunks,)), dma((chunks,)),
            dma((chunks,)), dma((chunks,)),
            dma((chunks,)), dma((chunks,)),
            dma((xs, ys)), dma((count,)),
        ],
        compiler_params=pltpu.CompilerParams(
            collective_id=0, has_side_effects=True, vmem_limit_bytes=VM
        ),
        name="chain",
    )(*[
        pltpu.with_memory_space_constraint(v, pltpu.HBM)
        for v in (signal.reshape(depth, gates), *map(jnp.asarray, consts))
    ])


def shards(signal, steering, spectrum):
    zs, xs, ys = (lax.axis_size(a) for a in ("chan", "pulse", "range"))
    _, _, pulse_own, gates = signal.shape
    fits = (
        zs == 4
        and xs == 4
        and pulse_own == ROWS
        and steering.shape[1] == zs * xs * ys
        and gates * ys * 2 == LANES * LANES
        and gates % (CHUNKS * LANES) == 0
    )
    return (shards_chain if fits else shards_split)(signal, steering, spectrum)


def solution(mesh):
    in_specs = (P(None, "chan", "pulse", "range"), P(), P())
    out_specs = P("chan", "pulse", "range")
    return jax.shard_map(shards, mesh=mesh, in_specs=in_specs, out_specs=out_specs, check_vma=False)
```

```python
import functools
import math

import jax
import jax.numpy as jnp
import numpy as np
from jax import lax
from jax.experimental import pallas as pl
from jax.experimental.pallas import tpu as pltpu
from jax.sharding import PartitionSpec as P

GUARD = 4
TRAIN = 16
NOISE_FLOOR = 0.25
LANES = 128
ROWS = 8
CHUNKS = 16
GROUP = 1
LAG = 2
BF = jnp.bfloat16
F32 = jnp.float32
VM = 44 * 1024 * 1024


def dot(a, b):
    return jnp.dot(a, b, preferred_element_type=F32)


def doppler_table(count):
    ids = np.arange(count)
    angle = (np.outer(ids, ids) % count) * (2.0 * np.pi / count)
    scale = 1.0 / math.sqrt(count)
    return jnp.asarray(np.cos(angle) * scale, BF), jnp.asarray(-np.sin(angle) * scale, BF)


def expand(left_ids, left_tag, table, right_ids, right_tag):
    n, m = table.shape
    left = (jnp.asarray(left_ids, jnp.int32)[:, None] == jnp.arange(n)[None, :]).astype(BF)
    right = (jnp.arange(m)[:, None] == jnp.asarray(right_ids, jnp.int32)[None, :]).astype(BF)
    wide = dot(dot(left, table).astype(BF), right)
    same = jnp.asarray(left_tag, jnp.int32)[:, None] == jnp.asarray(right_tag, jnp.int32)[None, :]
    return jnp.where(same, wide, 0.0).astype(BF)


def grid_ids(*sizes):
    return [g.reshape(-1) for g in np.meshgrid(*[np.arange(s) for s in sizes], indexing="ij")]


def call(body, out_shape, name):
    return pl.pallas_call(
        body,
        out_shape=out_shape,
        compiler_params=pltpu.CompilerParams(vmem_limit_bytes=VM),
        name=name,
    )


def form_kernel(w_ref, x_ref, o_ref):
    o_ref[...] = dot(w_ref[...], x_ref[...]).astype(BF)


def range_kernel(blocks, x_ref, f_ref, fi_ref, t_ref, l_ref, li_ref, h_ref, o_ref):
    sources, rows, width = x_ref.shape
    per = width // LANES
    groups = rows // 16
    m_count = sources * per
    tile = []
    for g in range(groups):
        parts = [
            x_ref[s, 16 * g : 16 * g + 16, LANES * j : LANES * j + LANES]
            for s in range(sources)
            for j in range(per)
        ]
        tile.append(jnp.concatenate(parts, axis=0))
    outer = dot(f_ref[...], jnp.concatenate(tile, axis=1))
    tr, ti = t_ref[0], t_ref[1]
    hr, hi = h_ref[0], h_ref[1]
    back = []
    for g in range(groups):
        a = outer[:, LANES * g : LANES * g + LANES].reshape(m_count, 2, ROWS, LANES)
        ar, ai = a[:, 0], a[:, 1]
        b = jnp.concatenate([ar * tr - ai * ti, ar * ti + ai * tr], axis=-1)
        c = dot(b.reshape(m_count * ROWS, 2 * LANES).astype(BF), l_ref[...])
        c = c.reshape(m_count, ROWS, 2 * LANES)
        cr, ci = c[..., :LANES], c[..., LANES:]
        d = jnp.concatenate([cr * hr - ci * hi, cr * hi + ci * hr], axis=-1)
        e = dot(d.reshape(m_count * ROWS, 2 * LANES).astype(BF), li_ref[...])
        e = e.reshape(m_count, ROWS, 2 * LANES)
        er, ei = e[..., :LANES], e[..., LANES:]
        f = jnp.stack([er * tr + ei * ti, ei * tr - er * ti], axis=1)
        back.append(f.reshape(m_count * 16, LANES).astype(BF))
    y = dot(fi_ref[...], jnp.concatenate(back, axis=1)).astype(BF)
    span = m_count // blocks
    for d in range(blocks):
        for j in range(-1, span + 1):
            m = d * span + j
            for g in range(groups):
                if 0 <= m < m_count:
                    v = y[16 * m : 16 * m + 16, LANES * g : LANES * g + LANES]
                else:
                    v = jnp.zeros((16, LANES), BF)
                o_ref[d, 16 * g : 16 * g + 16, LANES * (j + 1) : LANES * (j + 2)] = v


def cfar_kernel(d_ref, x_ref, n_ref, o_ref):
    half = d_ref.shape[0] // 2
    mix = dot(d_ref[...], x_ref[...].reshape(d_ref.shape[1], x_ref.shape[-1]))
    re, im = mix[:half], mix[half:]
    power = re * re + im * im
    narrow = power.astype(BF)
    shape = o_ref.shape[:-1] + (LANES,)
    for j in range(o_ref.shape[-1] // LANES):
        noise = dot(narrow[:, LANES * j : LANES * (j + 3)], n_ref[...])
        own = power[:, LANES * (j + 1) : LANES * (j + 2)]
        found = (own / (noise + NOISE_FLOOR)).astype(BF)
        o_ref[..., LANES * j : LANES * j + LANES] = found.reshape(shape)


def cfar_only_kernel(p_ref, n_ref, o_ref):
    narrow = p_ref[...].astype(BF)
    for j in range(o_ref.shape[1] // LANES):
        noise = dot(narrow[:, LANES * j : LANES * (j + 3)], n_ref[...])
        own = p_ref[:, LANES * (j + 1) : LANES * (j + 2)]
        o_ref[:, LANES * j : LANES * j + LANES] = (own / (noise + NOISE_FLOOR)).astype(BF)


def place_kernel(x_ref, o_ref):
    count, _, width = x_ref.shape
    for s in range(count):
        o_ref[:, width * s : width * s + width] = x_ref[s].astype(F32)


def complex_rows(re, im):
    top = np.stack([re, -im], -1)
    low = np.stack([im, re], -1)
    return np.stack([top, low], 1).reshape(2 * re.shape[0], 2 * re.shape[1])


def shards_split(signal, steering, spectrum):
    beams, chans = steering.shape[1], steering.shape[2]
    _, chan_own, pulse_own, gates = signal.shape
    zs, xs, ys = (lax.axis_size(a) for a in ("chan", "pulse", "range"))
    beam_own = beams // zs
    part = pulse_own // ys
    full = gates * ys
    block = gates // zs
    m_count = full // LANES
    groups = beam_own * part // ROWS
    pulses = pulse_own * xs

    w_real, w_imag = steering[0], steering[1]
    weights = jnp.concatenate(
        [jnp.concatenate([w_real, -w_imag], 1), jnp.concatenate([w_imag, w_real], 1)], 0
    )
    dy, dz, gr, cp, it = grid_ids(ys, zs, groups, 2, ROWS)
    bp = gr * ROWS + it
    left = cp * beams + dz * beam_own + bp // part
    left_pulse = dy * part + bp % part
    sz, ci, ch, pi = grid_ids(zs, 2, chan_own, pulse_own)
    right = ci * chans + sz * chan_own + ch
    form = expand(left, left_pulse, weights, right, pi)

    ms = np.arange(m_count)
    angle = 2.0 * np.pi * (np.outer(ms, ms) % m_count) / m_count
    outer_f = jnp.asarray(complex_rows(np.cos(angle), -np.sin(angle)), BF)
    outer_i = jnp.asarray(complex_rows(np.cos(angle), np.sin(angle)), BF)
    mk, mc, mi = grid_ids(m_count, 2, ROWS)
    outer_f = expand(mk * 2 + mc, mi, outer_f, mk * 2 + mc, mi)
    outer_i = expand(mk * 2 + mc, mi, outer_i, mk * 2 + mc, mi)
    ls = np.arange(LANES)
    angle = 2.0 * np.pi * (np.outer(ls, ls) % LANES) / LANES
    co, si = np.cos(angle), np.sin(angle)
    inner_f = jnp.asarray(np.block([[co, -si], [si, co]]), BF)
    inner_i = jnp.asarray(np.block([[co, si], [-si, co]]), BF)
    angle = 2.0 * np.pi * np.outer(ms, ls) / full
    twiddle = jnp.asarray(np.stack([np.cos(angle), -np.sin(angle)]), F32)
    spread = (2, m_count, ROWS, LANES)
    twiddle = jnp.broadcast_to(twiddle[:, :, None, :], spread)
    response = jnp.swapaxes(spectrum.reshape(2, LANES, m_count), 1, 2) * (1.0 / full)
    response = jnp.broadcast_to(response[:, :, None, :], spread)

    samples = lax.all_to_all(signal, "chan", split_axis=3, concat_axis=0, tiled=True)
    samples = samples.reshape(zs * 2 * chan_own * pulse_own, block)
    rows = 2 * beam_own * part
    formed = call(
        form_kernel, jax.ShapeDtypeStruct((ys * zs * rows, block), BF), "form"
    )(form, samples).reshape(ys * zs, rows, block)
    formed = lax.all_to_all(formed, ("range", "chan"), split_axis=0, concat_axis=0, tiled=True)

    blocks = ys * xs
    own = full // blocks
    padded = own + 2 * LANES
    packed = call(
        functools.partial(range_kernel, blocks),
        jax.ShapeDtypeStruct((blocks, rows, padded), BF),
        "compress",
    )(formed, outer_f, outer_i, twiddle, inner_f, inner_i, response)
    columns = lax.all_to_all(packed, ("range", "pulse"), split_axis=0, concat_axis=0, tiled=True)

    src, dst = np.arange(3 * LANES)[:, None] - LANES, np.arange(LANES)[None, :]
    gap = np.abs(src - dst)
    window = jnp.asarray(((gap > GUARD) & (gap <= GUARD + TRAIN)) / (2.0 * TRAIN), BF)

    dr, di = doppler_table(pulses)
    out_shape = jax.ShapeDtypeStruct((pulses * beam_own, own), BF)
    if 2 * pulses * beam_own <= 1024:
        table = jnp.concatenate([jnp.concatenate([dr, -di], 1), jnp.concatenate([di, dr], 1)], 0)
        oc, oq, ob, of = grid_ids(2, xs, beam_own, pulse_own)
        sy, sx, gr, cp, it = grid_ids(ys, xs, groups, 2, ROWS)
        bp = gr * ROWS + it
        pulse = sx * pulse_own + sy * part + bp % part
        mix = expand(oc * pulses + oq * pulse_own + of, ob, table, cp * pulses + pulse, bp // part)
        found = call(cfar_kernel, out_shape, "cfar")(
            mix, columns.reshape(blocks * rows, padded), window
        )
    else:
        v = columns.reshape(ys, xs, groups, 2, ROWS // part, part, padded)
        v = jnp.transpose(v, (3, 2, 4, 1, 0, 5, 6)).reshape(2, beam_own, pulses, padded)

        def product(t, x):
            return jnp.einsum("fp,bpr->fbr", t, x, preferred_element_type=F32)

        re = product(dr, v[0]) - product(di, v[1])
        im = product(dr, v[1]) + product(di, v[0])
        power = (re * re + im * im).reshape(xs, pulse_own, beam_own, padded)
        power = jnp.swapaxes(power, 1, 2).reshape(pulses * beam_own, padded)
        found = call(cfar_only_kernel, out_shape, "cfar")(power, window)
    found = found.reshape(xs, beam_own * pulse_own, own)
    found = lax.all_to_all(found, "pulse", split_axis=0, concat_axis=0, tiled=True)
    out = call(
        place_kernel, jax.ShapeDtypeStruct((beam_own * pulse_own, gates), F32), "place"
    )(found)
    return out.reshape(beam_own, pulse_own, gates)


MESH = pl.DeviceIdType.MESH


def iota(shape, dim):
    return lax.broadcasted_iota(jnp.int32, shape, dim)


def pick(ids, other):
    return (ids == other).astype(F32).astype(BF)


def widen(row_ids, row_tags, table, col_ids, col_tags):
    n, m = table.shape
    r, c = row_ids.shape[0], col_ids.shape[1]
    wide = dot(pick(row_ids, iota((r, n), 1)), table).astype(BF)
    wide = dot(wide, pick(iota((m, c), 0), col_ids))
    return jnp.where(row_tags == col_tags, wide, 0.0).astype(BF)


def chain_kernel(
    sizes, sig, steer_h, spec_h, f_h, fi_h, inf_h, ini_h, tw_h, dop_h, win_h, out,
    steer, spec, f_t, fi_t, inf, ini, tw, dop_t, win,
    own1, recv1, sendp, recvp, acc, send2, recv2, dop, send4, recv4,
    wide_w, mix, resp, gates_t, edges, turn,
    const_sem, own_sem, s1, r1, sp, rp, s2, r2, s4, r4,
):
    zs, ys, xs, chunks = sizes
    depth, gates = own1.shape
    width = gates // chunks
    beams, chans = steer.shape[1], steer.shape[2]
    count = ys * xs
    beam_rows = send2.shape[1]
    m_count = tw.shape[1]
    span = m_count // ys
    stride = m_count + ROWS
    turn_row = span + ROWS
    z, y, x = (lax.axis_index(a) for a in ("chan", "range", "pulse"))
    me = y * xs + x
    half = lax.div(z, 2)
    hub, edge = 1 + half, 3 * half
    is_hub = z == hub
    is_edge = z == edge

    consts = [
        pltpu.make_async_copy(a, b, const_sem.at[i])
        for i, (a, b) in enumerate(
            zip(
                (steer_h, spec_h, f_h, fi_h, inf_h, ini_h, tw_h, dop_h, win_h),
                (steer, spec, f_t, fi_t, inf, ini, tw, dop_t, win),
            )
        )
    ]

    def lanes(c):
        return pl.ds(pl.multiple_of(c * width, LANES), width)

    def wide_lanes(c):
        return pl.ds(pl.multiple_of(c * width * GROUP, LANES), width * GROUP)

    def mine(c):
        return pltpu.make_async_copy(
            sig.at[:, lanes(c)], own1.at[:, lanes(c)], own_sem.at[c]
        )

    def loop(body, start=0, stop=chunks):
        def step(c, carry):
            body(c)
            return carry

        lax.fori_loop(start, stop, step, 0)

    both = 2 * count
    barrier = pltpu.get_barrier_semaphore()

    def greet(**target):
        pl.semaphore_signal(barrier, inc=1, device_id=target, device_id_type=MESH)

    @pl.when(is_hub)
    def _():
        greet(chan=edge)
        for k in range(1, count):
            to = lax.rem(me + k, count)
            greet(range=lax.div(to, xs), pulse=lax.rem(to, xs))
        greet(chan=3 - hub)
        loop(lambda c: mine(c).start())

    @pl.when(is_edge)
    def _():
        for k in range(count):
            to = lax.rem(me + k, count)
            greet(chan=hub, range=lax.div(to, xs), pulse=lax.rem(to, xs))
        pl.semaphore_wait(barrier, 1)

    for copy in consts:
        copy.start()

    def plan(src, dst, send, recv, target):
        return pltpu.make_async_remote_copy(
            src_ref=src, dst_ref=dst, send_sem=send, recv_sem=recv,
            device_id=target, device_id_type=MESH,
        )

    def raw(c):
        return plan(
            sig.at[:, lanes(c)], recv1.at[:, lanes(c)], s1.at[c], r1.at[c], {"chan": hub}
        )

    @pl.when(is_edge)
    def _():
        loop(lambda c: raw(c).start())

    for copy in consts:
        copy.wait()

    def tables():
        for i in range(2):
            for t in range(m_count):
                gates_t[i, t : t + 1] = spec[i : i + 1, LANES * t : LANES * t + LANES]
            turned = gates_t[i].T * (1.0 / (m_count * LANES))
            resp[i] = jnp.concatenate([turned[:m_count], turned[m_count:]], axis=1)
        edges[...] = jnp.zeros_like(edges)
        for i, g in enumerate(order):
            mix[beam_rows * i : beam_rows * i + beam_rows] = dop_t[
                pl.ds(pl.multiple_of(beam_rows * g, beam_rows), beam_rows)
            ]

    chip, core = lax.div(x, 2), lax.rem(x, 2)
    order = [2 * (1 - chip) + core, 2 * chip + 1 - core, 2 * (1 - chip) + 1 - core, x]

    hops = sorted(
        np.ndindex(2, ys, 2, 2), key=lambda k: -(4 * (k[0] + k[1] + k[2]) + k[3])
    )
    far_first = [
        (dz, lax.rem(y + dy, ys), 2 * lax.rem(chip + dx, 2) + lax.rem(core + dc, 2))
        for dz, dy, dx, dc in hops
        if (dz, dy, dx, dc) != (0, 0, 0, 0)
    ]

    def doppler(c):
        tiles = width * GROUP // LANES
        for i in range(ys):
            found = dot(mix[...], recv2[i, :, wide_lanes(c)])
            for t in range(tiles):
                m = i * (gates // LANES) + c * tiles + t
                dop[pl.ds(m, xs * beam_rows, stride=stride)] = found[
                    :, LANES * t : LANES * t + LANES
                ]

    @pl.when(is_hub)
    def _():
        re, im = steer[0], steer[1]
        weights = jnp.concatenate(
            [jnp.concatenate([re, -im], 1), jnp.concatenate([im, re], 1)], 0
        )
        pulse_own = beam_rows // 2
        chan_own = chans // zs
        r = iota((both * beam_rows, 1), 0)
        c = iota((1, depth), 1)
        row_tag, col_tag = lax.rem(r, pulse_own), lax.rem(c, pulse_own)
        r, c = lax.div(r, pulse_own), lax.div(c, pulse_own)
        dest = lax.div(r, 2)
        for i, h in enumerate((half, 1 - half)):
            at = jnp.where(dest < count, 1 + h, 3 * h)
            row = lax.rem(r, 2) * beams + at * count + lax.rem(dest, count)
            for j, source in enumerate((hub, edge)):
                col = lax.div(c, chan_own) * chans + source * chan_own + lax.rem(c, chan_own)
                wide_w[i, j] = widen(row, row_tag, weights, col, col_tag)

        def swap(c):
            return plan(
                sendp.at[:, lanes(c)], recvp.at[:, lanes(c)], sp.at[c], rp.at[c],
                {"chan": 3 - hub},
            )

        def form(c):
            mine(c).wait()
            raw(c).wait_recv()
            a, b = own1[:, lanes(c)], recv1[:, lanes(c)]
            sendp[:, lanes(c)] = (dot(wide_w[1, 0], a) + dot(wide_w[1, 1], b)).astype(BF)
            swap(c).start()
            acc[:, lanes(c)] = dot(wide_w[0, 0], a) + dot(wide_w[0, 1], b)

        def finish(c):
            swap(c).wait_recv()
            total = (acc[:, lanes(c)] + recvp[:, lanes(c)].astype(F32)).astype(BF)
            send2[:, :, lanes(c)] = total.reshape(both, beam_rows, width)

        def spray(c):
            mine_rows = pl.ds(pl.multiple_of(beam_rows * x, beam_rows), beam_rows)
            for plane_to, to_y, to_x in far_first:
                to = to_y * xs + to_x
                plan(
                    send2.at[plane_to * count + to, :, wide_lanes(c)],
                    recv2.at[y, mine_rows, wide_lanes(c)], s2.at[c], r2.at[c],
                    {"chan": edge if plane_to else hub, "range": to_y, "pulse": to_x},
                ).start()
            recv2[y, mine_rows, wide_lanes(c)] = send2[me, :, wide_lanes(c)]

        def arrived(c):
            plan(
                send2.at[pl.ds(0, count - 1), :, wide_lanes(c)],
                send2.at[pl.ds(0, count - 1), :, wide_lanes(c)],
                s2.at[c], r2.at[c], {"chan": edge},
            ).wait_recv()

        pl.semaphore_wait(barrier, both)

        def body(c):
            form(c)

            @pl.when(c == 0)
            def _():
                tables()

            @pl.when(c >= LAG)
            def _():
                step(c - LAG)

        def step(c):
            finish(c)

            @pl.when(lax.rem(c, GROUP) == GROUP - 1)
            def _():
                g = lax.div(c, GROUP)
                spray(g)

                @pl.when(g >= 3)
                def _():
                    arrived(g - 3)
                    doppler(g - 3)

        loop(body)
        loop(step, chunks - LAG)

        def rest(c):
            arrived(c)
            doppler(c)

        loop(rest, chunks // GROUP - 3, chunks // GROUP)

    @pl.when(is_edge)
    def _():
        tables()

        def body(c):
            plan(
                send2.at[pl.ds(0, count), :, wide_lanes(c)],
                send2.at[pl.ds(0, count), :, wide_lanes(c)],
                s2.at[c], r2.at[c], {"chan": hub},
            ).wait_recv()
            doppler(c)

        loop(body, 0, chunks // GROUP)

    tr, ti = tw[0], tw[1]
    hr, hi = resp[0], resp[1]
    fourth = []

    def split(v, i):
        w = v[:, LANES * i : LANES * i + LANES]
        return w[:m_count], w[m_count:]

    def cut(v, i):
        w = v[m_count * i : m_count * i + m_count]
        return w[:, :LANES], w[:, LANES:]

    for p in range(xs):
        cols = []
        for i in range(ROWS):
            at = stride * (beam_rows * p + 2 * i)
            pair = [dop[at : at + m_count], dop[at + stride : at + stride + m_count]]
            cols.append(jnp.concatenate(pair, axis=0).astype(BF))
        outer = dot(f_t[...], jnp.concatenate(cols, axis=1))
        rows = []
        for i in range(ROWS):
            ar, ai = split(outer, i)
            rows.append(
                jnp.concatenate([ar * tr - ai * ti, ar * ti + ai * tr], axis=1).astype(BF)
            )
        inner = dot(jnp.concatenate(rows, axis=0), inf[...])
        rows = []
        for i in range(ROWS):
            cr, ci = cut(inner, i)
            rows.append(
                jnp.concatenate([cr * hr - ci * hi, cr * hi + ci * hr], axis=1).astype(BF)
            )
        inner = dot(jnp.concatenate(rows, axis=0), ini[...])
        cols = []
        for i in range(ROWS):
            er, ei = cut(inner, i)
            cols.append(
                jnp.concatenate([er * tr + ei * ti, ei * tr - er * ti], axis=0).astype(BF)
            )
        outer = dot(fi_t[...], jnp.concatenate(cols, axis=1))
        rows, powers = [], []
        for i in range(ROWS):
            re, im = split(outer, i)
            power = re * re + im * im
            slot = (p * ROWS + i) % edges.shape[0]
            edges[slot, ROWS : ROWS + m_count] = power
            before = edges[slot, ROWS - 1 : ROWS - 1 + m_count]
            after = edges[slot, ROWS + 1 : ROWS + 1 + m_count]
            side = jnp.where(iota((m_count, LANES), 1) < LANES // 2, after, before)
            rows.append(jnp.concatenate([power, side], axis=1).astype(BF))
            powers.append(power)
        noise = dot(jnp.concatenate(rows, axis=0), win[...])
        for i in range(ROWS):
            level = noise[m_count * i : m_count * i + m_count] + NOISE_FLOOR
            found = (powers[i] / level).astype(BF)
            for k in range(ys):
                send4[p, k, span * i : span * i + span] = found[span * k : span * k + span]
        for k in reversed(range(ys)):
            if p == xs - 1 and k == 0:
                recv4[me] = send4[p, y]
                continue
            to_y = lax.rem(y + k, ys)
            copy = plan(
                send4.at[p, to_y], recv4.at[me], s4.at[p, k], r4.at[me],
                {"range": to_y, "pulse": order[p]},
            )
            copy.start()
            fourth.append(copy)

    def place(i):
        for b in range(ROWS):
            turn[turn_row * b : turn_row * b + span] = recv4[
                i, span * b : span * b + span
            ].astype(F32)
        for t in range(span):
            out[i, :, LANES * t : LANES * t + LANES] = turn[pl.ds(t, ROWS, stride=turn_row)]

    def final_step(k, carry):
        i = lax.rem(me + k, count)

        @pl.when(k > 0)
        def _():
            plan(
                send4.at[0, 0], recv4.at[i], s4.at[0, 0], r4.at[i], {"chan": 3 - z}
            ).wait_recv()

        place(i)
        return carry

    lax.fori_loop(0, count, final_step, 0)
    for copy in fourth:
        copy.wait_send()

    @pl.when(is_edge)
    def _():
        loop(lambda c: raw(c).wait_send())

    @pl.when(is_hub)
    def _():
        def body(c):
            plan(
                sendp.at[:, lanes(c)], recvp.at[:, lanes(c)], sp.at[c], rp.at[c],
                {"chan": 3 - hub},
            ).wait_send()

        loop(body)

        def sprayed(c):
            plan(
                send2.at[pl.ds(0, both - 1), :, wide_lanes(c)],
                send2.at[pl.ds(0, both - 1), :, wide_lanes(c)],
                s2.at[c], r2.at[c], {"chan": edge},
            ).wait_send()

        loop(sprayed, 0, chunks // GROUP)


def shards_chain(signal, steering, spectrum):
    beams, chans = steering.shape[1], steering.shape[2]
    _, chan_own, pulse_own, gates = signal.shape
    zs, xs, ys = (lax.axis_size(a) for a in ("chan", "pulse", "range"))
    count = xs * ys
    full = gates * ys
    m_count = full // LANES
    pulses = pulse_own * xs
    depth = 2 * chan_own * pulse_own
    chunks = CHUNKS

    ms = np.arange(m_count)
    angle = 2.0 * np.pi * (np.outer(ms, ms) % m_count) / m_count
    co, si = np.cos(angle), np.sin(angle)
    outer_f = jnp.asarray(np.block([[co, si], [-si, co]]), BF)
    outer_i = jnp.asarray(np.block([[co, -si], [si, co]]), BF)
    ls = np.arange(LANES)
    times = LANES // m_count
    bins = (ls % m_count) * times + ls // m_count
    angle = 2.0 * np.pi * (np.outer(ls, bins) % LANES) / LANES
    co, si = np.cos(angle), np.sin(angle)
    inner_f = jnp.asarray(np.block([[co, -si], [si, co]]), BF)
    inner_i = jnp.asarray(np.block([[co.T, si.T], [-si.T, co.T]]), BF)
    angle = 2.0 * np.pi * np.outer(ms, ls) / full
    twiddle = jnp.asarray(np.stack([np.cos(angle), -np.sin(angle)]), F32)

    dst = np.arange(LANES)
    side = np.where(dst < LANES // 2, dst + LANES, dst - LANES)
    gap = np.abs(np.concatenate([dst, side])[:, None] - dst[None, :])
    window = jnp.asarray(((gap > GUARD) & (gap <= GUARD + TRAIN)) / (2.0 * TRAIN), BF)

    ids = np.arange(pulses)
    angle = (np.outer(ids, ids) % pulses) * (2.0 * np.pi / pulses)
    scale = 1.0 / math.sqrt(pulses)
    dr, di = np.cos(angle) * scale, -np.sin(angle) * scale
    table = np.stack([np.stack([dr, -di], -1), np.stack([di, dr], -1)])
    table = table.reshape(2, xs, pulse_own, xs, pulse_own, 2)
    table = table.transpose(1, 2, 0, 3, 5, 4).reshape(2 * pulses, 2 * pulses)
    table = jnp.asarray(table, BF)

    beam_rows = 2 * pulse_own
    vmem, dma = pltpu.VMEM, pltpu.SemaphoreType.DMA
    any_space = pl.BlockSpec(memory_space=pl.ANY)
    consts = (steering, spectrum, outer_f, outer_i, inner_f, inner_i, twiddle, table, window)
    return pl.pallas_call(
        functools.partial(chain_kernel, (zs, ys, xs, chunks)),
        out_shape=jax.ShapeDtypeStruct((count, pulse_own, gates), F32),
        in_specs=[any_space] * (1 + len(consts)),
        out_specs=pl.BlockSpec(memory_space=vmem),
        scratch_shapes=[vmem(a.shape, a.dtype) for a in consts]
        + [
            vmem((depth, gates), BF),
            vmem((depth, gates), BF),
            vmem((2 * count * beam_rows, gates), BF),
            vmem((2 * count * beam_rows, gates), BF),
            vmem((2 * count * beam_rows, gates), F32),
            vmem((2 * count, beam_rows, gates), BF),
            vmem((ys, xs * beam_rows, gates), BF),
            vmem((xs * beam_rows * (m_count + ROWS), LANES), F32),
            vmem((xs, ys, gates // LANES * pulse_own, LANES), BF),
            vmem((count, gates // LANES * pulse_own, LANES), BF),
            vmem((2, 2, 2 * count * beam_rows, depth), BF),
            vmem((2 * pulses, 2 * pulses), BF),
            vmem((2, m_count, LANES), F32),
            vmem((2, m_count, LANES), F32),
            vmem((2 * ROWS, m_count + 2 * ROWS, LANES), F32),
            vmem((pulse_own * (m_count // ys + ROWS), LANES), F32),
            dma((len(consts),)),
            dma((chunks,)),
            dma((chunks,)), dma((chunks,)),
            dma((chunks,)), dma((chunks,)),
            dma((chunks,)), dma((chunks,)),
            dma((xs, ys)), dma((count,)),
        ],
        compiler_params=pltpu.CompilerParams(
            collective_id=0, has_side_effects=True, vmem_limit_bytes=VM
        ),
        name="chain",
    )(*[
        pltpu.with_memory_space_constraint(v, pltpu.HBM)
        for v in (signal.reshape(depth, gates), *map(jnp.asarray, consts))
    ])


def shards(signal, steering, spectrum):
    zs, xs, ys = (lax.axis_size(a) for a in ("chan", "pulse", "range"))
    _, _, pulse_own, gates = signal.shape
    fits = (
        zs == 4
        and xs == 4
        and pulse_own == ROWS
        and steering.shape[1] == zs * xs * ys
        and gates * ys * 2 == LANES * LANES
        and gates % (CHUNKS * LANES) == 0
    )
    return (shards_chain if fits else shards_split)(signal, steering, spectrum)


def solution(mesh):
    in_specs = (P(None, "chan", "pulse", "range"), P(), P())
    out_specs = P("chan", "pulse", "range")
    return jax.shard_map(shards, mesh=mesh, in_specs=in_specs, out_specs=out_specs, check_vma=False)
```

```python
import functools
import math

import jax
import jax.numpy as jnp
import numpy as np
from jax import lax
from jax.experimental import pallas as pl
from jax.experimental.pallas import tpu as pltpu
from jax.sharding import PartitionSpec as P

GUARD = 4
TRAIN = 16
NOISE_FLOOR = 0.25
LANES = 128
ROWS = 8
CHUNKS = 16
LAG = 2
BF = jnp.bfloat16
F32 = jnp.float32
VM = 44 * 1024 * 1024


def dot(a, b):
    return jnp.dot(a, b, preferred_element_type=F32)


def doppler_table(count):
    ids = np.arange(count)
    angle = (np.outer(ids, ids) % count) * (2.0 * np.pi / count)
    scale = 1.0 / math.sqrt(count)
    return jnp.asarray(np.cos(angle) * scale, BF), jnp.asarray(-np.sin(angle) * scale, BF)


def expand(left_ids, left_tag, table, right_ids, right_tag):
    n, m = table.shape
    left = (jnp.asarray(left_ids, jnp.int32)[:, None] == jnp.arange(n)[None, :]).astype(BF)
    right = (jnp.arange(m)[:, None] == jnp.asarray(right_ids, jnp.int32)[None, :]).astype(BF)
    wide = dot(dot(left, table).astype(BF), right)
    same = jnp.asarray(left_tag, jnp.int32)[:, None] == jnp.asarray(right_tag, jnp.int32)[None, :]
    return jnp.where(same, wide, 0.0).astype(BF)


def grid_ids(*sizes):
    return [g.reshape(-1) for g in np.meshgrid(*[np.arange(s) for s in sizes], indexing="ij")]


def call(body, out_shape, name):
    return pl.pallas_call(
        body,
        out_shape=out_shape,
        compiler_params=pltpu.CompilerParams(vmem_limit_bytes=VM),
        name=name,
    )


def form_kernel(w_ref, x_ref, o_ref):
    o_ref[...] = dot(w_ref[...], x_ref[...]).astype(BF)


def range_kernel(blocks, x_ref, f_ref, fi_ref, t_ref, l_ref, li_ref, h_ref, o_ref):
    sources, rows, width = x_ref.shape
    per = width // LANES
    groups = rows // 16
    m_count = sources * per
    tile = []
    for g in range(groups):
        parts = [
            x_ref[s, 16 * g : 16 * g + 16, LANES * j : LANES * j + LANES]
            for s in range(sources)
            for j in range(per)
        ]
        tile.append(jnp.concatenate(parts, axis=0))
    outer = dot(f_ref[...], jnp.concatenate(tile, axis=1))
    tr, ti = t_ref[0], t_ref[1]
    hr, hi = h_ref[0], h_ref[1]
    back = []
    for g in range(groups):
        a = outer[:, LANES * g : LANES * g + LANES].reshape(m_count, 2, ROWS, LANES)
        ar, ai = a[:, 0], a[:, 1]
        b = jnp.concatenate([ar * tr - ai * ti, ar * ti + ai * tr], axis=-1)
        c = dot(b.reshape(m_count * ROWS, 2 * LANES).astype(BF), l_ref[...])
        c = c.reshape(m_count, ROWS, 2 * LANES)
        cr, ci = c[..., :LANES], c[..., LANES:]
        d = jnp.concatenate([cr * hr - ci * hi, cr * hi + ci * hr], axis=-1)
        e = dot(d.reshape(m_count * ROWS, 2 * LANES).astype(BF), li_ref[...])
        e = e.reshape(m_count, ROWS, 2 * LANES)
        er, ei = e[..., :LANES], e[..., LANES:]
        f = jnp.stack([er * tr + ei * ti, ei * tr - er * ti], axis=1)
        back.append(f.reshape(m_count * 16, LANES).astype(BF))
    y = dot(fi_ref[...], jnp.concatenate(back, axis=1)).astype(BF)
    span = m_count // blocks
    for d in range(blocks):
        for j in range(-1, span + 1):
            m = d * span + j
            for g in range(groups):
                if 0 <= m < m_count:
                    v = y[16 * m : 16 * m + 16, LANES * g : LANES * g + LANES]
                else:
                    v = jnp.zeros((16, LANES), BF)
                o_ref[d, 16 * g : 16 * g + 16, LANES * (j + 1) : LANES * (j + 2)] = v


def cfar_kernel(d_ref, x_ref, n_ref, o_ref):
    half = d_ref.shape[0] // 2
    mix = dot(d_ref[...], x_ref[...].reshape(d_ref.shape[1], x_ref.shape[-1]))
    re, im = mix[:half], mix[half:]
    power = re * re + im * im
    narrow = power.astype(BF)
    shape = o_ref.shape[:-1] + (LANES,)
    for j in range(o_ref.shape[-1] // LANES):
        noise = dot(narrow[:, LANES * j : LANES * (j + 3)], n_ref[...])
        own = power[:, LANES * (j + 1) : LANES * (j + 2)]
        found = (own / (noise + NOISE_FLOOR)).astype(BF)
        o_ref[..., LANES * j : LANES * j + LANES] = found.reshape(shape)


def cfar_only_kernel(p_ref, n_ref, o_ref):
    narrow = p_ref[...].astype(BF)
    for j in range(o_ref.shape[1] // LANES):
        noise = dot(narrow[:, LANES * j : LANES * (j + 3)], n_ref[...])
        own = p_ref[:, LANES * (j + 1) : LANES * (j + 2)]
        o_ref[:, LANES * j : LANES * j + LANES] = (own / (noise + NOISE_FLOOR)).astype(BF)


def place_kernel(x_ref, o_ref):
    count, _, width = x_ref.shape
    for s in range(count):
        o_ref[:, width * s : width * s + width] = x_ref[s].astype(F32)


def complex_rows(re, im):
    top = np.stack([re, -im], -1)
    low = np.stack([im, re], -1)
    return np.stack([top, low], 1).reshape(2 * re.shape[0], 2 * re.shape[1])


def shards_split(signal, steering, spectrum):
    beams, chans = steering.shape[1], steering.shape[2]
    _, chan_own, pulse_own, gates = signal.shape
    zs, xs, ys = (lax.axis_size(a) for a in ("chan", "pulse", "range"))
    beam_own = beams // zs
    part = pulse_own // ys
    full = gates * ys
    block = gates // zs
    m_count = full // LANES
    groups = beam_own * part // ROWS
    pulses = pulse_own * xs

    w_real, w_imag = steering[0], steering[1]
    weights = jnp.concatenate(
        [jnp.concatenate([w_real, -w_imag], 1), jnp.concatenate([w_imag, w_real], 1)], 0
    )
    dy, dz, gr, cp, it = grid_ids(ys, zs, groups, 2, ROWS)
    bp = gr * ROWS + it
    left = cp * beams + dz * beam_own + bp // part
    left_pulse = dy * part + bp % part
    sz, ci, ch, pi = grid_ids(zs, 2, chan_own, pulse_own)
    right = ci * chans + sz * chan_own + ch
    form = expand(left, left_pulse, weights, right, pi)

    ms = np.arange(m_count)
    angle = 2.0 * np.pi * (np.outer(ms, ms) % m_count) / m_count
    outer_f = jnp.asarray(complex_rows(np.cos(angle), -np.sin(angle)), BF)
    outer_i = jnp.asarray(complex_rows(np.cos(angle), np.sin(angle)), BF)
    mk, mc, mi = grid_ids(m_count, 2, ROWS)
    outer_f = expand(mk * 2 + mc, mi, outer_f, mk * 2 + mc, mi)
    outer_i = expand(mk * 2 + mc, mi, outer_i, mk * 2 + mc, mi)
    ls = np.arange(LANES)
    angle = 2.0 * np.pi * (np.outer(ls, ls) % LANES) / LANES
    co, si = np.cos(angle), np.sin(angle)
    inner_f = jnp.asarray(np.block([[co, -si], [si, co]]), BF)
    inner_i = jnp.asarray(np.block([[co, si], [-si, co]]), BF)
    angle = 2.0 * np.pi * np.outer(ms, ls) / full
    twiddle = jnp.asarray(np.stack([np.cos(angle), -np.sin(angle)]), F32)
    spread = (2, m_count, ROWS, LANES)
    twiddle = jnp.broadcast_to(twiddle[:, :, None, :], spread)
    response = jnp.swapaxes(spectrum.reshape(2, LANES, m_count), 1, 2) * (1.0 / full)
    response = jnp.broadcast_to(response[:, :, None, :], spread)

    samples = lax.all_to_all(signal, "chan", split_axis=3, concat_axis=0, tiled=True)
    samples = samples.reshape(zs * 2 * chan_own * pulse_own, block)
    rows = 2 * beam_own * part
    formed = call(
        form_kernel, jax.ShapeDtypeStruct((ys * zs * rows, block), BF), "form"
    )(form, samples).reshape(ys * zs, rows, block)
    formed = lax.all_to_all(formed, ("range", "chan"), split_axis=0, concat_axis=0, tiled=True)

    blocks = ys * xs
    own = full // blocks
    padded = own + 2 * LANES
    packed = call(
        functools.partial(range_kernel, blocks),
        jax.ShapeDtypeStruct((blocks, rows, padded), BF),
        "compress",
    )(formed, outer_f, outer_i, twiddle, inner_f, inner_i, response)
    columns = lax.all_to_all(packed, ("range", "pulse"), split_axis=0, concat_axis=0, tiled=True)

    src, dst = np.arange(3 * LANES)[:, None] - LANES, np.arange(LANES)[None, :]
    gap = np.abs(src - dst)
    window = jnp.asarray(((gap > GUARD) & (gap <= GUARD + TRAIN)) / (2.0 * TRAIN), BF)

    dr, di = doppler_table(pulses)
    out_shape = jax.ShapeDtypeStruct((pulses * beam_own, own), BF)
    if 2 * pulses * beam_own <= 1024:
        table = jnp.concatenate([jnp.concatenate([dr, -di], 1), jnp.concatenate([di, dr], 1)], 0)
        oc, oq, ob, of = grid_ids(2, xs, beam_own, pulse_own)
        sy, sx, gr, cp, it = grid_ids(ys, xs, groups, 2, ROWS)
        bp = gr * ROWS + it
        pulse = sx * pulse_own + sy * part + bp % part
        mix = expand(oc * pulses + oq * pulse_own + of, ob, table, cp * pulses + pulse, bp // part)
        found = call(cfar_kernel, out_shape, "cfar")(
            mix, columns.reshape(blocks * rows, padded), window
        )
    else:
        v = columns.reshape(ys, xs, groups, 2, ROWS // part, part, padded)
        v = jnp.transpose(v, (3, 2, 4, 1, 0, 5, 6)).reshape(2, beam_own, pulses, padded)

        def product(t, x):
            return jnp.einsum("fp,bpr->fbr", t, x, preferred_element_type=F32)

        re = product(dr, v[0]) - product(di, v[1])
        im = product(dr, v[1]) + product(di, v[0])
        power = (re * re + im * im).reshape(xs, pulse_own, beam_own, padded)
        power = jnp.swapaxes(power, 1, 2).reshape(pulses * beam_own, padded)
        found = call(cfar_only_kernel, out_shape, "cfar")(power, window)
    found = found.reshape(xs, beam_own * pulse_own, own)
    found = lax.all_to_all(found, "pulse", split_axis=0, concat_axis=0, tiled=True)
    out = call(
        place_kernel, jax.ShapeDtypeStruct((beam_own * pulse_own, gates), F32), "place"
    )(found)
    return out.reshape(beam_own, pulse_own, gates)


MESH = pl.DeviceIdType.MESH


def iota(shape, dim):
    return lax.broadcasted_iota(jnp.int32, shape, dim)


def pick(ids, other):
    return (ids == other).astype(F32).astype(BF)


def widen(row_ids, row_tags, table, col_ids, col_tags):
    n, m = table.shape
    r, c = row_ids.shape[0], col_ids.shape[1]
    wide = dot(pick(row_ids, iota((r, n), 1)), table).astype(BF)
    wide = dot(wide, pick(iota((m, c), 0), col_ids))
    return jnp.where(row_tags == col_tags, wide, 0.0).astype(BF)


def chain_kernel(
    sizes, sig, steer_h, spec_h, f_h, fi_h, inf_h, ini_h, tw_h, dop_h, win_h, out,
    steer, spec, f_t, fi_t, inf, ini, tw, dop_t, win,
    own1, recv1, sendp, recvp, acc, send2, recv2, recvx, dop, send4, recv4,
    wide_w, mix, resp, gates_t, edges, turn,
    const_sem, own_sem, s1, r1, sp, rp, s2, r2, sx, rx, s4, r4,
):
    zs, ys, xs, chunks = sizes
    depth, gates = own1.shape
    width = gates // chunks
    beams, chans = steer.shape[1], steer.shape[2]
    count = ys * xs
    beam_rows = send2.shape[1]
    m_count = tw.shape[1]
    span = m_count // ys
    stride = m_count + ROWS
    turn_row = span + ROWS
    z, y, x = (lax.axis_index(a) for a in ("chan", "range", "pulse"))
    me = y * xs + x
    half = lax.div(z, 2)
    hub, edge = 1 + half, 3 * half
    is_hub = z == hub
    is_edge = z == edge

    consts = [
        pltpu.make_async_copy(a, b, const_sem.at[i])
        for i, (a, b) in enumerate(
            zip(
                (steer_h, spec_h, f_h, fi_h, inf_h, ini_h, tw_h, dop_h, win_h),
                (steer, spec, f_t, fi_t, inf, ini, tw, dop_t, win),
            )
        )
    ]

    def lanes(c):
        return pl.ds(pl.multiple_of(c * width, LANES), width)

    def mine(c):
        return pltpu.make_async_copy(
            sig.at[:, lanes(c)], own1.at[:, lanes(c)], own_sem.at[c]
        )

    def loop(body, start=0, stop=chunks):
        def step(c, carry):
            body(c)
            return carry

        lax.fori_loop(start, stop, step, 0)

    both = 2 * count
    barrier = pltpu.get_barrier_semaphore()

    def greet(**target):
        pl.semaphore_signal(barrier, inc=1, device_id=target, device_id_type=MESH)

    @pl.when(is_hub)
    def _():
        greet(chan=edge)
        for k in range(1, count):
            to = lax.rem(me + k, count)
            greet(range=lax.div(to, xs), pulse=lax.rem(to, xs))
        greet(chan=3 - hub)
        loop(lambda c: mine(c).start())

    @pl.when(is_edge)
    def _():
        for k in range(count):
            to = lax.rem(me + k, count)
            greet(chan=hub, range=lax.div(to, xs), pulse=lax.rem(to, xs))
        pl.semaphore_wait(barrier, 1)

    for copy in consts:
        copy.start()

    def plan(src, dst, send, recv, target):
        return pltpu.make_async_remote_copy(
            src_ref=src, dst_ref=dst, send_sem=send, recv_sem=recv,
            device_id=target, device_id_type=MESH,
        )

    def raw(c):
        return plan(
            sig.at[:, lanes(c)], recv1.at[:, lanes(c)], s1.at[c], r1.at[c], {"chan": hub}
        )

    @pl.when(is_edge)
    def _():
        loop(lambda c: raw(c).start())

    for copy in consts:
        copy.wait()

    def tables():
        for i in range(2):
            for t in range(m_count):
                gates_t[i, t : t + 1] = spec[i : i + 1, LANES * t : LANES * t + LANES]
            turned = gates_t[i].T * (1.0 / (m_count * LANES))
            resp[i] = jnp.concatenate([turned[:m_count], turned[m_count:]], axis=1)
        edges[...] = jnp.zeros_like(edges)
        for i, g in enumerate(order):
            mix[beam_rows * i : beam_rows * i + beam_rows] = dop_t[
                pl.ds(pl.multiple_of(beam_rows * g, beam_rows), beam_rows)
            ]

    chip, core = lax.div(x, 2), lax.rem(x, 2)
    order = [2 * (1 - chip) + core, 2 * chip + 1 - core, 2 * (1 - chip) + 1 - core, x]

    hops = sorted(
        np.ndindex(2, ys, 2, 2), key=lambda k: -(4 * (k[0] + k[1] + k[2]) + k[3])
    )
    far_first = [
        (dz, lax.rem(y + dy, ys), 2 * lax.rem(chip + dx, 2) + lax.rem(core + dc, 2))
        for dz, dy, dx, dc in hops
        if (dz, dy, dx, dc) != (0, 0, 0, 0)
    ]

    def doppler(c, extra=False):
        tiles = width // LANES
        for i in range(ys):
            v = recv2[i, :, lanes(c)]
            if extra:
                v = (v.astype(F32) + recvx[i].astype(F32)).astype(BF)
            found = dot(mix[...], v)
            for t in range(tiles):
                m = i * (gates // LANES) + c * tiles + t
                dop[pl.ds(m, xs * beam_rows, stride=stride)] = found[
                    :, LANES * t : LANES * t + LANES
                ]

    last = chunks - 1

    def doppler_last():
        plan(recvx, recvx, sx.at[0], rx.at[0], {"chan": 3 - z}).wait_recv()
        doppler(last, True)

    @pl.when(is_hub)
    def _():
        re, im = steer[0], steer[1]
        weights = jnp.concatenate(
            [jnp.concatenate([re, -im], 1), jnp.concatenate([im, re], 1)], 0
        )
        pulse_own = beam_rows // 2
        chan_own = chans // zs
        r = iota((both * beam_rows, 1), 0)
        c = iota((1, depth), 1)
        row_tag, col_tag = lax.rem(r, pulse_own), lax.rem(c, pulse_own)
        r, c = lax.div(r, pulse_own), lax.div(c, pulse_own)
        dest = lax.div(r, 2)
        for i, h in enumerate((half, 1 - half)):
            at = jnp.where(dest < count, 1 + h, 3 * h)
            row = lax.rem(r, 2) * beams + at * count + lax.rem(dest, count)
            for j, source in enumerate((hub, edge)):
                col = lax.div(c, chan_own) * chans + source * chan_own + lax.rem(c, chan_own)
                wide_w[i, j] = widen(row, row_tag, weights, col, col_tag)

        part = count * beam_rows
        mine_rows = pl.ds(pl.multiple_of(beam_rows * x, beam_rows), beam_rows)

        def rows(u):
            return slice(part * u, part * u + part)

        def swap(c, u):
            at = pl.ds(part * u, part)
            return plan(
                sendp.at[at, lanes(c)], recvp.at[at, lanes(c)], sp.at[c, u], rp.at[c, u],
                {"chan": 3 - hub},
            )

        def form(c):
            mine(c).wait()
            raw(c).wait_recv()
            a, b = own1[:, lanes(c)], recv1[:, lanes(c)]
            for u in (1, 0):
                far = dot(wide_w[1, 0, rows(u)], a) + dot(wide_w[1, 1, rows(u)], b)
                sendp[rows(u), lanes(c)] = far.astype(BF)
                swap(c, u).start()
            acc[:, lanes(c)] = dot(wide_w[0, 0], a) + dot(wide_w[0, 1], b)

        def spray(c, u):
            for plane_to, to_y, to_x in far_first:
                if plane_to != u:
                    continue
                to = to_y * xs + to_x
                plan(
                    send2.at[plane_to * count + to, :, lanes(c)],
                    recv2.at[y, mine_rows, lanes(c)], s2.at[c], r2.at[c],
                    {"chan": edge if plane_to else hub, "range": to_y, "pulse": to_x},
                ).start()

        def finish(c):
            for u in (1, 0):
                swap(c, u).wait_recv()
                total = acc[rows(u), lanes(c)] + recvp[rows(u), lanes(c)].astype(F32)
                total = total.astype(BF).reshape(count, beam_rows, width)
                send2[count * u : count * u + count, :, lanes(c)] = total
                spray(c, u)
            recv2[y, mine_rows, lanes(c)] = send2[me, :, lanes(c)]

        def form_last():
            mine(last).wait()
            raw(last).wait_recv()
            a, b = own1[:, lanes(last)], recv1[:, lanes(last)]
            for u in (1, 0):
                far = dot(wide_w[1, 0, rows(u)], a) + dot(wide_w[1, 1, rows(u)], b)
                sendp[rows(u), lanes(last)] = far.astype(BF)
                for plane_to, to_y, to_x in far_first + [(0, y, x)]:
                    if plane_to != u:
                        continue
                    to = plane_to * count + to_y * xs + to_x
                    at = pl.ds(pl.multiple_of(beam_rows * to, beam_rows), beam_rows)
                    plan(
                        sendp.at[at, lanes(last)], recvx.at[y, mine_rows], sx.at[0], rx.at[0],
                        {
                            "chan": 3 - edge if plane_to else 3 - hub,
                            "range": to_y,
                            "pulse": to_x,
                        },
                    ).start()
            for u in (1, 0):
                total = dot(wide_w[0, 0, rows(u)], a) + dot(wide_w[0, 1, rows(u)], b)
                total = total.astype(BF).reshape(count, beam_rows, width)
                send2[count * u : count * u + count, :, lanes(last)] = total
                spray(last, u)
            recv2[y, mine_rows, lanes(last)] = send2[me, :, lanes(last)]

        def arrived(c):
            plan(
                send2.at[pl.ds(0, count - 1), :, lanes(c)],
                send2.at[pl.ds(0, count - 1), :, lanes(c)],
                s2.at[c], r2.at[c], {"chan": edge},
            ).wait_recv()

        pl.semaphore_wait(barrier, both)

        def body(c):
            form(c)

            @pl.when(c == 0)
            def _():
                tables()

            @pl.when(c >= LAG)
            def _():
                step(c - LAG)

        def step(c):
            finish(c)

            @pl.when(c >= 3)
            def _():
                arrived(c - 3)
                doppler(c - 3)

        loop(body, 0, last)
        loop(step, last - LAG, last - 1)
        form_last()
        step(last - 1)

        def rest(c):
            arrived(c)
            doppler(c)

        loop(rest, last - 3, last)
        arrived(last)
        doppler_last()

    @pl.when(is_edge)
    def _():
        tables()

        def arrived(c):
            plan(
                send2.at[pl.ds(0, count), :, lanes(c)],
                send2.at[pl.ds(0, count), :, lanes(c)],
                s2.at[c], r2.at[c], {"chan": hub},
            ).wait_recv()

        def body(c):
            arrived(c)
            doppler(c)

        loop(body, 0, last)
        arrived(last)
        doppler_last()

    tr, ti = tw[0], tw[1]
    hr, hi = resp[0], resp[1]
    fourth = []

    def split(v, i):
        w = v[:, LANES * i : LANES * i + LANES]
        return w[:m_count], w[m_count:]

    def cut(v, i):
        w = v[m_count * i : m_count * i + m_count]
        return w[:, :LANES], w[:, LANES:]

    for p in range(xs):
        cols = []
        for i in range(ROWS):
            at = stride * (beam_rows * p + 2 * i)
            pair = [dop[at : at + m_count], dop[at + stride : at + stride + m_count]]
            cols.append(jnp.concatenate(pair, axis=0).astype(BF))
        outer = dot(f_t[...], jnp.concatenate(cols, axis=1))
        rows = []
        for i in range(ROWS):
            ar, ai = split(outer, i)
            rows.append(
                jnp.concatenate([ar * tr - ai * ti, ar * ti + ai * tr], axis=1).astype(BF)
            )
        inner = dot(jnp.concatenate(rows, axis=0), inf[...])
        rows = []
        for i in range(ROWS):
            cr, ci = cut(inner, i)
            rows.append(
                jnp.concatenate([cr * hr - ci * hi, cr * hi + ci * hr], axis=1).astype(BF)
            )
        inner = dot(jnp.concatenate(rows, axis=0), ini[...])
        cols = []
        for i in range(ROWS):
            er, ei = cut(inner, i)
            cols.append(
                jnp.concatenate([er * tr + ei * ti, ei * tr - er * ti], axis=0).astype(BF)
            )
        outer = dot(fi_t[...], jnp.concatenate(cols, axis=1))
        rows, powers = [], []
        for i in range(ROWS):
            re, im = split(outer, i)
            power = re * re + im * im
            slot = (p * ROWS + i) % edges.shape[0]
            edges[slot, ROWS : ROWS + m_count] = power
            before = edges[slot, ROWS - 1 : ROWS - 1 + m_count]
            after = edges[slot, ROWS + 1 : ROWS + 1 + m_count]
            side = jnp.where(iota((m_count, LANES), 1) < LANES // 2, after, before)
            rows.append(jnp.concatenate([power, side], axis=1).astype(BF))
            powers.append(power)
        noise = dot(jnp.concatenate(rows, axis=0), win[...])
        for i in range(ROWS):
            level = noise[m_count * i : m_count * i + m_count] + NOISE_FLOOR
            found = (powers[i] / level).astype(BF)
            for k in range(ys):
                send4[p, k, span * i : span * i + span] = found[span * k : span * k + span]
        for k in reversed(range(ys)):
            if p == xs - 1 and k == 0:
                recv4[me] = send4[p, y]
                continue
            to_y = lax.rem(y + k, ys)
            copy = plan(
                send4.at[p, to_y], recv4.at[me], s4.at[p, k], r4.at[me],
                {"range": to_y, "pulse": order[p]},
            )
            copy.start()
            fourth.append(copy)

    def place(i):
        for b in range(ROWS):
            turn[turn_row * b : turn_row * b + span] = recv4[
                i, span * b : span * b + span
            ].astype(F32)
        for t in range(span):
            out[i, :, LANES * t : LANES * t + LANES] = turn[pl.ds(t, ROWS, stride=turn_row)]

    def final_step(k, carry):
        i = lax.rem(me + k, count)

        @pl.when(k > 0)
        def _():
            plan(
                send4.at[0, 0], recv4.at[i], s4.at[0, 0], r4.at[i], {"chan": 3 - z}
            ).wait_recv()

        place(i)
        return carry

    lax.fori_loop(0, count, final_step, 0)
    for copy in fourth:
        copy.wait_send()

    @pl.when(is_edge)
    def _():
        loop(lambda c: raw(c).wait_send())

    @pl.when(is_hub)
    def _():
        def body(c):
            for u in range(2):
                at = pl.ds(count * beam_rows * u, count * beam_rows)
                plan(
                    sendp.at[at, lanes(c)], recvp.at[at, lanes(c)], sp.at[c, u], rp.at[c, u],
                    {"chan": 3 - hub},
                ).wait_send()

        loop(body, 0, last)
        plan(
            sendp.at[:, lanes(last)], sendp.at[:, lanes(last)], sx.at[0], rx.at[0],
            {"chan": 3 - hub},
        ).wait_send()

        def sprayed(c):
            plan(
                send2.at[pl.ds(0, both - 1), :, lanes(c)],
                send2.at[pl.ds(0, both - 1), :, lanes(c)],
                s2.at[c], r2.at[c], {"chan": edge},
            ).wait_send()

        loop(sprayed, 0, chunks)


def shards_chain(signal, steering, spectrum):
    beams, chans = steering.shape[1], steering.shape[2]
    _, chan_own, pulse_own, gates = signal.shape
    zs, xs, ys = (lax.axis_size(a) for a in ("chan", "pulse", "range"))
    count = xs * ys
    full = gates * ys
    m_count = full // LANES
    pulses = pulse_own * xs
    depth = 2 * chan_own * pulse_own
    chunks = CHUNKS

    ms = np.arange(m_count)
    angle = 2.0 * np.pi * (np.outer(ms, ms) % m_count) / m_count
    co, si = np.cos(angle), np.sin(angle)
    outer_f = jnp.asarray(np.block([[co, si], [-si, co]]), BF)
    outer_i = jnp.asarray(np.block([[co, -si], [si, co]]), BF)
    ls = np.arange(LANES)
    times = LANES // m_count
    bins = (ls % m_count) * times + ls // m_count
    angle = 2.0 * np.pi * (np.outer(ls, bins) % LANES) / LANES
    co, si = np.cos(angle), np.sin(angle)
    inner_f = jnp.asarray(np.block([[co, -si], [si, co]]), BF)
    inner_i = jnp.asarray(np.block([[co.T, si.T], [-si.T, co.T]]), BF)
    angle = 2.0 * np.pi * np.outer(ms, ls) / full
    twiddle = jnp.asarray(np.stack([np.cos(angle), -np.sin(angle)]), F32)

    dst = np.arange(LANES)
    side = np.where(dst < LANES // 2, dst + LANES, dst - LANES)
    gap = np.abs(np.concatenate([dst, side])[:, None] - dst[None, :])
    window = jnp.asarray(((gap > GUARD) & (gap <= GUARD + TRAIN)) / (2.0 * TRAIN), BF)

    ids = np.arange(pulses)
    angle = (np.outer(ids, ids) % pulses) * (2.0 * np.pi / pulses)
    scale = 1.0 / math.sqrt(pulses)
    dr, di = np.cos(angle) * scale, -np.sin(angle) * scale
    table = np.stack([np.stack([dr, -di], -1), np.stack([di, dr], -1)])
    table = table.reshape(2, xs, pulse_own, xs, pulse_own, 2)
    table = table.transpose(1, 2, 0, 3, 5, 4).reshape(2 * pulses, 2 * pulses)
    table = jnp.asarray(table, BF)

    beam_rows = 2 * pulse_own
    vmem, dma = pltpu.VMEM, pltpu.SemaphoreType.DMA
    any_space = pl.BlockSpec(memory_space=pl.ANY)
    consts = (steering, spectrum, outer_f, outer_i, inner_f, inner_i, twiddle, table, window)
    return pl.pallas_call(
        functools.partial(chain_kernel, (zs, ys, xs, chunks)),
        out_shape=jax.ShapeDtypeStruct((count, pulse_own, gates), F32),
        in_specs=[any_space] * (1 + len(consts)),
        out_specs=pl.BlockSpec(memory_space=vmem),
        scratch_shapes=[vmem(a.shape, a.dtype) for a in consts]
        + [
            vmem((depth, gates), BF),
            vmem((depth, gates), BF),
            vmem((2 * count * beam_rows, gates), BF),
            vmem((2 * count * beam_rows, gates), BF),
            vmem((2 * count * beam_rows, gates), F32),
            vmem((2 * count, beam_rows, gates), BF),
            vmem((ys, xs * beam_rows, gates), BF),
            vmem((ys, xs * beam_rows, gates // chunks), BF),
            vmem((xs * beam_rows * (m_count + ROWS), LANES), F32),
            vmem((xs, ys, gates // LANES * pulse_own, LANES), BF),
            vmem((count, gates // LANES * pulse_own, LANES), BF),
            vmem((2, 2, 2 * count * beam_rows, depth), BF),
            vmem((2 * pulses, 2 * pulses), BF),
            vmem((2, m_count, LANES), F32),
            vmem((2, m_count, LANES), F32),
            vmem((2 * ROWS, m_count + 2 * ROWS, LANES), F32),
            vmem((pulse_own * (m_count // ys + ROWS), LANES), F32),
            dma((len(consts),)),
            dma((chunks,)),
            dma((chunks,)), dma((chunks,)),
            dma((chunks, 2)), dma((chunks, 2)),
            dma((chunks,)), dma((chunks,)),
            dma((1,)), dma((1,)),
            dma((xs, ys)), dma((count,)),
        ],
        compiler_params=pltpu.CompilerParams(
            collective_id=0, has_side_effects=True, vmem_limit_bytes=VM
        ),
        name="chain",
    )(*[
        pltpu.with_memory_space_constraint(v, pltpu.HBM)
        for v in (signal.reshape(depth, gates), *map(jnp.asarray, consts))
    ])


def shards(signal, steering, spectrum):
    zs, xs, ys = (lax.axis_size(a) for a in ("chan", "pulse", "range"))
    _, _, pulse_own, gates = signal.shape
    fits = (
        zs == 4
        and xs == 4
        and pulse_own == ROWS
        and steering.shape[1] == zs * xs * ys
        and gates * ys * 2 == LANES * LANES
        and gates % (CHUNKS * LANES) == 0
    )
    return (shards_chain if fits else shards_split)(signal, steering, spectrum)


def solution(mesh):
    in_specs = (P(None, "chan", "pulse", "range"), P(), P())
    out_specs = P("chan", "pulse", "range")
    return jax.shard_map(shards, mesh=mesh, in_specs=in_specs, out_specs=out_specs, check_vma=False)
```

```python
import functools
import math

import jax
import jax.numpy as jnp
import numpy as np
from jax import lax
from jax.experimental import pallas as pl
from jax.experimental.pallas import tpu as pltpu
from jax.sharding import PartitionSpec as P

GUARD = 4
TRAIN = 16
NOISE_FLOOR = 0.25
LANES = 128
ROWS = 8
CHUNKS = 16
LAG = 2
DIRECT = 2
BF = jnp.bfloat16
F32 = jnp.float32
VM = 44 * 1024 * 1024


def dot(a, b):
    return jnp.dot(a, b, preferred_element_type=F32)


def doppler_table(count):
    ids = np.arange(count)
    angle = (np.outer(ids, ids) % count) * (2.0 * np.pi / count)
    scale = 1.0 / math.sqrt(count)
    return jnp.asarray(np.cos(angle) * scale, BF), jnp.asarray(-np.sin(angle) * scale, BF)


def expand(left_ids, left_tag, table, right_ids, right_tag):
    n, m = table.shape
    left = (jnp.asarray(left_ids, jnp.int32)[:, None] == jnp.arange(n)[None, :]).astype(BF)
    right = (jnp.arange(m)[:, None] == jnp.asarray(right_ids, jnp.int32)[None, :]).astype(BF)
    wide = dot(dot(left, table).astype(BF), right)
    same = jnp.asarray(left_tag, jnp.int32)[:, None] == jnp.asarray(right_tag, jnp.int32)[None, :]
    return jnp.where(same, wide, 0.0).astype(BF)


def grid_ids(*sizes):
    return [g.reshape(-1) for g in np.meshgrid(*[np.arange(s) for s in sizes], indexing="ij")]


def call(body, out_shape, name):
    return pl.pallas_call(
        body,
        out_shape=out_shape,
        compiler_params=pltpu.CompilerParams(vmem_limit_bytes=VM),
        name=name,
    )


def form_kernel(w_ref, x_ref, o_ref):
    o_ref[...] = dot(w_ref[...], x_ref[...]).astype(BF)


def range_kernel(blocks, x_ref, f_ref, fi_ref, t_ref, l_ref, li_ref, h_ref, o_ref):
    sources, rows, width = x_ref.shape
    per = width // LANES
    groups = rows // 16
    m_count = sources * per
    tile = []
    for g in range(groups):
        parts = [
            x_ref[s, 16 * g : 16 * g + 16, LANES * j : LANES * j + LANES]
            for s in range(sources)
            for j in range(per)
        ]
        tile.append(jnp.concatenate(parts, axis=0))
    outer = dot(f_ref[...], jnp.concatenate(tile, axis=1))
    tr, ti = t_ref[0], t_ref[1]
    hr, hi = h_ref[0], h_ref[1]
    back = []
    for g in range(groups):
        a = outer[:, LANES * g : LANES * g + LANES].reshape(m_count, 2, ROWS, LANES)
        ar, ai = a[:, 0], a[:, 1]
        b = jnp.concatenate([ar * tr - ai * ti, ar * ti + ai * tr], axis=-1)
        c = dot(b.reshape(m_count * ROWS, 2 * LANES).astype(BF), l_ref[...])
        c = c.reshape(m_count, ROWS, 2 * LANES)
        cr, ci = c[..., :LANES], c[..., LANES:]
        d = jnp.concatenate([cr * hr - ci * hi, cr * hi + ci * hr], axis=-1)
        e = dot(d.reshape(m_count * ROWS, 2 * LANES).astype(BF), li_ref[...])
        e = e.reshape(m_count, ROWS, 2 * LANES)
        er, ei = e[..., :LANES], e[..., LANES:]
        f = jnp.stack([er * tr + ei * ti, ei * tr - er * ti], axis=1)
        back.append(f.reshape(m_count * 16, LANES).astype(BF))
    y = dot(fi_ref[...], jnp.concatenate(back, axis=1)).astype(BF)
    span = m_count // blocks
    for d in range(blocks):
        for j in range(-1, span + 1):
            m = d * span + j
            for g in range(groups):
                if 0 <= m < m_count:
                    v = y[16 * m : 16 * m + 16, LANES * g : LANES * g + LANES]
                else:
                    v = jnp.zeros((16, LANES), BF)
                o_ref[d, 16 * g : 16 * g + 16, LANES * (j + 1) : LANES * (j + 2)] = v


def cfar_kernel(d_ref, x_ref, n_ref, o_ref):
    half = d_ref.shape[0] // 2
    mix = dot(d_ref[...], x_ref[...].reshape(d_ref.shape[1], x_ref.shape[-1]))
    re, im = mix[:half], mix[half:]
    power = re * re + im * im
    narrow = power.astype(BF)
    shape = o_ref.shape[:-1] + (LANES,)
    for j in range(o_ref.shape[-1] // LANES):
        noise = dot(narrow[:, LANES * j : LANES * (j + 3)], n_ref[...])
        own = power[:, LANES * (j + 1) : LANES * (j + 2)]
        found = (own / (noise + NOISE_FLOOR)).astype(BF)
        o_ref[..., LANES * j : LANES * j + LANES] = found.reshape(shape)


def cfar_only_kernel(p_ref, n_ref, o_ref):
    narrow = p_ref[...].astype(BF)
    for j in range(o_ref.shape[1] // LANES):
        noise = dot(narrow[:, LANES * j : LANES * (j + 3)], n_ref[...])
        own = p_ref[:, LANES * (j + 1) : LANES * (j + 2)]
        o_ref[:, LANES * j : LANES * j + LANES] = (own / (noise + NOISE_FLOOR)).astype(BF)


def place_kernel(x_ref, o_ref):
    count, _, width = x_ref.shape
    for s in range(count):
        o_ref[:, width * s : width * s + width] = x_ref[s].astype(F32)


def complex_rows(re, im):
    top = np.stack([re, -im], -1)
    low = np.stack([im, re], -1)
    return np.stack([top, low], 1).reshape(2 * re.shape[0], 2 * re.shape[1])


def shards_split(signal, steering, spectrum):
    beams, chans = steering.shape[1], steering.shape[2]
    _, chan_own, pulse_own, gates = signal.shape
    zs, xs, ys = (lax.axis_size(a) for a in ("chan", "pulse", "range"))
    beam_own = beams // zs
    part = pulse_own // ys
    full = gates * ys
    block = gates // zs
    m_count = full // LANES
    groups = beam_own * part // ROWS
    pulses = pulse_own * xs

    w_real, w_imag = steering[0], steering[1]
    weights = jnp.concatenate(
        [jnp.concatenate([w_real, -w_imag], 1), jnp.concatenate([w_imag, w_real], 1)], 0
    )
    dy, dz, gr, cp, it = grid_ids(ys, zs, groups, 2, ROWS)
    bp = gr * ROWS + it
    left = cp * beams + dz * beam_own + bp // part
    left_pulse = dy * part + bp % part
    sz, ci, ch, pi = grid_ids(zs, 2, chan_own, pulse_own)
    right = ci * chans + sz * chan_own + ch
    form = expand(left, left_pulse, weights, right, pi)

    ms = np.arange(m_count)
    angle = 2.0 * np.pi * (np.outer(ms, ms) % m_count) / m_count
    outer_f = jnp.asarray(complex_rows(np.cos(angle), -np.sin(angle)), BF)
    outer_i = jnp.asarray(complex_rows(np.cos(angle), np.sin(angle)), BF)
    mk, mc, mi = grid_ids(m_count, 2, ROWS)
    outer_f = expand(mk * 2 + mc, mi, outer_f, mk * 2 + mc, mi)
    outer_i = expand(mk * 2 + mc, mi, outer_i, mk * 2 + mc, mi)
    ls = np.arange(LANES)
    angle = 2.0 * np.pi * (np.outer(ls, ls) % LANES) / LANES
    co, si = np.cos(angle), np.sin(angle)
    inner_f = jnp.asarray(np.block([[co, -si], [si, co]]), BF)
    inner_i = jnp.asarray(np.block([[co, si], [-si, co]]), BF)
    angle = 2.0 * np.pi * np.outer(ms, ls) / full
    twiddle = jnp.asarray(np.stack([np.cos(angle), -np.sin(angle)]), F32)
    spread = (2, m_count, ROWS, LANES)
    twiddle = jnp.broadcast_to(twiddle[:, :, None, :], spread)
    response = jnp.swapaxes(spectrum.reshape(2, LANES, m_count), 1, 2) * (1.0 / full)
    response = jnp.broadcast_to(response[:, :, None, :], spread)

    samples = lax.all_to_all(signal, "chan", split_axis=3, concat_axis=0, tiled=True)
    samples = samples.reshape(zs * 2 * chan_own * pulse_own, block)
    rows = 2 * beam_own * part
    formed = call(
        form_kernel, jax.ShapeDtypeStruct((ys * zs * rows, block), BF), "form"
    )(form, samples).reshape(ys * zs, rows, block)
    formed = lax.all_to_all(formed, ("range", "chan"), split_axis=0, concat_axis=0, tiled=True)

    blocks = ys * xs
    own = full // blocks
    padded = own + 2 * LANES
    packed = call(
        functools.partial(range_kernel, blocks),
        jax.ShapeDtypeStruct((blocks, rows, padded), BF),
        "compress",
    )(formed, outer_f, outer_i, twiddle, inner_f, inner_i, response)
    columns = lax.all_to_all(packed, ("range", "pulse"), split_axis=0, concat_axis=0, tiled=True)

    src, dst = np.arange(3 * LANES)[:, None] - LANES, np.arange(LANES)[None, :]
    gap = np.abs(src - dst)
    window = jnp.asarray(((gap > GUARD) & (gap <= GUARD + TRAIN)) / (2.0 * TRAIN), BF)

    dr, di = doppler_table(pulses)
    out_shape = jax.ShapeDtypeStruct((pulses * beam_own, own), BF)
    if 2 * pulses * beam_own <= 1024:
        table = jnp.concatenate([jnp.concatenate([dr, -di], 1), jnp.concatenate([di, dr], 1)], 0)
        oc, oq, ob, of = grid_ids(2, xs, beam_own, pulse_own)
        sy, sx, gr, cp, it = grid_ids(ys, xs, groups, 2, ROWS)
        bp = gr * ROWS + it
        pulse = sx * pulse_own + sy * part + bp % part
        mix = expand(oc * pulses + oq * pulse_own + of, ob, table, cp * pulses + pulse, bp // part)
        found = call(cfar_kernel, out_shape, "cfar")(
            mix, columns.reshape(blocks * rows, padded), window
        )
    else:
        v = columns.reshape(ys, xs, groups, 2, ROWS // part, part, padded)
        v = jnp.transpose(v, (3, 2, 4, 1, 0, 5, 6)).reshape(2, beam_own, pulses, padded)

        def product(t, x):
            return jnp.einsum("fp,bpr->fbr", t, x, preferred_element_type=F32)

        re = product(dr, v[0]) - product(di, v[1])
        im = product(dr, v[1]) + product(di, v[0])
        power = (re * re + im * im).reshape(xs, pulse_own, beam_own, padded)
        power = jnp.swapaxes(power, 1, 2).reshape(pulses * beam_own, padded)
        found = call(cfar_only_kernel, out_shape, "cfar")(power, window)
    found = found.reshape(xs, beam_own * pulse_own, own)
    found = lax.all_to_all(found, "pulse", split_axis=0, concat_axis=0, tiled=True)
    out = call(
        place_kernel, jax.ShapeDtypeStruct((beam_own * pulse_own, gates), F32), "place"
    )(found)
    return out.reshape(beam_own, pulse_own, gates)


MESH = pl.DeviceIdType.MESH


def iota(shape, dim):
    return lax.broadcasted_iota(jnp.int32, shape, dim)


def pick(ids, other):
    return (ids == other).astype(F32).astype(BF)


def widen(row_ids, row_tags, table, col_ids, col_tags):
    n, m = table.shape
    r, c = row_ids.shape[0], col_ids.shape[1]
    wide = dot(pick(row_ids, iota((r, n), 1)), table).astype(BF)
    wide = dot(wide, pick(iota((m, c), 0), col_ids))
    return jnp.where(row_tags == col_tags, wide, 0.0).astype(BF)


def chain_kernel(
    sizes, sig, steer_h, spec_h, f_h, fi_h, inf_h, ini_h, tw_h, dop_h, win_h, out,
    steer, spec, f_t, fi_t, inf, ini, tw, dop_t, win,
    own1, recv1, sendp, recvp, acc, send2, recv2, recvx, dop, send4, recv4,
    wide_w, mix, resp, gates_t, edges, turn,
    const_sem, own_sem, s1, r1, sp, rp, s2, r2, sx, rx, s4, r4,
):
    zs, ys, xs, chunks = sizes
    depth, gates = own1.shape
    width = gates // chunks
    beams, chans = steer.shape[1], steer.shape[2]
    count = ys * xs
    beam_rows = send2.shape[1]
    m_count = tw.shape[1]
    span = m_count // ys
    stride = m_count + ROWS
    turn_row = span + ROWS
    z, y, x = (lax.axis_index(a) for a in ("chan", "range", "pulse"))
    me = y * xs + x
    half = lax.div(z, 2)
    hub, edge = 1 + half, 3 * half
    is_hub = z == hub
    is_edge = z == edge

    consts = [
        pltpu.make_async_copy(a, b, const_sem.at[i])
        for i, (a, b) in enumerate(
            zip(
                (steer_h, spec_h, f_h, fi_h, inf_h, ini_h, tw_h, dop_h, win_h),
                (steer, spec, f_t, fi_t, inf, ini, tw, dop_t, win),
            )
        )
    ]

    def lanes(c):
        return pl.ds(pl.multiple_of(c * width, LANES), width)

    def mine(c):
        return pltpu.make_async_copy(
            sig.at[:, lanes(c)], own1.at[:, lanes(c)], own_sem.at[c]
        )

    def loop(body, start=0, stop=chunks):
        def step(c, carry):
            body(c)
            return carry

        lax.fori_loop(start, stop, step, 0)

    both = 2 * count
    barrier = pltpu.get_barrier_semaphore()

    def greet(**target):
        pl.semaphore_signal(barrier, inc=1, device_id=target, device_id_type=MESH)

    @pl.when(is_hub)
    def _():
        greet(chan=edge)
        for k in range(1, count):
            to = lax.rem(me + k, count)
            greet(range=lax.div(to, xs), pulse=lax.rem(to, xs))
        greet(chan=3 - hub)
        loop(lambda c: mine(c).start())

    @pl.when(is_edge)
    def _():
        for k in range(count):
            to = lax.rem(me + k, count)
            greet(chan=hub, range=lax.div(to, xs), pulse=lax.rem(to, xs))
        pl.semaphore_wait(barrier, 1)

    for copy in consts:
        copy.start()

    def plan(src, dst, send, recv, target):
        return pltpu.make_async_remote_copy(
            src_ref=src, dst_ref=dst, send_sem=send, recv_sem=recv,
            device_id=target, device_id_type=MESH,
        )

    def raw(c):
        return plan(
            sig.at[:, lanes(c)], recv1.at[:, lanes(c)], s1.at[c], r1.at[c], {"chan": hub}
        )

    @pl.when(is_edge)
    def _():
        loop(lambda c: raw(c).start())

    for copy in consts:
        copy.wait()

    def tables():
        for i in range(2):
            for t in range(m_count):
                gates_t[i, t : t + 1] = spec[i : i + 1, LANES * t : LANES * t + LANES]
            turned = gates_t[i].T * (1.0 / (m_count * LANES))
            resp[i] = jnp.concatenate([turned[:m_count], turned[m_count:]], axis=1)
        edges[...] = jnp.zeros_like(edges)
        for i, g in enumerate(order):
            mix[beam_rows * i : beam_rows * i + beam_rows] = dop_t[
                pl.ds(pl.multiple_of(beam_rows * g, beam_rows), beam_rows)
            ]

    chip, core = lax.div(x, 2), lax.rem(x, 2)
    order = [2 * (1 - chip) + core, 2 * chip + 1 - core, 2 * (1 - chip) + 1 - core, x]

    hops = sorted(
        np.ndindex(2, ys, 2, 2), key=lambda k: -(4 * (k[0] + k[1] + k[2]) + k[3])
    )
    far_first = [
        (dz, lax.rem(y + dy, ys), 2 * lax.rem(chip + dx, 2) + lax.rem(core + dc, 2))
        for dz, dy, dx, dc in hops
        if (dz, dy, dx, dc) != (0, 0, 0, 0)
    ]

    def doppler(c, extra=False):
        tiles = width // LANES
        for i in range(ys):
            v = recv2[i, :, lanes(c)]
            if extra:
                v = (v.astype(F32) + recvx[c - first, i].astype(F32)).astype(BF)
            found = dot(mix[...], v)
            for t in range(tiles):
                m = i * (gates // LANES) + c * tiles + t
                dop[pl.ds(m, xs * beam_rows, stride=stride)] = found[
                    :, LANES * t : LANES * t + LANES
                ]

    first = chunks - DIRECT

    def doppler_both(c):
        k = c - first
        plan(recvx.at[k], recvx.at[k], sx.at[k], rx.at[k], {"chan": 3 - z}).wait_recv()
        doppler(c, True)

    @pl.when(is_hub)
    def _():
        re, im = steer[0], steer[1]
        weights = jnp.concatenate(
            [jnp.concatenate([re, -im], 1), jnp.concatenate([im, re], 1)], 0
        )
        pulse_own = beam_rows // 2
        chan_own = chans // zs
        r = iota((both * beam_rows, 1), 0)
        c = iota((1, depth), 1)
        row_tag, col_tag = lax.rem(r, pulse_own), lax.rem(c, pulse_own)
        r, c = lax.div(r, pulse_own), lax.div(c, pulse_own)
        dest = lax.div(r, 2)
        for i, h in enumerate((half, 1 - half)):
            at = jnp.where(dest < count, 1 + h, 3 * h)
            row = lax.rem(r, 2) * beams + at * count + lax.rem(dest, count)
            for j, source in enumerate((hub, edge)):
                col = lax.div(c, chan_own) * chans + source * chan_own + lax.rem(c, chan_own)
                wide_w[i, j] = widen(row, row_tag, weights, col, col_tag)

        part = count * beam_rows
        mine_rows = pl.ds(pl.multiple_of(beam_rows * x, beam_rows), beam_rows)

        def rows(u):
            return slice(part * u, part * u + part)

        def swap(c, u):
            at = pl.ds(part * u, part)
            return plan(
                sendp.at[at, lanes(c)], recvp.at[at, lanes(c)], sp.at[c, u], rp.at[c, u],
                {"chan": 3 - hub},
            )

        def form(c):
            mine(c).wait()
            raw(c).wait_recv()
            a, b = own1[:, lanes(c)], recv1[:, lanes(c)]
            for u in (1, 0):
                far = dot(wide_w[1, 0, rows(u)], a) + dot(wide_w[1, 1, rows(u)], b)
                sendp[rows(u), lanes(c)] = far.astype(BF)
                swap(c, u).start()
            acc[:, lanes(c)] = dot(wide_w[0, 0], a) + dot(wide_w[0, 1], b)

        def spray(c, u):
            for plane_to, to_y, to_x in far_first:
                if plane_to != u:
                    continue
                to = to_y * xs + to_x
                plan(
                    send2.at[plane_to * count + to, :, lanes(c)],
                    recv2.at[y, mine_rows, lanes(c)], s2.at[c], r2.at[c],
                    {"chan": edge if plane_to else hub, "range": to_y, "pulse": to_x},
                ).start()

        def finish(c):
            for u in (1, 0):
                swap(c, u).wait_recv()
                total = acc[rows(u), lanes(c)] + recvp[rows(u), lanes(c)].astype(F32)
                total = total.astype(BF).reshape(count, beam_rows, width)
                send2[count * u : count * u + count, :, lanes(c)] = total
                spray(c, u)
            recv2[y, mine_rows, lanes(c)] = send2[me, :, lanes(c)]

        def form_both(c):
            mine(c).wait()
            raw(c).wait_recv()
            a, b = own1[:, lanes(c)], recv1[:, lanes(c)]
            for u in (1, 0):
                far = dot(wide_w[1, 0, rows(u)], a) + dot(wide_w[1, 1, rows(u)], b)
                sendp[rows(u), lanes(c)] = far.astype(BF)
                for plane_to, to_y, to_x in far_first + [(0, y, x)]:
                    if plane_to != u:
                        continue
                    to = plane_to * count + to_y * xs + to_x
                    at = pl.ds(pl.multiple_of(beam_rows * to, beam_rows), beam_rows)
                    plan(
                        sendp.at[at, lanes(c)], recvx.at[c - first, y, mine_rows], sx.at[c - first], rx.at[c - first],
                        {
                            "chan": 3 - edge if plane_to else 3 - hub,
                            "range": to_y,
                            "pulse": to_x,
                        },
                    ).start()
            for u in (1, 0):
                total = dot(wide_w[0, 0, rows(u)], a) + dot(wide_w[0, 1, rows(u)], b)
                total = total.astype(BF).reshape(count, beam_rows, width)
                send2[count * u : count * u + count, :, lanes(c)] = total
                spray(c, u)
            recv2[y, mine_rows, lanes(c)] = send2[me, :, lanes(c)]

        def arrived(c):
            plan(
                send2.at[pl.ds(0, count - 1), :, lanes(c)],
                send2.at[pl.ds(0, count - 1), :, lanes(c)],
                s2.at[c], r2.at[c], {"chan": edge},
            ).wait_recv()

        pl.semaphore_wait(barrier, both)

        def body(c):
            form(c)

            @pl.when(c == 0)
            def _():
                tables()

            @pl.when(c >= LAG)
            def _():
                step(c - LAG)

        def step(c):
            finish(c)

            @pl.when(c >= 3)
            def _():
                arrived(c - 3)
                doppler(c - 3)

        loop(body, 0, first)
        step(first - 2)

        def final(c):
            form_both(c)

            @pl.when(c == first)
            def _():
                step(first - 1)

        loop(final, first)

        def rest(c):
            arrived(c)
            doppler(c)

        loop(rest, first - 3, first)

        def rest_both(c):
            arrived(c)
            doppler_both(c)

        loop(rest_both, first)

    @pl.when(is_edge)
    def _():
        tables()

        def arrived(c):
            plan(
                send2.at[pl.ds(0, count), :, lanes(c)],
                send2.at[pl.ds(0, count), :, lanes(c)],
                s2.at[c], r2.at[c], {"chan": hub},
            ).wait_recv()

        def body(c):
            arrived(c)
            doppler(c)

        loop(body, 0, first)

        def body_both(c):
            arrived(c)
            doppler_both(c)

        loop(body_both, first)

    tr, ti = tw[0], tw[1]
    hr, hi = resp[0], resp[1]
    fourth = []

    def split(v, i):
        w = v[:, LANES * i : LANES * i + LANES]
        return w[:m_count], w[m_count:]

    def cut(v, i):
        w = v[m_count * i : m_count * i + m_count]
        return w[:, :LANES], w[:, LANES:]

    for p in range(xs):
        cols = []
        for i in range(ROWS):
            at = stride * (beam_rows * p + 2 * i)
            pair = [dop[at : at + m_count], dop[at + stride : at + stride + m_count]]
            cols.append(jnp.concatenate(pair, axis=0).astype(BF))
        outer = dot(f_t[...], jnp.concatenate(cols, axis=1))
        rows = []
        for i in range(ROWS):
            ar, ai = split(outer, i)
            rows.append(
                jnp.concatenate([ar * tr - ai * ti, ar * ti + ai * tr], axis=1).astype(BF)
            )
        inner = dot(jnp.concatenate(rows, axis=0), inf[...])
        rows = []
        for i in range(ROWS):
            cr, ci = cut(inner, i)
            rows.append(
                jnp.concatenate([cr * hr - ci * hi, cr * hi + ci * hr], axis=1).astype(BF)
            )
        inner = dot(jnp.concatenate(rows, axis=0), ini[...])
        cols = []
        for i in range(ROWS):
            er, ei = cut(inner, i)
            cols.append(
                jnp.concatenate([er * tr + ei * ti, ei * tr - er * ti], axis=0).astype(BF)
            )
        outer = dot(fi_t[...], jnp.concatenate(cols, axis=1))
        rows, powers = [], []
        for i in range(ROWS):
            re, im = split(outer, i)
            power = re * re + im * im
            slot = (p * ROWS + i) % edges.shape[0]
            edges[slot, ROWS : ROWS + m_count] = power
            before = edges[slot, ROWS - 1 : ROWS - 1 + m_count]
            after = edges[slot, ROWS + 1 : ROWS + 1 + m_count]
            side = jnp.where(iota((m_count, LANES), 1) < LANES // 2, after, before)
            rows.append(jnp.concatenate([power, side], axis=1).astype(BF))
            powers.append(power)
        noise = dot(jnp.concatenate(rows, axis=0), win[...])
        for i in range(ROWS):
            level = noise[m_count * i : m_count * i + m_count] + NOISE_FLOOR
            found = (powers[i] / level).astype(BF)
            for k in range(ys):
                send4[p, k, span * i : span * i + span] = found[span * k : span * k + span]
        for k in reversed(range(ys)):
            if p == xs - 1 and k == 0:
                recv4[me] = send4[p, y]
                continue
            to_y = lax.rem(y + k, ys)
            copy = plan(
                send4.at[p, to_y], recv4.at[me], s4.at[p, k], r4.at[me],
                {"range": to_y, "pulse": order[p]},
            )
            copy.start()
            fourth.append(copy)

    def place(i):
        for b in range(ROWS):
            turn[turn_row * b : turn_row * b + span] = recv4[
                i, span * b : span * b + span
            ].astype(F32)
        for t in range(span):
            out[i, :, LANES * t : LANES * t + LANES] = turn[pl.ds(t, ROWS, stride=turn_row)]

    @pl.when(is_edge)
    def _():
        loop(lambda c: raw(c).wait_send())

    @pl.when(is_hub)
    def _():
        def body(c):
            for u in range(2):
                at = pl.ds(count * beam_rows * u, count * beam_rows)
                plan(
                    sendp.at[at, lanes(c)], recvp.at[at, lanes(c)], sp.at[c, u], rp.at[c, u],
                    {"chan": 3 - hub},
                ).wait_send()

        loop(body, 0, first)
        for k in range(DIRECT):
            plan(
                sendp.at[:, lanes(first + k)], sendp.at[:, lanes(first + k)], sx.at[k],
                rx.at[k], {"chan": 3 - hub},
            ).wait_send()

        def sprayed(c):
            plan(
                send2.at[pl.ds(0, both - 1), :, lanes(c)],
                send2.at[pl.ds(0, both - 1), :, lanes(c)],
                s2.at[c], r2.at[c], {"chan": edge},
            ).wait_send()

        loop(sprayed, 0, chunks)

    def from_peer(dy, dx, dc):
        i = lax.rem(y + dy, ys) * xs + 2 * lax.rem(chip + dx, 2) + lax.rem(core + dc, 2)
        if (dy, dx, dc) != (0, 0, 0):
            plan(
                send4.at[0, 0], recv4.at[i], s4.at[0, 0], r4.at[i], {"chan": 3 - z}
            ).wait_recv()
        place(i)

    near_first = sorted(np.ndindex(ys, 2, 2), key=lambda k: (k[1], k[0], k[2]))
    for k in near_first[:-2]:
        from_peer(*k)
    for copy in fourth:
        copy.wait_send()
    for k in near_first[-2:]:
        from_peer(*k)


def shards_chain(signal, steering, spectrum):
    beams, chans = steering.shape[1], steering.shape[2]
    _, chan_own, pulse_own, gates = signal.shape
    zs, xs, ys = (lax.axis_size(a) for a in ("chan", "pulse", "range"))
    count = xs * ys
    full = gates * ys
    m_count = full // LANES
    pulses = pulse_own * xs
    depth = 2 * chan_own * pulse_own
    chunks = CHUNKS

    ms = np.arange(m_count)
    angle = 2.0 * np.pi * (np.outer(ms, ms) % m_count) / m_count
    co, si = np.cos(angle), np.sin(angle)
    outer_f = jnp.asarray(np.block([[co, si], [-si, co]]), BF)
    outer_i = jnp.asarray(np.block([[co, -si], [si, co]]), BF)
    ls = np.arange(LANES)
    times = LANES // m_count
    bins = (ls % m_count) * times + ls // m_count
    angle = 2.0 * np.pi * (np.outer(ls, bins) % LANES) / LANES
    co, si = np.cos(angle), np.sin(angle)
    inner_f = jnp.asarray(np.block([[co, -si], [si, co]]), BF)
    inner_i = jnp.asarray(np.block([[co.T, si.T], [-si.T, co.T]]), BF)
    angle = 2.0 * np.pi * np.outer(ms, ls) / full
    twiddle = jnp.asarray(np.stack([np.cos(angle), -np.sin(angle)]), F32)

    dst = np.arange(LANES)
    side = np.where(dst < LANES // 2, dst + LANES, dst - LANES)
    gap = np.abs(np.concatenate([dst, side])[:, None] - dst[None, :])
    window = jnp.asarray(((gap > GUARD) & (gap <= GUARD + TRAIN)) / (2.0 * TRAIN), BF)

    ids = np.arange(pulses)
    angle = (np.outer(ids, ids) % pulses) * (2.0 * np.pi / pulses)
    scale = 1.0 / math.sqrt(pulses)
    dr, di = np.cos(angle) * scale, -np.sin(angle) * scale
    table = np.stack([np.stack([dr, -di], -1), np.stack([di, dr], -1)])
    table = table.reshape(2, xs, pulse_own, xs, pulse_own, 2)
    table = table.transpose(1, 2, 0, 3, 5, 4).reshape(2 * pulses, 2 * pulses)
    table = jnp.asarray(table, BF)

    beam_rows = 2 * pulse_own
    vmem, dma = pltpu.VMEM, pltpu.SemaphoreType.DMA
    any_space = pl.BlockSpec(memory_space=pl.ANY)
    consts = (steering, spectrum, outer_f, outer_i, inner_f, inner_i, twiddle, table, window)
    return pl.pallas_call(
        functools.partial(chain_kernel, (zs, ys, xs, chunks)),
        out_shape=jax.ShapeDtypeStruct((count, pulse_own, gates), F32),
        in_specs=[any_space] * (1 + len(consts)),
        out_specs=pl.BlockSpec(memory_space=vmem),
        scratch_shapes=[vmem(a.shape, a.dtype) for a in consts]
        + [
            vmem((depth, gates), BF),
            vmem((depth, gates), BF),
            vmem((2 * count * beam_rows, gates), BF),
            vmem((2 * count * beam_rows, gates), BF),
            vmem((2 * count * beam_rows, gates), F32),
            vmem((2 * count, beam_rows, gates), BF),
            vmem((ys, xs * beam_rows, gates), BF),
            vmem((DIRECT, ys, xs * beam_rows, gates // chunks), BF),
            vmem((xs * beam_rows * (m_count + ROWS), LANES), F32),
            vmem((xs, ys, gates // LANES * pulse_own, LANES), BF),
            vmem((count, gates // LANES * pulse_own, LANES), BF),
            vmem((2, 2, 2 * count * beam_rows, depth), BF),
            vmem((2 * pulses, 2 * pulses), BF),
            vmem((2, m_count, LANES), F32),
            vmem((2, m_count, LANES), F32),
            vmem((2 * ROWS, m_count + 2 * ROWS, LANES), F32),
            vmem((pulse_own * (m_count // ys + ROWS), LANES), F32),
            dma((len(consts),)),
            dma((chunks,)),
            dma((chunks,)), dma((chunks,)),
            dma((chunks, 2)), dma((chunks, 2)),
            dma((chunks,)), dma((chunks,)),
            dma((DIRECT,)), dma((DIRECT,)),
            dma((xs, ys)), dma((count,)),
        ],
        compiler_params=pltpu.CompilerParams(
            collective_id=0, has_side_effects=True, vmem_limit_bytes=VM
        ),
        name="chain",
    )(*[
        pltpu.with_memory_space_constraint(v, pltpu.HBM)
        for v in (signal.reshape(depth, gates), *map(jnp.asarray, consts))
    ])


def shards(signal, steering, spectrum):
    zs, xs, ys = (lax.axis_size(a) for a in ("chan", "pulse", "range"))
    _, _, pulse_own, gates = signal.shape
    fits = (
        zs == 4
        and xs == 4
        and pulse_own == ROWS
        and steering.shape[1] == zs * xs * ys
        and gates * ys * 2 == LANES * LANES
        and gates % (CHUNKS * LANES) == 0
    )
    return (shards_chain if fits else shards_split)(signal, steering, spectrum)


def solution(mesh):
    in_specs = (P(None, "chan", "pulse", "range"), P(), P())
    out_specs = P("chan", "pulse", "range")
    return jax.shard_map(shards, mesh=mesh, in_specs=in_specs, out_specs=out_specs, check_vma=False)
```

```python
import functools
import math

import jax
import jax.numpy as jnp
import numpy as np
from jax import lax
from jax.experimental import pallas as pl
from jax.experimental.pallas import tpu as pltpu
from jax.sharding import PartitionSpec as P

GUARD = 4
TRAIN = 16
NOISE_FLOOR = 0.25
LANES = 128
ROWS = 8
CHUNKS = 16
LAG = 2
DIRECT = 2
BF = jnp.bfloat16
F32 = jnp.float32
VM = 44 * 1024 * 1024


def dot(a, b):
    return jnp.dot(a, b, preferred_element_type=F32)


def doppler_table(count):
    ids = np.arange(count)
    angle = (np.outer(ids, ids) % count) * (2.0 * np.pi / count)
    scale = 1.0 / math.sqrt(count)
    return jnp.asarray(np.cos(angle) * scale, BF), jnp.asarray(-np.sin(angle) * scale, BF)


def expand(left_ids, left_tag, table, right_ids, right_tag):
    n, m = table.shape
    left = (jnp.asarray(left_ids, jnp.int32)[:, None] == jnp.arange(n)[None, :]).astype(BF)
    right = (jnp.arange(m)[:, None] == jnp.asarray(right_ids, jnp.int32)[None, :]).astype(BF)
    wide = dot(dot(left, table).astype(BF), right)
    same = jnp.asarray(left_tag, jnp.int32)[:, None] == jnp.asarray(right_tag, jnp.int32)[None, :]
    return jnp.where(same, wide, 0.0).astype(BF)


def grid_ids(*sizes):
    return [g.reshape(-1) for g in np.meshgrid(*[np.arange(s) for s in sizes], indexing="ij")]


def call(body, out_shape, name):
    return pl.pallas_call(
        body,
        out_shape=out_shape,
        compiler_params=pltpu.CompilerParams(vmem_limit_bytes=VM),
        name=name,
    )


def form_kernel(w_ref, x_ref, o_ref):
    o_ref[...] = dot(w_ref[...], x_ref[...]).astype(BF)


def range_kernel(blocks, x_ref, f_ref, fi_ref, t_ref, l_ref, li_ref, h_ref, o_ref):
    sources, rows, width = x_ref.shape
    per = width // LANES
    groups = rows // 16
    m_count = sources * per
    tile = []
    for g in range(groups):
        parts = [
            x_ref[s, 16 * g : 16 * g + 16, LANES * j : LANES * j + LANES]
            for s in range(sources)
            for j in range(per)
        ]
        tile.append(jnp.concatenate(parts, axis=0))
    outer = dot(f_ref[...], jnp.concatenate(tile, axis=1))
    tr, ti = t_ref[0], t_ref[1]
    hr, hi = h_ref[0], h_ref[1]
    back = []
    for g in range(groups):
        a = outer[:, LANES * g : LANES * g + LANES].reshape(m_count, 2, ROWS, LANES)
        ar, ai = a[:, 0], a[:, 1]
        b = jnp.concatenate([ar * tr - ai * ti, ar * ti + ai * tr], axis=-1)
        c = dot(b.reshape(m_count * ROWS, 2 * LANES).astype(BF), l_ref[...])
        c = c.reshape(m_count, ROWS, 2 * LANES)
        cr, ci = c[..., :LANES], c[..., LANES:]
        d = jnp.concatenate([cr * hr - ci * hi, cr * hi + ci * hr], axis=-1)
        e = dot(d.reshape(m_count * ROWS, 2 * LANES).astype(BF), li_ref[...])
        e = e.reshape(m_count, ROWS, 2 * LANES)
        er, ei = e[..., :LANES], e[..., LANES:]
        f = jnp.stack([er * tr + ei * ti, ei * tr - er * ti], axis=1)
        back.append(f.reshape(m_count * 16, LANES).astype(BF))
    y = dot(fi_ref[...], jnp.concatenate(back, axis=1)).astype(BF)
    span = m_count // blocks
    for d in range(blocks):
        for j in range(-1, span + 1):
            m = d * span + j
            for g in range(groups):
                if 0 <= m < m_count:
                    v = y[16 * m : 16 * m + 16, LANES * g : LANES * g + LANES]
                else:
                    v = jnp.zeros((16, LANES), BF)
                o_ref[d, 16 * g : 16 * g + 16, LANES * (j + 1) : LANES * (j + 2)] = v


def cfar_kernel(d_ref, x_ref, n_ref, o_ref):
    half = d_ref.shape[0] // 2
    mix = dot(d_ref[...], x_ref[...].reshape(d_ref.shape[1], x_ref.shape[-1]))
    re, im = mix[:half], mix[half:]
    power = re * re + im * im
    narrow = power.astype(BF)
    shape = o_ref.shape[:-1] + (LANES,)
    for j in range(o_ref.shape[-1] // LANES):
        noise = dot(narrow[:, LANES * j : LANES * (j + 3)], n_ref[...])
        own = power[:, LANES * (j + 1) : LANES * (j + 2)]
        found = (own / (noise + NOISE_FLOOR)).astype(BF)
        o_ref[..., LANES * j : LANES * j + LANES] = found.reshape(shape)


def cfar_only_kernel(p_ref, n_ref, o_ref):
    narrow = p_ref[...].astype(BF)
    for j in range(o_ref.shape[1] // LANES):
        noise = dot(narrow[:, LANES * j : LANES * (j + 3)], n_ref[...])
        own = p_ref[:, LANES * (j + 1) : LANES * (j + 2)]
        o_ref[:, LANES * j : LANES * j + LANES] = (own / (noise + NOISE_FLOOR)).astype(BF)


def place_kernel(x_ref, o_ref):
    count, _, width = x_ref.shape
    for s in range(count):
        o_ref[:, width * s : width * s + width] = x_ref[s].astype(F32)


def complex_rows(re, im):
    top = np.stack([re, -im], -1)
    low = np.stack([im, re], -1)
    return np.stack([top, low], 1).reshape(2 * re.shape[0], 2 * re.shape[1])


def shards_split(signal, steering, spectrum):
    beams, chans = steering.shape[1], steering.shape[2]
    _, chan_own, pulse_own, gates = signal.shape
    zs, xs, ys = (lax.axis_size(a) for a in ("chan", "pulse", "range"))
    beam_own = beams // zs
    part = pulse_own // ys
    full = gates * ys
    block = gates // zs
    m_count = full // LANES
    groups = beam_own * part // ROWS
    pulses = pulse_own * xs

    w_real, w_imag = steering[0], steering[1]
    weights = jnp.concatenate(
        [jnp.concatenate([w_real, -w_imag], 1), jnp.concatenate([w_imag, w_real], 1)], 0
    )
    dy, dz, gr, cp, it = grid_ids(ys, zs, groups, 2, ROWS)
    bp = gr * ROWS + it
    left = cp * beams + dz * beam_own + bp // part
    left_pulse = dy * part + bp % part
    sz, ci, ch, pi = grid_ids(zs, 2, chan_own, pulse_own)
    right = ci * chans + sz * chan_own + ch
    form = expand(left, left_pulse, weights, right, pi)

    ms = np.arange(m_count)
    angle = 2.0 * np.pi * (np.outer(ms, ms) % m_count) / m_count
    outer_f = jnp.asarray(complex_rows(np.cos(angle), -np.sin(angle)), BF)
    outer_i = jnp.asarray(complex_rows(np.cos(angle), np.sin(angle)), BF)
    mk, mc, mi = grid_ids(m_count, 2, ROWS)
    outer_f = expand(mk * 2 + mc, mi, outer_f, mk * 2 + mc, mi)
    outer_i = expand(mk * 2 + mc, mi, outer_i, mk * 2 + mc, mi)
    ls = np.arange(LANES)
    angle = 2.0 * np.pi * (np.outer(ls, ls) % LANES) / LANES
    co, si = np.cos(angle), np.sin(angle)
    inner_f = jnp.asarray(np.block([[co, -si], [si, co]]), BF)
    inner_i = jnp.asarray(np.block([[co, si], [-si, co]]), BF)
    angle = 2.0 * np.pi * np.outer(ms, ls) / full
    twiddle = jnp.asarray(np.stack([np.cos(angle), -np.sin(angle)]), F32)
    spread = (2, m_count, ROWS, LANES)
    twiddle = jnp.broadcast_to(twiddle[:, :, None, :], spread)
    response = jnp.swapaxes(spectrum.reshape(2, LANES, m_count), 1, 2) * (1.0 / full)
    response = jnp.broadcast_to(response[:, :, None, :], spread)

    samples = lax.all_to_all(signal, "chan", split_axis=3, concat_axis=0, tiled=True)
    samples = samples.reshape(zs * 2 * chan_own * pulse_own, block)
    rows = 2 * beam_own * part
    formed = call(
        form_kernel, jax.ShapeDtypeStruct((ys * zs * rows, block), BF), "form"
    )(form, samples).reshape(ys * zs, rows, block)
    formed = lax.all_to_all(formed, ("range", "chan"), split_axis=0, concat_axis=0, tiled=True)

    blocks = ys * xs
    own = full // blocks
    padded = own + 2 * LANES
    packed = call(
        functools.partial(range_kernel, blocks),
        jax.ShapeDtypeStruct((blocks, rows, padded), BF),
        "compress",
    )(formed, outer_f, outer_i, twiddle, inner_f, inner_i, response)
    columns = lax.all_to_all(packed, ("range", "pulse"), split_axis=0, concat_axis=0, tiled=True)

    src, dst = np.arange(3 * LANES)[:, None] - LANES, np.arange(LANES)[None, :]
    gap = np.abs(src - dst)
    window = jnp.asarray(((gap > GUARD) & (gap <= GUARD + TRAIN)) / (2.0 * TRAIN), BF)

    dr, di = doppler_table(pulses)
    out_shape = jax.ShapeDtypeStruct((pulses * beam_own, own), BF)
    if 2 * pulses * beam_own <= 1024:
        table = jnp.concatenate([jnp.concatenate([dr, -di], 1), jnp.concatenate([di, dr], 1)], 0)
        oc, oq, ob, of = grid_ids(2, xs, beam_own, pulse_own)
        sy, sx, gr, cp, it = grid_ids(ys, xs, groups, 2, ROWS)
        bp = gr * ROWS + it
        pulse = sx * pulse_own + sy * part + bp % part
        mix = expand(oc * pulses + oq * pulse_own + of, ob, table, cp * pulses + pulse, bp // part)
        found = call(cfar_kernel, out_shape, "cfar")(
            mix, columns.reshape(blocks * rows, padded), window
        )
    else:
        v = columns.reshape(ys, xs, groups, 2, ROWS // part, part, padded)
        v = jnp.transpose(v, (3, 2, 4, 1, 0, 5, 6)).reshape(2, beam_own, pulses, padded)

        def product(t, x):
            return jnp.einsum("fp,bpr->fbr", t, x, preferred_element_type=F32)

        re = product(dr, v[0]) - product(di, v[1])
        im = product(dr, v[1]) + product(di, v[0])
        power = (re * re + im * im).reshape(xs, pulse_own, beam_own, padded)
        power = jnp.swapaxes(power, 1, 2).reshape(pulses * beam_own, padded)
        found = call(cfar_only_kernel, out_shape, "cfar")(power, window)
    found = found.reshape(xs, beam_own * pulse_own, own)
    found = lax.all_to_all(found, "pulse", split_axis=0, concat_axis=0, tiled=True)
    out = call(
        place_kernel, jax.ShapeDtypeStruct((beam_own * pulse_own, gates), F32), "place"
    )(found)
    return out.reshape(beam_own, pulse_own, gates)


MESH = pl.DeviceIdType.MESH


def iota(shape, dim):
    return lax.broadcasted_iota(jnp.int32, shape, dim)


def pick(ids, other):
    return (ids == other).astype(F32).astype(BF)


def widen(row_ids, row_tags, table, col_ids, col_tags):
    n, m = table.shape
    r, c = row_ids.shape[0], col_ids.shape[1]
    wide = dot(pick(row_ids, iota((r, n), 1)), table).astype(BF)
    wide = dot(wide, pick(iota((m, c), 0), col_ids))
    return jnp.where(row_tags == col_tags, wide, 0.0).astype(BF)


def chain_kernel(
    sizes, sig, steer_h, spec_h, f_h, fi_h, inf_h, ini_h, tw_h, dop_h, win_h, out,
    steer, spec, f_t, fi_t, inf, ini, tw, dop_t, win,
    own1, recv1, sendp, recvp, acc, send2, recv2, recvx, dop, send4, recv4,
    wide_w, mix, resp, gates_t, edges, turn,
    const_sem, own_sem, s1, r1, sp, rp, s2, r2, sx, rx, s4, r4,
):
    zs, ys, xs, chunks = sizes
    depth, gates = own1.shape
    width = gates // chunks
    beams, chans = steer.shape[1], steer.shape[2]
    count = ys * xs
    beam_rows = send2.shape[1]
    m_count = tw.shape[1]
    span = m_count // ys
    stride = m_count + ROWS
    turn_row = span + ROWS
    z, y, x = (lax.axis_index(a) for a in ("chan", "range", "pulse"))
    me = y * xs + x
    half = lax.div(z, 2)
    hub, edge = 1 + half, 3 * half
    is_hub = z == hub
    is_edge = z == edge

    consts = [
        pltpu.make_async_copy(a, b, const_sem.at[i])
        for i, (a, b) in enumerate(
            zip(
                (steer_h, spec_h, f_h, fi_h, inf_h, ini_h, tw_h, dop_h, win_h),
                (steer, spec, f_t, fi_t, inf, ini, tw, dop_t, win),
            )
        )
    ]

    def lanes(c):
        return pl.ds(pl.multiple_of(c * width, LANES), width)

    def mine(c):
        return pltpu.make_async_copy(
            sig.at[:, lanes(c)], own1.at[:, lanes(c)], own_sem.at[c]
        )

    def loop(body, start=0, stop=chunks):
        def step(c, carry):
            body(c)
            return carry

        lax.fori_loop(start, stop, step, 0)

    both = 2 * count
    barrier = pltpu.get_barrier_semaphore()

    def greet(**target):
        pl.semaphore_signal(barrier, inc=1, device_id=target, device_id_type=MESH)

    @pl.when(is_hub)
    def _():
        greet(chan=edge)
        for k in range(1, count):
            to = lax.rem(me + k, count)
            greet(range=lax.div(to, xs), pulse=lax.rem(to, xs))
        greet(chan=3 - hub)
        loop(lambda c: mine(c).start())

    def plan(src, dst, send, recv, target):
        return pltpu.make_async_remote_copy(
            src_ref=src, dst_ref=dst, send_sem=send, recv_sem=recv,
            device_id=target, device_id_type=MESH,
        )

    def raw(c):
        return plan(
            sig.at[:, lanes(c)], recv1.at[:, lanes(c)], s1.at[c], r1.at[c], {"chan": hub}
        )

    @pl.when(is_edge)
    def _():
        greet(chan=hub)
        pl.semaphore_wait(barrier, 1)
        loop(lambda c: raw(c).start())
        for k in range(1, count):
            to = lax.rem(me + k, count)
            greet(chan=hub, range=lax.div(to, xs), pulse=lax.rem(to, xs))

    for copy in consts:
        copy.start()
    for copy in consts:
        copy.wait()

    def tables():
        for i in range(2):
            for t in range(m_count):
                gates_t[i, t : t + 1] = spec[i : i + 1, LANES * t : LANES * t + LANES]
            turned = gates_t[i].T * (1.0 / (m_count * LANES))
            resp[i] = jnp.concatenate([turned[:m_count], turned[m_count:]], axis=1)
        edges[...] = jnp.zeros_like(edges)
        for i, g in enumerate(order):
            mix[beam_rows * i : beam_rows * i + beam_rows] = dop_t[
                pl.ds(pl.multiple_of(beam_rows * g, beam_rows), beam_rows)
            ]

    chip, core = lax.div(x, 2), lax.rem(x, 2)
    order = [2 * (1 - chip) + core, 2 * chip + 1 - core, 2 * (1 - chip) + 1 - core, x]

    hops = sorted(
        np.ndindex(2, ys, 2, 2), key=lambda k: -(4 * (k[0] + k[1] + k[2]) + k[3])
    )
    far_first = [
        (dz, lax.rem(y + dy, ys), 2 * lax.rem(chip + dx, 2) + lax.rem(core + dc, 2))
        for dz, dy, dx, dc in hops
        if (dz, dy, dx, dc) != (0, 0, 0, 0)
    ]

    def doppler(c, extra=False):
        tiles = width // LANES
        for i in range(ys):
            v = recv2[i, :, lanes(c)]
            if extra:
                v = (v.astype(F32) + recvx[c - first, i].astype(F32)).astype(BF)
            found = dot(mix[...], v)
            for t in range(tiles):
                m = i * (gates // LANES) + c * tiles + t
                dop[pl.ds(m, xs * beam_rows, stride=stride)] = found[
                    :, LANES * t : LANES * t + LANES
                ]

    first = chunks - DIRECT

    def doppler_both(c):
        k = c - first
        plan(recvx.at[k], recvx.at[k], sx.at[k], rx.at[k], {"chan": 3 - z}).wait_recv()
        doppler(c, True)

    @pl.when(is_hub)
    def _():
        re, im = steer[0], steer[1]
        weights = jnp.concatenate(
            [jnp.concatenate([re, -im], 1), jnp.concatenate([im, re], 1)], 0
        )
        pulse_own = beam_rows // 2
        chan_own = chans // zs
        r = iota((both * beam_rows, 1), 0)
        c = iota((1, depth), 1)
        row_tag, col_tag = lax.rem(r, pulse_own), lax.rem(c, pulse_own)
        r, c = lax.div(r, pulse_own), lax.div(c, pulse_own)
        dest = lax.div(r, 2)
        for i, h in enumerate((half, 1 - half)):
            at = jnp.where(dest < count, 1 + h, 3 * h)
            row = lax.rem(r, 2) * beams + at * count + lax.rem(dest, count)
            for j, source in enumerate((hub, edge)):
                col = lax.div(c, chan_own) * chans + source * chan_own + lax.rem(c, chan_own)
                wide_w[i, j] = widen(row, row_tag, weights, col, col_tag)

        part = count * beam_rows
        mine_rows = pl.ds(pl.multiple_of(beam_rows * x, beam_rows), beam_rows)

        def rows(u):
            return slice(part * u, part * u + part)

        def swap(c, u):
            at = pl.ds(part * u, part)
            return plan(
                sendp.at[at, lanes(c)], recvp.at[at, lanes(c)], sp.at[c, u], rp.at[c, u],
                {"chan": 3 - hub},
            )

        def form(c):
            mine(c).wait()
            raw(c).wait_recv()
            a, b = own1[:, lanes(c)], recv1[:, lanes(c)]
            for u in (1, 0):
                far = dot(wide_w[1, 0, rows(u)], a) + dot(wide_w[1, 1, rows(u)], b)
                sendp[rows(u), lanes(c)] = far.astype(BF)
                swap(c, u).start()
            acc[:, lanes(c)] = dot(wide_w[0, 0], a) + dot(wide_w[0, 1], b)

        def spray(c, u):
            for plane_to, to_y, to_x in far_first:
                if plane_to != u:
                    continue
                to = to_y * xs + to_x
                plan(
                    send2.at[plane_to * count + to, :, lanes(c)],
                    recv2.at[y, mine_rows, lanes(c)], s2.at[c], r2.at[c],
                    {"chan": edge if plane_to else hub, "range": to_y, "pulse": to_x},
                ).start()

        def finish(c):
            for u in (1, 0):
                swap(c, u).wait_recv()
                total = acc[rows(u), lanes(c)] + recvp[rows(u), lanes(c)].astype(F32)
                total = total.astype(BF).reshape(count, beam_rows, width)
                send2[count * u : count * u + count, :, lanes(c)] = total
                spray(c, u)
            recv2[y, mine_rows, lanes(c)] = send2[me, :, lanes(c)]

        def form_both(c):
            mine(c).wait()
            raw(c).wait_recv()
            a, b = own1[:, lanes(c)], recv1[:, lanes(c)]
            for u in (1, 0):
                far = dot(wide_w[1, 0, rows(u)], a) + dot(wide_w[1, 1, rows(u)], b)
                sendp[rows(u), lanes(c)] = far.astype(BF)
                for plane_to, to_y, to_x in far_first + [(0, y, x)]:
                    if plane_to != u:
                        continue
                    to = plane_to * count + to_y * xs + to_x
                    at = pl.ds(pl.multiple_of(beam_rows * to, beam_rows), beam_rows)
                    plan(
                        sendp.at[at, lanes(c)], recvx.at[c - first, y, mine_rows], sx.at[c - first], rx.at[c - first],
                        {
                            "chan": 3 - edge if plane_to else 3 - hub,
                            "range": to_y,
                            "pulse": to_x,
                        },
                    ).start()
            for u in (1, 0):
                total = dot(wide_w[0, 0, rows(u)], a) + dot(wide_w[0, 1, rows(u)], b)
                total = total.astype(BF).reshape(count, beam_rows, width)
                send2[count * u : count * u + count, :, lanes(c)] = total
                spray(c, u)
            recv2[y, mine_rows, lanes(c)] = send2[me, :, lanes(c)]

        def arrived(c):
            plan(
                send2.at[pl.ds(0, count - 1), :, lanes(c)],
                send2.at[pl.ds(0, count - 1), :, lanes(c)],
                s2.at[c], r2.at[c], {"chan": edge},
            ).wait_recv()

        pl.semaphore_wait(barrier, both)

        def body(c):
            form(c)

            @pl.when(c == 0)
            def _():
                tables()

            @pl.when(c >= LAG)
            def _():
                step(c - LAG)

        def step(c):
            finish(c)

            @pl.when(c >= 3)
            def _():
                arrived(c - 3)
                doppler(c - 3)

        loop(body, 0, first)
        step(first - 2)

        def final(c):
            form_both(c)

            @pl.when(c == first)
            def _():
                step(first - 1)

        loop(final, first)

        def rest(c):
            arrived(c)
            doppler(c)

        loop(rest, first - 3, first)

        def rest_both(c):
            arrived(c)
            doppler_both(c)

        loop(rest_both, first)

    @pl.when(is_edge)
    def _():
        tables()

        def arrived(c):
            plan(
                send2.at[pl.ds(0, count), :, lanes(c)],
                send2.at[pl.ds(0, count), :, lanes(c)],
                s2.at[c], r2.at[c], {"chan": hub},
            ).wait_recv()

        def body(c):
            arrived(c)
            doppler(c)

        loop(body, 0, first)

        def body_both(c):
            arrived(c)
            doppler_both(c)

        loop(body_both, first)

    tr, ti = tw[0], tw[1]
    hr, hi = resp[0], resp[1]
    fourth = []

    def split(v, i):
        w = v[:, LANES * i : LANES * i + LANES]
        return w[:m_count], w[m_count:]

    def cut(v, i):
        w = v[m_count * i : m_count * i + m_count]
        return w[:, :LANES], w[:, LANES:]

    for p in range(xs):
        cols = []
        for i in range(ROWS):
            at = stride * (beam_rows * p + 2 * i)
            pair = [dop[at : at + m_count], dop[at + stride : at + stride + m_count]]
            cols.append(jnp.concatenate(pair, axis=0).astype(BF))
        outer = dot(f_t[...], jnp.concatenate(cols, axis=1))
        rows = []
        for i in range(ROWS):
            ar, ai = split(outer, i)
            rows.append(
                jnp.concatenate([ar * tr - ai * ti, ar * ti + ai * tr], axis=1).astype(BF)
            )
        inner = dot(jnp.concatenate(rows, axis=0), inf[...])
        rows = []
        for i in range(ROWS):
            cr, ci = cut(inner, i)
            rows.append(
                jnp.concatenate([cr * hr - ci * hi, cr * hi + ci * hr], axis=1).astype(BF)
            )
        inner = dot(jnp.concatenate(rows, axis=0), ini[...])
        cols = []
        for i in range(ROWS):
            er, ei = cut(inner, i)
            cols.append(
                jnp.concatenate([er * tr + ei * ti, ei * tr - er * ti], axis=0).astype(BF)
            )
        outer = dot(fi_t[...], jnp.concatenate(cols, axis=1))
        rows, powers = [], []
        for i in range(ROWS):
            re, im = split(outer, i)
            power = re * re + im * im
            slot = (p * ROWS + i) % edges.shape[0]
            edges[slot, ROWS : ROWS + m_count] = power
            before = edges[slot, ROWS - 1 : ROWS - 1 + m_count]
            after = edges[slot, ROWS + 1 : ROWS + 1 + m_count]
            side = jnp.where(iota((m_count, LANES), 1) < LANES // 2, after, before)
            rows.append(jnp.concatenate([power, side], axis=1).astype(BF))
            powers.append(power)
        noise = dot(jnp.concatenate(rows, axis=0), win[...])
        for i in range(ROWS):
            level = noise[m_count * i : m_count * i + m_count] + NOISE_FLOOR
            found = (powers[i] / level).astype(BF)
            for k in range(ys):
                send4[p, k, span * i : span * i + span] = found[span * k : span * k + span]
        for k in reversed(range(ys)):
            if p == xs - 1 and k == 0:
                recv4[me] = send4[p, y]
                continue
            to_y = lax.rem(y + k, ys)
            copy = plan(
                send4.at[p, to_y], recv4.at[me], s4.at[p, k], r4.at[me],
                {"range": to_y, "pulse": order[p]},
            )
            copy.start()
            fourth.append(copy)

    def place(i):
        for b in range(ROWS):
            turn[turn_row * b : turn_row * b + span] = recv4[
                i, span * b : span * b + span
            ].astype(F32)
        for t in range(span):
            out[i, :, LANES * t : LANES * t + LANES] = turn[pl.ds(t, ROWS, stride=turn_row)]

    @pl.when(is_edge)
    def _():
        loop(lambda c: raw(c).wait_send())

    @pl.when(is_hub)
    def _():
        def body(c):
            for u in range(2):
                at = pl.ds(count * beam_rows * u, count * beam_rows)
                plan(
                    sendp.at[at, lanes(c)], recvp.at[at, lanes(c)], sp.at[c, u], rp.at[c, u],
                    {"chan": 3 - hub},
                ).wait_send()

        loop(body, 0, first)
        for k in range(DIRECT):
            plan(
                sendp.at[:, lanes(first + k)], sendp.at[:, lanes(first + k)], sx.at[k],
                rx.at[k], {"chan": 3 - hub},
            ).wait_send()

        def sprayed(c):
            plan(
                send2.at[pl.ds(0, both - 1), :, lanes(c)],
                send2.at[pl.ds(0, both - 1), :, lanes(c)],
                s2.at[c], r2.at[c], {"chan": edge},
            ).wait_send()

        loop(sprayed, 0, chunks)

    def from_peer(dy, dx, dc):
        i = lax.rem(y + dy, ys) * xs + 2 * lax.rem(chip + dx, 2) + lax.rem(core + dc, 2)
        if (dy, dx, dc) != (0, 0, 0):
            plan(
                send4.at[0, 0], recv4.at[i], s4.at[0, 0], r4.at[i], {"chan": 3 - z}
            ).wait_recv()
        place(i)

    near_first = sorted(np.ndindex(ys, 2, 2), key=lambda k: (k[1], k[0], k[2]))
    for k in near_first[:-2]:
        from_peer(*k)
    for copy in fourth:
        copy.wait_send()
    for k in near_first[-2:]:
        from_peer(*k)


def shards_chain(signal, steering, spectrum):
    beams, chans = steering.shape[1], steering.shape[2]
    _, chan_own, pulse_own, gates = signal.shape
    zs, xs, ys = (lax.axis_size(a) for a in ("chan", "pulse", "range"))
    count = xs * ys
    full = gates * ys
    m_count = full // LANES
    pulses = pulse_own * xs
    depth = 2 * chan_own * pulse_own
    chunks = CHUNKS

    ms = np.arange(m_count)
    angle = 2.0 * np.pi * (np.outer(ms, ms) % m_count) / m_count
    co, si = np.cos(angle), np.sin(angle)
    outer_f = jnp.asarray(np.block([[co, si], [-si, co]]), BF)
    outer_i = jnp.asarray(np.block([[co, -si], [si, co]]), BF)
    ls = np.arange(LANES)
    times = LANES // m_count
    bins = (ls % m_count) * times + ls // m_count
    angle = 2.0 * np.pi * (np.outer(ls, bins) % LANES) / LANES
    co, si = np.cos(angle), np.sin(angle)
    inner_f = jnp.asarray(np.block([[co, -si], [si, co]]), BF)
    inner_i = jnp.asarray(np.block([[co.T, si.T], [-si.T, co.T]]), BF)
    angle = 2.0 * np.pi * np.outer(ms, ls) / full
    twiddle = jnp.asarray(np.stack([np.cos(angle), -np.sin(angle)]), F32)

    dst = np.arange(LANES)
    side = np.where(dst < LANES // 2, dst + LANES, dst - LANES)
    gap = np.abs(np.concatenate([dst, side])[:, None] - dst[None, :])
    window = jnp.asarray(((gap > GUARD) & (gap <= GUARD + TRAIN)) / (2.0 * TRAIN), BF)

    ids = np.arange(pulses)
    angle = (np.outer(ids, ids) % pulses) * (2.0 * np.pi / pulses)
    scale = 1.0 / math.sqrt(pulses)
    dr, di = np.cos(angle) * scale, -np.sin(angle) * scale
    table = np.stack([np.stack([dr, -di], -1), np.stack([di, dr], -1)])
    table = table.reshape(2, xs, pulse_own, xs, pulse_own, 2)
    table = table.transpose(1, 2, 0, 3, 5, 4).reshape(2 * pulses, 2 * pulses)
    table = jnp.asarray(table, BF)

    beam_rows = 2 * pulse_own
    vmem, dma = pltpu.VMEM, pltpu.SemaphoreType.DMA
    any_space = pl.BlockSpec(memory_space=pl.ANY)
    consts = (steering, spectrum, outer_f, outer_i, inner_f, inner_i, twiddle, table, window)
    return pl.pallas_call(
        functools.partial(chain_kernel, (zs, ys, xs, chunks)),
        out_shape=jax.ShapeDtypeStruct((count, pulse_own, gates), F32),
        in_specs=[any_space] * (1 + len(consts)),
        out_specs=pl.BlockSpec(memory_space=vmem),
        scratch_shapes=[vmem(a.shape, a.dtype) for a in consts]
        + [
            vmem((depth, gates), BF),
            vmem((depth, gates), BF),
            vmem((2 * count * beam_rows, gates), BF),
            vmem((2 * count * beam_rows, gates), BF),
            vmem((2 * count * beam_rows, gates), F32),
            vmem((2 * count, beam_rows, gates), BF),
            vmem((ys, xs * beam_rows, gates), BF),
            vmem((DIRECT, ys, xs * beam_rows, gates // chunks), BF),
            vmem((xs * beam_rows * (m_count + ROWS), LANES), F32),
            vmem((xs, ys, gates // LANES * pulse_own, LANES), BF),
            vmem((count, gates // LANES * pulse_own, LANES), BF),
            vmem((2, 2, 2 * count * beam_rows, depth), BF),
            vmem((2 * pulses, 2 * pulses), BF),
            vmem((2, m_count, LANES), F32),
            vmem((2, m_count, LANES), F32),
            vmem((2 * ROWS, m_count + 2 * ROWS, LANES), F32),
            vmem((pulse_own * (m_count // ys + ROWS), LANES), F32),
            dma((len(consts),)),
            dma((chunks,)),
            dma((chunks,)), dma((chunks,)),
            dma((chunks, 2)), dma((chunks, 2)),
            dma((chunks,)), dma((chunks,)),
            dma((DIRECT,)), dma((DIRECT,)),
            dma((xs, ys)), dma((count,)),
        ],
        compiler_params=pltpu.CompilerParams(
            collective_id=0, has_side_effects=True, vmem_limit_bytes=VM
        ),
        name="chain",
    )(*[
        pltpu.with_memory_space_constraint(v, pltpu.HBM)
        for v in (signal.reshape(depth, gates), *map(jnp.asarray, consts))
    ])


def shards(signal, steering, spectrum):
    zs, xs, ys = (lax.axis_size(a) for a in ("chan", "pulse", "range"))
    _, _, pulse_own, gates = signal.shape
    fits = (
        zs == 4
        and xs == 4
        and pulse_own == ROWS
        and steering.shape[1] == zs * xs * ys
        and gates * ys * 2 == LANES * LANES
        and gates % (CHUNKS * LANES) == 0
    )
    return (shards_chain if fits else shards_split)(signal, steering, spectrum)


def solution(mesh):
    in_specs = (P(None, "chan", "pulse", "range"), P(), P())
    out_specs = P("chan", "pulse", "range")
    return jax.shard_map(shards, mesh=mesh, in_specs=in_specs, out_specs=out_specs, check_vma=False)
```
